32 devices in a mesh: dp: 1 (over z), col: 4 (over y), row: 8 (over x, core).
Axes of the slice: x: 4, y: 4, z: 1, core: 2. Of those that a mesh axis runs over, the one named last changes fastest.
The devices are a block of a 4x4x8 slice.
Arguments:
- seq_in: bfloat16 [64, 16, 2048], P(None, 'dp', 'row')
- w_in1: bfloat16 [2048, 8192], P('row', 'col')
- w_rec1: bfloat16 [2048, 8192], P('row', 'col')
- b_gate1: float32 [8192], P(('col', 'row'))
- w_in2: bfloat16 [2048, 8192], P('row', 'col')
- w_rec2: bfloat16 [2048, 8192], P('row', 'col')
- b_gate2: float32 [8192], P(('col', 'row'))
- h_init: float32 [2, 16, 2048], P(None, 'dp', 'row')
- c_init: float32 [2, 16, 2048], P(None, 'dp', 'row')
Outputs:
- output 1: bfloat16 [64, 16, 2048], P(None, 'dp', ('row', 'col'))
- output 2: float32 [16, 2048], P('dp', ('row', 'col'))
- output 3: float32 [16, 2048], P('dp', ('row', 'col'))
All inputs are finite; a program needn't handle non-finite values.
Results may differ from the reference program's by a relative error of at most 0.00347769.
Values are sent between devices in bfloat16 or wider.
A program may use at most 768 MiB of HBM per device.

```python
import jax
import jax.numpy as jnp
from jax import lax

HIDDEN = 2048
TIME_STEPS = 64
GROUP_BATCH = 16
ROW_SPLIT = 8
COL_SPLIT = 4


def forget_offset():
    unit_dev = HIDDEN // (ROW_SPLIT * COL_SPLIT)
    gate_index = (jnp.arange(4 * HIDDEN) // unit_dev) % 4
    return jnp.where(gate_index == 1, 1.0, 0.0).astype(jnp.float32)


def setup_inputs(seed: int = 0, part: int = 0) -> dict:
    shared_keys = jax.random.split(jax.random.key(seed), 6)
    part_keys = jax.random.split(jax.random.fold_in(jax.random.key(seed + 1), part), 3)
    w_scale = HIDDEN ** -0.5

    def weight_draw(rng_key):
        return (w_scale * jax.random.normal(rng_key, (HIDDEN, 4 * HIDDEN), jnp.float32)).astype(jnp.bfloat16)

    def bias_draw(rng_key):
        return 0.5 * jax.random.normal(rng_key, (4 * HIDDEN,), jnp.float32) + forget_offset()

    return {
        "seq_in": jax.random.normal(part_keys[0], (TIME_STEPS, GROUP_BATCH, HIDDEN), jnp.float32).astype(jnp.bfloat16),
        "w_in1": weight_draw(shared_keys[0]),
        "w_rec1": weight_draw(shared_keys[1]),
        "b_gate1": bias_draw(shared_keys[2]),
        "w_in2": weight_draw(shared_keys[3]),
        "w_rec2": weight_draw(shared_keys[4]),
        "b_gate2": bias_draw(shared_keys[5]),
        "h_init": 0.5 * jax.random.normal(part_keys[1], (2, GROUP_BATCH, HIDDEN), jnp.float32),
        "c_init": 1.2 * jax.random.normal(part_keys[2], (2, GROUP_BATCH, HIDDEN), jnp.float32),
    }


def lstm_layer(in_seq, w_in, w_rec, b_gate, h_first, c_first):
    batch_rows = in_seq.shape[1]
    unit_dev = HIDDEN // (ROW_SPLIT * COL_SPLIT)

    def to_packed(flat_state):
        return flat_state.reshape(batch_rows, ROW_SPLIT, COL_SPLIT, unit_dev).transpose(0, 2, 1, 3)

    def to_plain(packed_state):
        return packed_state.transpose(0, 2, 1, 3).reshape(batch_rows, HIDDEN)

    def lstm_step(carry_in, in_step):
        h_prev, c_prev = carry_in
        z_cols = jnp.dot(in_step, w_in, preferred_element_type=jnp.float32) + b_gate
        z_cols = z_cols + jnp.dot(h_prev, w_rec, preferred_element_type=jnp.float32)
        z_pack = z_cols.reshape(batch_rows, COL_SPLIT, ROW_SPLIT, 4, unit_dev)
        in_gate = jax.nn.sigmoid(z_pack[:, :, :, 0])
        forget = jax.nn.sigmoid(z_pack[:, :, :, 1])
        cell_in = jnp.tanh(z_pack[:, :, :, 2])
        out_gate = jax.nn.sigmoid(z_pack[:, :, :, 3])
        c_new = forget * c_prev + in_gate * cell_in
        h_new = to_plain(out_gate * jnp.tanh(c_new)).astype(jnp.bfloat16)
        return (h_new, c_new), h_new

    carry_out, h_seq = lax.scan(lstm_step, (h_first.astype(jnp.bfloat16), to_packed(c_first)), in_seq)
    return h_seq, to_plain(carry_out[1])


def reference(seq_in, w_in1, w_rec1, b_gate1, w_in2, w_rec2, b_gate2, h_init, c_init):
    h1_seq, c1_last = lstm_layer(seq_in, w_in1, w_rec1, b_gate1, h_init[0], c_init[0])
    h2_seq, c2_last = lstm_layer(h1_seq, w_in2, w_rec2, b_gate2, h_init[1], c_init[1])
    return h2_seq, c1_last, c2_last
```

```python
import functools

import jax
import jax.numpy as jnp
from jax import lax
from jax.experimental import pallas as pl
from jax.experimental.pallas import tpu as pltpu
from jax.sharding import PartitionSpec as P

MESH = pl.DeviceIdType.MESH
F32, BF16 = jnp.float32, jnp.bfloat16
AHEAD = 4
OUT_STEPS = 8


def sigmoid(v):
    return 0.5 * jnp.tanh(0.5 * v) + 0.5


def lstm_kernel(
    n_row, n_col, wr1, wr2, wi1, wi2, x_in, bias, h0, c0, h2_out, c1_out, c2_out,
    wbuf, wi1b, wi2b, xb, bb, bias2, hist, za, zb, h1in, zout, zpre, cst, hin, cin,
    w_send, w_recv, w_relay, rel_recv, rel_send, in_send, in_recv, in_local, hc_send, hin_recv, cin_recv,
    hx_send, hx_recv, za_recv, zb_recv, z_send, h1_send, h1_recv, o_send, o_recv, c_send, c_recv,
):
    steps = x_in.shape[0]
    n_x = n_row // 2
    n_out = steps // OUT_STEPS
    col, row = lax.axis_index("col"), lax.axis_index("row")
    xx, cc = row // 2, row % 2
    head_chip = xx % 2 == 0
    layer = xx // 2
    is_rec = head_chip & (cc == 1)
    is_relay = jnp.logical_not(head_chip) & (cc == 0)
    is_input = jnp.logical_not(is_rec) & jnp.logical_not(is_relay)

    def at(x, c):
        return {"row": x * 2 + c}

    def remote(src, dst, ssem, rsem, dev):
        return pltpu.make_async_remote_copy(
            src_ref=src, dst_ref=dst, send_sem=ssem, recv_sem=rsem, device_id=dev, device_id_type=MESH)

    barrier = pltpu.get_barrier_semaphore()
    for d in range(1, n_row):
        pl.semaphore_signal(barrier, inc=1, device_id={"row": (row + d) % n_row}, device_id_type=MESH)
    for d in range(1, n_col):
        pl.semaphore_signal(barrier, inc=1, device_id={"col": (col + d) % n_col}, device_id_type=MESH)
    pl.semaphore_wait(barrier, n_row + n_col - 2)

    def weight_copies(l, go):
        wr = (wr1, wr2)[l]
        hx = 2 * l
        at_head = (xx == hx) & (cc == 1)
        relayed = ((xx - hx + n_x) % n_x == 2) & (cc == 0)
        own = pltpu.make_async_copy(wr, wbuf.at[:, row], w_send.at[l])
        direct = remote(wr, wbuf.at[:, row], w_send.at[l], w_recv.at[row], at(hx, 1))
        parts = [
            remote(wr.at[j], wbuf.at[j, row], rel_send.at[j], rel_recv.at[j], at((hx + 1) % n_x, 0))
            for j in range(n_col)
        ]

        @pl.when(at_head)
        def _():
            own.start() if go else own.wait()

        @pl.when(relayed)
        def _():
            for part in parts:
                part.start() if go else part.wait_send()

        @pl.when(jnp.logical_not(at_head) & jnp.logical_not(relayed))
        def _():
            direct.start() if go else direct.wait_send()

    def small_copies(l, go):
        hx = 2 * l
        at_head = (xx == hx) & (cc == 1)
        own = [
            pltpu.make_async_copy(h0.at[l], hin.at[row], hc_send.at[l, 0]),
            pltpu.make_async_copy(c0.at[l], cin.at[row], hc_send.at[l, 1]),
        ]
        away = [
            remote(h0.at[l], hin.at[row], hc_send.at[l, 0], hin_recv.at[row], at(hx, 1)),
            remote(c0.at[l], cin.at[row], hc_send.at[l, 1], cin_recv.at[row], at(hx, 1)),
        ]

        @pl.when(at_head)
        def _():
            for cp in own:
                cp.start() if go else cp.wait()

        @pl.when(jnp.logical_not(at_head))
        def _():
            for cp in away:
                cp.start() if go else cp.wait_send()

    pairs = [(x_in, xb.at[cc]), (wi1, wi1b.at[cc]), (bias, bb.at[cc]), (wi2, wi2b.at[:, cc])]
    to_input = [remote(s, d, in_send.at[i], in_recv.at[i], at(xx, 1 - cc)) for i, (s, d) in enumerate(pairs)]
    to_self = [pltpu.make_async_copy(s, d, in_local.at[i]) for i, (s, d) in enumerate(pairs)]
    others = [xb.at[1 - cc], wi1b.at[1 - cc], bb.at[1 - cc], wi2b.at[:, 1 - cc]]
    from_other = [remote(s, d, in_send.at[i], in_recv.at[i], at(xx, 1 - cc))
                  for i, ((s, _), d) in enumerate(zip(pairs, others))]

    @pl.when(is_input)
    def _():
        for cp in to_self:
            cp.start()

    @pl.when(jnp.logical_not(is_input))
    def _():
        for cp in to_input:
            cp.start()

    for l in range(2):
        small_copies(l, True)
    for l in range(2):
        weight_copies(l, True)

    @pl.when(is_relay)
    def _():
        origin = ((xx + 1) % n_x) * 2
        dst = at((xx + n_x - 1) % n_x, 1)
        for j in range(n_col):
            remote(wr1.at[j], wbuf.at[j, origin], rel_send.at[j], rel_recv.at[j], dst).wait_recv()
            remote(wbuf.at[j, origin], wbuf.at[j, origin], rel_send.at[j], w_relay.at[j], dst).start()
        for j in range(n_col):
            remote(wbuf.at[j, origin], wbuf.at[j, origin], rel_send.at[j], w_relay.at[j], dst).wait_send()

    @pl.when(is_rec)
    def _():
        last = (col + 2) % n_col

        def peer(d):
            return {"col": (col + d) % n_col}

        def h_copy(t, owner, half, d, par):
            ref = hist.at[t, owner, half]
            return remote(ref, ref, hx_send.at[par, d - 1, half], hx_recv.at[par, owner, half], peer(d))

        def w_half(owner, half):
            return wbuf.at[owner, pl.ds(half * 4, 4)]

        def product(t, owner, half):
            w = wbuf[owner, half * 4:half * 4 + 4].reshape(256, 2048)
            return jnp.dot(hist[t, owner, half], w, preferred_element_type=F32)

        def z_arrival(t):
            return remote(za.at[t], za.at[t], z_send.at[0, 0], za_recv.at[t], at(xx, 0))

        def forward(t, go):
            for x in range(n_x):
                src = hist.at[t + 1, :, x // 2, :, pl.ds((x % 2) * 128, 128)]
                cp = remote(src, h1in.at[t], h1_send.at[x], h1_recv.at[t], at(x, x % 2))
                cp.start() if go else cp.wait_send()

        def out_copies(n, go):
            rows = pl.ds(n * OUT_STEPS, OUT_STEPS)
            for r in range(n_row):
                x = r // 2
                src = hist.at[pl.ds(n * OUT_STEPS + 1, OUT_STEPS), col, x // 2, :, pl.ds((x % 2) * 128, 128)]
                own = pltpu.make_async_copy(src, h2_out.at[rows], o_send.at[r])
                away = remote(src, h2_out.at[rows], o_send.at[r], o_recv.at[n], {"row": r})
                if r == 5:
                    own.start() if go else own.wait()
                else:
                    away.start() if go else away.wait_send()

        for r in range(n_row):
            @pl.when(row != r)
            def _(r=r):
                remote(h0.at[0], hin.at[r], hc_send.at[0, 0], hin_recv.at[r], at(xx, 0)).wait_recv()
                remote(c0.at[0], cin.at[r], hc_send.at[0, 1], cin_recv.at[r], at(xx, 0)).wait_recv()
        for l in range(2):
            @pl.when(layer == l)
            def _(l=l):
                small_copies(l, False)
        for x in range(n_x):
            cst[x // 2, :, (x % 2) * 128:(x % 2) * 128 + 128] = cin[2 * x] + cin[2 * x + 1]
        hist[0, last] = jnp.zeros(hist.shape[2:], BF16)
        for l in range(2):
            @pl.when(layer == l)
            def _(l=l):
                weight_copies(l, False)
        relayed = ((xx + 2) % n_x) * 2
        for r in range(n_row):
            @pl.when((row != r) & (relayed != r))
            def _(r=r):
                remote(wr1, wbuf.at[:, r], w_send.at[0], w_recv.at[r], at(xx, 0)).wait_recv()
        for j in range(n_col):
            remote(wbuf.at[j, relayed], wbuf.at[j, relayed], rel_send.at[j], w_relay.at[j], at(xx, 0)).wait_recv()

        z_arrival(0).wait_recv()
        zpre[...] = za[0]
        for r in range(n_row):
            w = wbuf[:, r].reshape(256, 2048)
            zpre[...] += jnp.dot(hin[r], w, preferred_element_type=F32)

        def step(t, carry):
            par, par_before = t % 2, (t + 1) % 2
            exchange = (t < steps - 1) | (layer == 0)

            @pl.when(t > 0)
            def _():
                h_copy(t, last, 0, 2, par_before).wait_recv()

            zpre[...] += product(t, last, 0)

            @pl.when(t > 0)
            def _():
                h_copy(t, last, 1, 2, par_before).wait_recv()

            h_last = hist[t, last, 1]
            for half in range(2):
                z = []
                for m in range(4):
                    cols = slice(half * 1024 + m * 256, half * 1024 + m * 256 + 256)
                    w = wbuf[last, 4:8, :, cols].reshape(256, 256)
                    z.append(jnp.dot(h_last, w, preferred_element_type=F32) + zpre[:, cols])
                c_new = sigmoid(z[1]) * cst[half] + sigmoid(z[0]) * jnp.tanh(z[2])
                cst[half] = c_new
                hist[t + 1, col, half] = (sigmoid(z[3]) * jnp.tanh(c_new)).astype(BF16)

                @pl.when(exchange)
                def _(half=half):
                    for d in (2, 1, 3):
                        h_copy(t + 1, col, half, d, par).start()

            @pl.when((t > 0) & (layer == 0))
            def _():
                forward(t - 1, True)

            @pl.when(t < steps - 1)
            def _():
                acc = product(t + 1, col, 0) + product(t + 1, col, 1)
                z_arrival(t + 1).wait_recv()
                zpre[...] = acc + za[t + 1]
                for d in (1, 3):
                    owner = (col + d) % n_col
                    h_copy(t + 1, owner, 0, d, par).wait_recv()
                    h_copy(t + 1, owner, 1, d, par).wait_recv()
                    zpre[...] += product(t + 1, owner, 0) + product(t + 1, owner, 1)

            @pl.when((t > 0) & (layer == 0))
            def _():
                forward(t - 1, False)

            @pl.when(exchange)
            def _():
                for d in (2, 1, 3):
                    for half in range(2):
                        h_copy(t + 1, col, half, d, par).wait_send()

            @pl.when((layer == 1) & (t % OUT_STEPS == OUT_STEPS - 1))
            def _():
                n = t // OUT_STEPS

                @pl.when(n > 0)
                def _():
                    out_copies(n - 1, False)

                out_copies(n, True)

            return carry

        lax.fori_loop(0, steps, step, 0)

        def c_copies(l, go):
            for r in range(n_row):
                x = r // 2
                src = cst.at[x // 2, :, pl.ds((x % 2) * 128, 128)]
                out = (c1_out, c2_out)[l]
                if r == 4 * l + 1:
                    cp = pltpu.make_async_copy(src, out, c_send.at[r])
                    cp.start() if go else cp.wait()
                else:
                    cp = remote(src, out, c_send.at[r], c_recv.at[l], {"row": r})
                    cp.start() if go else cp.wait_send()

        @pl.when(layer == 0)
        def _():
            c_copies(0, True)
            for d in (1, 3, 2):
                for half in range(2):
                    h_copy(steps, (col + d) % n_col, half, d, (steps - 1) % 2).wait_recv()
            forward(steps - 1, True)
            forward(steps - 1, False)
            c_copies(0, False)

        @pl.when(layer == 1)
        def _():
            c_copies(1, True)
            out_copies(n_out - 1, False)
            c_copies(1, False)

    @pl.when(is_input)
    def _():
        for cp in to_self:
            cp.wait()
        for cp in from_other:
            cp.wait_recv()
        bias2[...] = bb[0] + bb[1]
        place = [xx, (xx + 2) % n_x]

        def arrival(buf, sem, u):
            return remote(buf.at[u], buf.at[u], z_send.at[0, 0], sem.at[u], at(xx, 1 - cc))

        def departure(l, u, start):
            p = place[l]
            dst_x = jnp.where(p == 0, xx, jnp.where(p == 1, (xx + n_x - 1) % n_x, (xx + 1) % n_x))
            dst_c = jnp.where(p == 0, 1, dst_x % 2)
            src = zout.at[l, u % 2]
            to_a = remote(src, za.at[u], z_send.at[l, u % 2], za_recv.at[u], at(dst_x, dst_c))
            if not start:
                to_a.wait_send()
                return
            to_b = remote(src, zb.at[u], z_send.at[l, u % 2], zb_recv.at[u], at(dst_x, dst_c))

            @pl.when(p == 3)
            def _():
                to_b.start()

            @pl.when(p != 3)
            def _():
                to_a.start()

        def input_sum(l, u):
            p = place[l]

            @pl.when(u >= 2)
            def _():
                departure(l, u - 2, False)

            if l == 0:
                part = jnp.dot(xb[0, u], wi1b[0], preferred_element_type=F32)
                part += jnp.dot(xb[1, u], wi1b[1], preferred_element_type=F32)
            else:
                h1 = jnp.concatenate([h1in[u, j] for j in range(n_col)], axis=1)
                part = jnp.dot(h1, wi2b[...].reshape(512, 2048), preferred_element_type=F32)
            out = zout.at[l, u % 2]
            out[...] = part + bias2[l]

            @pl.when((p == 0) | (p == 3))
            def _():
                arrival(za, za_recv, u).wait_recv()
                out[...] += za[u]

            @pl.when(p == 0)
            def _():
                arrival(zb, zb_recv, u).wait_recv()
                out[...] += zb[u]

            departure(l, u, True)

        def ahead(u, carry):
            input_sum(0, u)
            return carry

        lax.fori_loop(0, AHEAD, ahead, 0)

        def step(t, carry):
            @pl.when(t + AHEAD < steps)
            def _():
                input_sum(0, t + AHEAD)

            remote(h1in.at[t], h1in.at[t], h1_send.at[0], h1_recv.at[t], at(xx, 1 - cc)).wait_recv()
            input_sum(1, t)
            return carry

        lax.fori_loop(0, steps, step, 0)
        for l in range(2):
            for u in range(steps - 2, steps):
                departure(l, u, False)

    for l in range(2):
        @pl.when(jnp.logical_not(is_rec & (layer == l)))
        def _(l=l):
            small_copies(l, False)
            weight_copies(l, False)

    @pl.when(jnp.logical_not(is_input))
    def _():
        for cp in to_input:
            cp.wait_send()

    @pl.when(jnp.logical_not(is_rec & (layer == 0)))
    def _():
        remote(c1_out, c1_out, c_send.at[0], c_recv.at[0], at(xx, 1 - cc)).wait_recv()

    @pl.when(jnp.logical_not(is_rec & (layer == 1)))
    def _():
        remote(c2_out, c2_out, c_send.at[0], c_recv.at[1], at(xx, 1 - cc)).wait_recv()
        for n in range(n_out):
            rows = pl.ds(n * OUT_STEPS, OUT_STEPS)
            remote(h2_out.at[rows], h2_out.at[rows], o_send.at[0], o_recv.at[n], at(xx, 1 - cc)).wait_recv()


def solution(mesh):
    n_row, n_col = mesh.shape["row"], mesh.shape["col"]

    def gate_major(w, unit):
        rows = w.shape[0]
        w = w.reshape(rows, n_row // 4, 4, 4, unit).transpose(0, 1, 3, 2, 4)
        return w.reshape(rows, n_row * 4 * unit)

    def local_program(seq_in, w_in1, w_rec1, b_gate1, w_in2, w_rec2, b_gate2, h_init, c_init):
        steps, batch, k_rows = seq_in.shape
        unit = b_gate1.shape[0] // 4
        cols = w_in1.shape[1]
        col, row = lax.axis_index("col"), lax.axis_index("row")

        def by_owner(w):
            return gate_major(w, unit).reshape(n_col, unit, cols)

        bias = jnp.stack([b_gate1, b_gate2]).reshape(2, 1, 4, 1, unit)
        bias = lax.dynamic_update_slice(
            jnp.zeros((2, n_row // 4, 4, 4, unit), F32), bias, (0, row // 4, 0, row % 4, 0)).reshape(2, 1, cols)
        c_own = lax.dynamic_slice_in_dim(c_init, col * unit, unit, axis=2)
        c_pad = lax.dynamic_update_slice(jnp.zeros((2, batch, 2 * unit), F32), c_own, (0, 0, (row % 2) * unit))
        hid = n_row * unit

        hbm = pl.BlockSpec(memory_space=pl.ANY)
        dma = pltpu.SemaphoreType.DMA
        vm = pltpu.VMEM
        h2_pair, c1_pair, c2_pair = pl.pallas_call(
            functools.partial(lstm_kernel, n_row, n_col),
            out_shape=(
                jax.ShapeDtypeStruct((steps, batch, 2 * unit), BF16),
                jax.ShapeDtypeStruct((batch, 2 * unit), F32),
                jax.ShapeDtypeStruct((batch, 2 * unit), F32),
            ),
            in_specs=[hbm] * 8,
            out_specs=(hbm, hbm, hbm),
            scratch_shapes=[
                vm((n_col, n_row, unit, cols), BF16),
                vm((2, k_rows, cols), BF16),
                vm((n_col, 2, unit, cols), BF16),
                vm((2, steps, batch, k_rows), BF16),
                vm((2, 2, 1, cols), F32),
                vm((2, 1, cols), F32),
                vm((steps + 1, n_col, 2, batch, hid // 2), BF16),
                vm((steps, batch, cols), F32),
                vm((steps, batch, cols), F32),
                vm((steps, n_col, batch, 2 * unit), BF16),
                vm((2, 2, batch, cols), F32),
                vm((batch, cols), F32),
                vm((2, batch, hid // 2), F32),
                vm((n_row, batch, k_rows), BF16),
                vm((n_row, batch, 2 * unit), F32),
                dma((2,)), dma((n_row,)), dma((n_col,)), dma((n_col,)), dma((n_col,)),
                dma((4,)), dma((4,)), dma((4,)),
                dma((2, 2)), dma((n_row,)), dma((n_row,)),
                dma((2, n_col - 1, 2)), dma((2, n_col, 2)),
                dma((steps,)), dma((steps,)), dma((2, 2)),
                dma((n_row // 2,)), dma((steps,)),
                dma((n_row,)), dma((steps // OUT_STEPS,)),
                dma((n_row,)), dma((2,)),
            ],
            compiler_params=pltpu.CompilerParams(
                collective_id=0, has_side_effects=True, vmem_limit_bytes=60 * 2**20),
        )(
            by_owner(w_rec1), by_owner(w_rec2), gate_major(w_in1, unit), by_owner(w_in2),
            seq_in, bias, h_init.astype(BF16), c_pad,
        )

        def own_half(pair):
            return lax.dynamic_slice_in_dim(pair, (row % 2) * unit, unit, axis=pair.ndim - 1)

        return own_half(h2_pair), own_half(c1_pair), own_half(c2_pair)

    row_spec = P(None, "dp", "row")
    weight_spec = P("row", "col")
    bias_spec = P(("col", "row"))
    seq_out_spec = P(None, "dp", ("row", "col"))
    cell_out_spec = P("dp", ("row", "col"))
    return jax.shard_map(
        local_program,
        mesh=mesh,
        in_specs=(row_spec, weight_spec, weight_spec, bias_spec, weight_spec, weight_spec, bias_spec, row_spec, row_spec),
        out_specs=(seq_out_spec, cell_out_spec, cell_out_spec),
        check_vma=False,
    )
```

```python
import functools

import jax
import jax.numpy as jnp
from jax import lax
from jax.experimental import pallas as pl
from jax.experimental.pallas import tpu as pltpu
from jax.sharding import PartitionSpec as P

MESH = pl.DeviceIdType.MESH
F32, BF16 = jnp.float32, jnp.bfloat16
AHEAD = (3, 6, 10, 6)
FIRST = (3, 4, 10, 4)
OUT_STEPS = 8


def sigmoid(v):
    return 0.5 * jnp.tanh(0.5 * v) + 0.5


def lstm_kernel(
    n_row, n_col, wr1, wr2, wi1, wi2, x_in, bias, h0, c0, h2_out, c1_out, c2_out,
    wbuf, wi1b, wi2b, xb, bb, bias2, hist, za, zb, h1in, zout, zpre, cst, hin, cin,
    w_send, w_recv, w_relay, rel_recv, rel_send, in_send, in_recv, in_local, hc_send, hin_recv, cin_recv,
    hx_send, hx_recv, za_recv, zb_recv, z_send, h1_send, h1_recv, o_send, o_recv, c_send, c_recv,
):
    steps = x_in.shape[0]
    n_x = n_row // 2
    n_out = steps // OUT_STEPS
    col, row = lax.axis_index("col"), lax.axis_index("row")
    xx, cc = row // 2, row % 2
    head_chip = xx % 2 == 0
    layer = xx // 2
    is_rec = head_chip & (cc == 1)
    is_relay = jnp.logical_not(head_chip) & (cc == 0)
    is_input = jnp.logical_not(is_rec) & jnp.logical_not(is_relay)

    def at(x, c):
        return {"row": x * 2 + c}

    def remote(src, dst, ssem, rsem, dev):
        return pltpu.make_async_remote_copy(
            src_ref=src, dst_ref=dst, send_sem=ssem, recv_sem=rsem, device_id=dev, device_id_type=MESH)

    barrier = pltpu.get_barrier_semaphore()
    for d in range(1, n_row):
        pl.semaphore_signal(barrier, inc=1, device_id={"row": (row + d) % n_row}, device_id_type=MESH)
    for d in range(1, n_col):
        pl.semaphore_signal(barrier, inc=1, device_id={"col": (col + d) % n_col}, device_id_type=MESH)
    pl.semaphore_wait(barrier, n_row + n_col - 2)

    def weight_copies(l, go):
        wr = (wr1, wr2)[l]
        hx = 2 * l
        at_head = (xx == hx) & (cc == 1)
        relayed = ((xx - hx + n_x) % n_x == 2) & (cc == 0)
        own = pltpu.make_async_copy(wr, wbuf.at[:, row], w_send.at[l])
        direct = remote(wr, wbuf.at[:, row], w_send.at[l], w_recv.at[row], at(hx, 1))
        parts = [
            remote(wr.at[j], wbuf.at[j, row], rel_send.at[j], rel_recv.at[j], at((hx + 1) % n_x, 0))
            for j in range(n_col)
        ]

        @pl.when(at_head)
        def _():
            own.start() if go else own.wait()

        @pl.when(relayed)
        def _():
            for part in parts:
                part.start() if go else part.wait_send()

        @pl.when(jnp.logical_not(at_head) & jnp.logical_not(relayed))
        def _():
            direct.start() if go else direct.wait_send()

    def small_copies(l, go):
        hx = 2 * l
        at_head = (xx == hx) & (cc == 1)
        own = [
            pltpu.make_async_copy(h0.at[l], hin.at[row], hc_send.at[l, 0]),
            pltpu.make_async_copy(c0.at[l], cin.at[row], hc_send.at[l, 1]),
        ]
        away = [
            remote(h0.at[l], hin.at[row], hc_send.at[l, 0], hin_recv.at[row], at(hx, 1)),
            remote(c0.at[l], cin.at[row], hc_send.at[l, 1], cin_recv.at[row], at(hx, 1)),
        ]

        @pl.when(at_head)
        def _():
            for cp in own:
                cp.start() if go else cp.wait()

        @pl.when(jnp.logical_not(at_head))
        def _():
            for cp in away:
                cp.start() if go else cp.wait_send()

    pairs = [(x_in, xb.at[cc]), (wi1, wi1b.at[cc]), (bias, bb.at[cc]), (wi2, wi2b.at[:, cc])]
    to_input = [remote(s, d, in_send.at[i], in_recv.at[i], at(xx, 1 - cc)) for i, (s, d) in enumerate(pairs)]
    to_self = [pltpu.make_async_copy(s, d, in_local.at[i]) for i, (s, d) in enumerate(pairs)]
    others = [xb.at[1 - cc], wi1b.at[1 - cc], bb.at[1 - cc], wi2b.at[:, 1 - cc]]
    from_other = [remote(s, d, in_send.at[i], in_recv.at[i], at(xx, 1 - cc))
                  for i, ((s, _), d) in enumerate(zip(pairs, others))]

    @pl.when(is_input)
    def _():
        for cp in to_self:
            cp.start()

    @pl.when(jnp.logical_not(is_input))
    def _():
        for cp in to_input:
            cp.start()

    for l in range(2):
        small_copies(l, True)
    for l in range(2):
        weight_copies(l, True)

    @pl.when(is_relay)
    def _():
        origin = ((xx + 1) % n_x) * 2
        dst = at((xx + n_x - 1) % n_x, 1)
        for j in range(n_col):
            remote(wr1.at[j], wbuf.at[j, origin], rel_send.at[j], rel_recv.at[j], dst).wait_recv()
            remote(wbuf.at[j, origin], wbuf.at[j, origin], rel_send.at[j], w_relay.at[j], dst).start()
        for j in range(n_col):
            remote(wbuf.at[j, origin], wbuf.at[j, origin], rel_send.at[j], w_relay.at[j], dst).wait_send()

    @pl.when(is_rec)
    def _():
        last = (col + 2) % n_col

        def peer(d):
            return {"col": (col + d) % n_col}

        def h_copy(t, owner, half, d, par):
            ref = hist.at[t, owner, half]
            return remote(ref, ref, hx_send.at[par, d - 1, half], hx_recv.at[par, owner, half], peer(d))

        def w_half(owner, half):
            return wbuf.at[owner, pl.ds(half * 4, 4)]

        def product(t, owner, half):
            w = wbuf[owner, half * 4:half * 4 + 4].reshape(256, 2048)
            return jnp.dot(hist[t, owner, half], w, preferred_element_type=F32)

        def z_arrival(t):
            return remote(za.at[t], za.at[t], z_send.at[0, 0], za_recv.at[t], at(xx, 0))

        def forward(t, go):
            for x in range(n_x):
                src = hist.at[t + 1, :, x // 2, :, pl.ds((x % 2) * 128, 128)]
                cp = remote(src, h1in.at[t], h1_send.at[x], h1_recv.at[t], at(x, x % 2))
                cp.start() if go else cp.wait_send()

        def out_copies(n, go):
            rows = pl.ds(n * OUT_STEPS, OUT_STEPS)
            for r in range(n_row):
                x = r // 2
                src = hist.at[pl.ds(n * OUT_STEPS + 1, OUT_STEPS), col, x // 2, :, pl.ds((x % 2) * 128, 128)]
                own = pltpu.make_async_copy(src, h2_out.at[rows], o_send.at[r])
                away = remote(src, h2_out.at[rows], o_send.at[r], o_recv.at[n], {"row": r})
                if r == 5:
                    own.start() if go else own.wait()
                else:
                    away.start() if go else away.wait_send()

        for r in range(n_row):
            @pl.when(row != r)
            def _(r=r):
                remote(h0.at[0], hin.at[r], hc_send.at[0, 0], hin_recv.at[r], at(xx, 0)).wait_recv()
                remote(c0.at[0], cin.at[r], hc_send.at[0, 1], cin_recv.at[r], at(xx, 0)).wait_recv()
        for l in range(2):
            @pl.when(layer == l)
            def _(l=l):
                small_copies(l, False)
        for x in range(n_x):
            cst[x // 2, :, (x % 2) * 128:(x % 2) * 128 + 128] = cin[2 * x] + cin[2 * x + 1]
        hist[0, last] = jnp.zeros(hist.shape[2:], BF16)
        for l in range(2):
            @pl.when(layer == l)
            def _(l=l):
                weight_copies(l, False)
        relayed = ((xx + 2) % n_x) * 2
        for r in range(n_row):
            @pl.when((row != r) & (relayed != r))
            def _(r=r):
                remote(wr1, wbuf.at[:, r], w_send.at[0], w_recv.at[r], at(xx, 0)).wait_recv()
        for j in range(n_col):
            remote(wbuf.at[j, relayed], wbuf.at[j, relayed], rel_send.at[j], w_relay.at[j], at(xx, 0)).wait_recv()

        z_arrival(0).wait_recv()
        zpre[...] = za[0]
        for r in range(n_row):
            w = wbuf[:, r].reshape(256, 2048)
            zpre[...] += jnp.dot(hin[r], w, preferred_element_type=F32)

        def step(t, carry):
            par, par_before = t % 2, (t + 1) % 2
            exchange = (t < steps - 1) | (layer == 0)

            @pl.when(t > 0)
            def _():
                h_copy(t, last, 0, 2, par_before).wait_recv()

            zpre[...] += product(t, last, 0)

            @pl.when(t > 0)
            def _():
                h_copy(t, last, 1, 2, par_before).wait_recv()

            h_last = hist[t, last, 1]
            for half in range(2):
                z = []
                for m in range(4):
                    cols = slice(half * 1024 + m * 256, half * 1024 + m * 256 + 256)
                    w = wbuf[last, 4:8, :, cols].reshape(256, 256)
                    z.append(jnp.dot(h_last, w, preferred_element_type=F32) + zpre[:, cols])
                c_new = sigmoid(z[1]) * cst[half] + sigmoid(z[0]) * jnp.tanh(z[2])
                cst[half] = c_new
                hist[t + 1, col, half] = (sigmoid(z[3]) * jnp.tanh(c_new)).astype(BF16)

                @pl.when(exchange)
                def _(half=half):
                    for d in (2, 1, 3):
                        h_copy(t + 1, col, half, d, par).start()

            @pl.when((t > 0) & (layer == 0))
            def _():
                forward(t - 1, True)

            @pl.when(t < steps - 1)
            def _():
                acc = product(t + 1, col, 0) + product(t + 1, col, 1)
                z_arrival(t + 1).wait_recv()
                zpre[...] = acc + za[t + 1]
                for d in (1, 3):
                    owner = (col + d) % n_col
                    h_copy(t + 1, owner, 0, d, par).wait_recv()
                    h_copy(t + 1, owner, 1, d, par).wait_recv()
                    zpre[...] += product(t + 1, owner, 0) + product(t + 1, owner, 1)

            @pl.when((t > 0) & (layer == 0))
            def _():
                forward(t - 1, False)

            @pl.when(exchange)
            def _():
                for d in (2, 1, 3):
                    for half in range(2):
                        h_copy(t + 1, col, half, d, par).wait_send()

            @pl.when((layer == 1) & (t % OUT_STEPS == OUT_STEPS - 1))
            def _():
                n = t // OUT_STEPS

                @pl.when(n > 0)
                def _():
                    out_copies(n - 1, False)

                out_copies(n, True)

            return carry

        lax.fori_loop(0, steps, step, 0)

        def c_copies(l, go):
            for r in range(n_row):
                x = r // 2
                src = cst.at[x // 2, :, pl.ds((x % 2) * 128, 128)]
                out = (c1_out, c2_out)[l]
                if r == 4 * l + 1:
                    cp = pltpu.make_async_copy(src, out, c_send.at[r])
                    cp.start() if go else cp.wait()
                else:
                    cp = remote(src, out, c_send.at[r], c_recv.at[l], {"row": r})
                    cp.start() if go else cp.wait_send()

        @pl.when(layer == 0)
        def _():
            c_copies(0, True)
            for d in (1, 3, 2):
                for half in range(2):
                    h_copy(steps, (col + d) % n_col, half, d, (steps - 1) % 2).wait_recv()
            forward(steps - 1, True)
            forward(steps - 1, False)
            c_copies(0, False)

        @pl.when(layer == 1)
        def _():
            c_copies(1, True)
            out_copies(n_out - 1, False)
            c_copies(1, False)

    @pl.when(is_input)
    def _():
        for cp in to_self:
            cp.wait()
        for cp in from_other:
            cp.wait_recv()
        bias2[...] = bb[0] + bb[1]
        place = [xx, (xx + 2) % n_x]

        def arrival(buf, sem, u):
            return remote(buf.at[u], buf.at[u], z_send.at[0, 0], sem.at[u], at(xx, 1 - cc))

        def departure(l, u, start):
            p = place[l]
            dst_x = jnp.where(p == 0, xx, jnp.where(p == 1, (xx + n_x - 1) % n_x, (xx + 1) % n_x))
            dst_c = jnp.where(p == 0, 1, dst_x % 2)
            src = zout.at[l, u % 2]
            to_a = remote(src, za.at[u], z_send.at[l, u % 2], za_recv.at[u], at(dst_x, dst_c))
            if not start:
                to_a.wait_send()
                return
            to_b = remote(src, zb.at[u], z_send.at[l, u % 2], zb_recv.at[u], at(dst_x, dst_c))

            @pl.when(p == 3)
            def _():
                to_b.start()

            @pl.when(p != 3)
            def _():
                to_a.start()

        def input_sum(l, u):
            p = place[l]

            @pl.when(u >= 2)
            def _():
                departure(l, u - 2, False)

            if l == 0:
                part = jnp.dot(xb[0, u], wi1b[0], preferred_element_type=F32)
                part += jnp.dot(xb[1, u], wi1b[1], preferred_element_type=F32)
            else:
                h1 = jnp.concatenate([h1in[u, j] for j in range(n_col)], axis=1)
                part = jnp.dot(h1, wi2b[...].reshape(512, 2048), preferred_element_type=F32)
            out = zout.at[l, u % 2]
            out[...] = part + bias2[l]

            @pl.when((p == 0) | (p == 3))
            def _():
                arrival(za, za_recv, u).wait_recv()
                out[...] += za[u]

            @pl.when(p == 0)
            def _():
                arrival(zb, zb_recv, u).wait_recv()
                out[...] += zb[u]

            departure(l, u, True)

        def ahead(u, carry):
            input_sum(0, u)
            return carry

        def by_place(values):
            p = place[0]
            return jnp.where(p == 0, values[0], jnp.where(p == 1, values[1], jnp.where(p == 2, values[2], values[3])))

        first, lead = by_place(FIRST), by_place(AHEAD)

        def made(t):
            return jnp.minimum(steps, jnp.minimum(first + 2 * t, lead + t))

        lax.fori_loop(0, first, ahead, 0)

        def step(t, carry):
            lax.fori_loop(made(t), made(t + 1), ahead, 0)
            remote(h1in.at[t], h1in.at[t], h1_send.at[0], h1_recv.at[t], at(xx, 1 - cc)).wait_recv()
            input_sum(1, t)
            return carry

        lax.fori_loop(0, steps, step, 0)
        for l in range(2):
            for u in range(steps - 2, steps):
                departure(l, u, False)

    for l in range(2):
        @pl.when(jnp.logical_not(is_rec & (layer == l)))
        def _(l=l):
            small_copies(l, False)
            weight_copies(l, False)

    @pl.when(jnp.logical_not(is_input))
    def _():
        for cp in to_input:
            cp.wait_send()

    @pl.when(jnp.logical_not(is_rec & (layer == 0)))
    def _():
        remote(c1_out, c1_out, c_send.at[0], c_recv.at[0], at(xx, 1 - cc)).wait_recv()

    @pl.when(jnp.logical_not(is_rec & (layer == 1)))
    def _():
        remote(c2_out, c2_out, c_send.at[0], c_recv.at[1], at(xx, 1 - cc)).wait_recv()
        for n in range(n_out):
            rows = pl.ds(n * OUT_STEPS, OUT_STEPS)
            remote(h2_out.at[rows], h2_out.at[rows], o_send.at[0], o_recv.at[n], at(xx, 1 - cc)).wait_recv()


def solution(mesh):
    n_row, n_col = mesh.shape["row"], mesh.shape["col"]

    def gate_major(w, unit):
        rows = w.shape[0]
        w = w.reshape(rows, n_row // 4, 4, 4, unit).transpose(0, 1, 3, 2, 4)
        return w.reshape(rows, n_row * 4 * unit)

    def local_program(seq_in, w_in1, w_rec1, b_gate1, w_in2, w_rec2, b_gate2, h_init, c_init):
        steps, batch, k_rows = seq_in.shape
        unit = b_gate1.shape[0] // 4
        cols = w_in1.shape[1]
        col, row = lax.axis_index("col"), lax.axis_index("row")

        def by_owner(w):
            return gate_major(w, unit).reshape(n_col, unit, cols)

        bias = jnp.stack([b_gate1, b_gate2]).reshape(2, 1, 4, 1, unit)
        bias = lax.dynamic_update_slice(
            jnp.zeros((2, n_row // 4, 4, 4, unit), F32), bias, (0, row // 4, 0, row % 4, 0)).reshape(2, 1, cols)
        c_own = lax.dynamic_slice_in_dim(c_init, col * unit, unit, axis=2)
        c_pad = lax.dynamic_update_slice(jnp.zeros((2, batch, 2 * unit), F32), c_own, (0, 0, (row % 2) * unit))
        hid = n_row * unit

        hbm = pl.BlockSpec(memory_space=pl.ANY)
        dma = pltpu.SemaphoreType.DMA
        vm = pltpu.VMEM
        h2_pair, c1_pair, c2_pair = pl.pallas_call(
            functools.partial(lstm_kernel, n_row, n_col),
            out_shape=(
                jax.ShapeDtypeStruct((steps, batch, 2 * unit), BF16),
                jax.ShapeDtypeStruct((batch, 2 * unit), F32),
                jax.ShapeDtypeStruct((batch, 2 * unit), F32),
            ),
            in_specs=[hbm] * 8,
            out_specs=(hbm, hbm, hbm),
            scratch_shapes=[
                vm((n_col, n_row, unit, cols), BF16),
                vm((2, k_rows, cols), BF16),
                vm((n_col, 2, unit, cols), BF16),
                vm((2, steps, batch, k_rows), BF16),
                vm((2, 2, 1, cols), F32),
                vm((2, 1, cols), F32),
                vm((steps + 1, n_col, 2, batch, hid // 2), BF16),
                vm((steps, batch, cols), F32),
                vm((steps, batch, cols), F32),
                vm((steps, n_col, batch, 2 * unit), BF16),
                vm((2, 2, batch, cols), F32),
                vm((batch, cols), F32),
                vm((2, batch, hid // 2), F32),
                vm((n_row, batch, k_rows), BF16),
                vm((n_row, batch, 2 * unit), F32),
                dma((2,)), dma((n_row,)), dma((n_col,)), dma((n_col,)), dma((n_col,)),
                dma((4,)), dma((4,)), dma((4,)),
                dma((2, 2)), dma((n_row,)), dma((n_row,)),
                dma((2, n_col - 1, 2)), dma((2, n_col, 2)),
                dma((steps,)), dma((steps,)), dma((2, 2)),
                dma((n_row // 2,)), dma((steps,)),
                dma((n_row,)), dma((steps // OUT_STEPS,)),
                dma((n_row,)), dma((2,)),
            ],
            compiler_params=pltpu.CompilerParams(
                collective_id=0, has_side_effects=True, vmem_limit_bytes=60 * 2**20),
        )(
            by_owner(w_rec1), by_owner(w_rec2), gate_major(w_in1, unit), by_owner(w_in2),
            seq_in, bias, h_init.astype(BF16), c_pad,
        )

        def own_half(pair):
            return lax.dynamic_slice_in_dim(pair, (row % 2) * unit, unit, axis=pair.ndim - 1)

        return own_half(h2_pair), own_half(c1_pair), own_half(c2_pair)

    row_spec = P(None, "dp", "row")
    weight_spec = P("row", "col")
    bias_spec = P(("col", "row"))
    seq_out_spec = P(None, "dp", ("row", "col"))
    cell_out_spec = P("dp", ("row", "col"))
    return jax.shard_map(
        local_program,
        mesh=mesh,
        in_specs=(row_spec, weight_spec, weight_spec, bias_spec, weight_spec, weight_spec, bias_spec, row_spec, row_spec),
        out_specs=(seq_out_spec, cell_out_spec, cell_out_spec),
        check_vma=False,
    )
```

```python
import functools

import jax
import jax.numpy as jnp
from jax import lax
from jax.experimental import pallas as pl
from jax.experimental.pallas import tpu as pltpu
from jax.sharding import PartitionSpec as P


MESH = pl.DeviceIdType.MESH
F32, BF16 = jnp.float32, jnp.bfloat16
AHEAD = (6, 9, 13, 12)
FIRST = (4, 4, 13, 4)
EARLY = 4
MIDDLE = (3, 2)
H1_AHEAD = 3
OUT_STEPS = 2


def sigmoid(v):
    return 0.5 * jnp.tanh(0.5 * v) + 0.5


def lstm_kernel(
    n_row, n_col, wr1, wr2, wi1, wi2, x_in, b1, b2, h0, c0, h2_out, c1_out, c2_out,
    raw, perm, relay, wbuf, wi1b, wi2b, xb, bb, bias2, hist, za, zb, zc, zmid, h1in, zout, zpre, cst, hin, cin, hst, cstart, bst,
    raw_sem, w_send, w_recv, rel_recv, rel_send, in_send, in_recv, x_local, hc_send, hin_recv, cin_recv,
    hx_send, hx_recv, za_recv, zb_recv, zc_recv, z_send, zm_send, h1_send, h1_recv, o_send, o_recv, c_send, c_recv, passed,
):
    steps = x_in.shape[0]
    n_x = n_row // 2
    col, row = lax.axis_index("col"), lax.axis_index("row")
    xx, cc = row // 2, row % 2
    in_block = (xx < 2) == (col < 2)
    layer = xx // 2
    is_rec = in_block & (cc == 1)
    is_input = in_block == (cc == 0)
    not_input = jnp.logical_not(is_input)

    def at(x, c, y):
        return {"row": x * 2 + c, "col": y}

    def input_core(x, y):
        return jnp.where((x < 2) == (y < 2), 0, 1)

    def owner_at(l, k):
        away = (k + n_col - 2 * l) % n_col // 2
        return at(2 * l + away, 1, jnp.where(away == 0, k, n_col - 1 - k))

    def remote(src, dst, ssem, rsem, dev):
        return pltpu.make_async_remote_copy(
            src_ref=src, dst_ref=dst, send_sem=ssem, recv_sem=rsem, device_id=dev, device_id_type=MESH)

    me_else = at(xx, 1 - cc, col)

    loads = [pltpu.make_async_copy(w, raw.at[i], raw_sem.at[i]) for i, w in enumerate((wr1, wr2, wi1, wi2))]
    for load in loads:
        load.start()
    barrier = pltpu.get_barrier_semaphore()
    for dy in range(n_col):
        for dx in range(n_row):
            if dx or dy:
                pl.semaphore_signal(
                    barrier, inc=1, device_id={"row": (row + dx) % n_row, "col": (col + dy) % n_col}, device_id_type=MESH)

    lane_half = lax.broadcasted_iota(jnp.int32, (1, 128), 1) // 64

    def gate_major(i):
        for q in range(n_row // 2):
            for pair in range(2):
                left = raw[i, :, q * 512 + pair * 128:q * 512 + pair * 128 + 128]
                right = raw[i, :, q * 512 + 256 + pair * 128:q * 512 + 256 + pair * 128 + 128]
                to = (q // 2) * 1024 + pair * 512 + (q % 2) * 128
                low = jnp.concatenate([left[:, :64], right[:, :64]], axis=1)
                high = jnp.concatenate([left[:, 64:], right[:, 64:]], axis=1)
                perm[i, :, :, to:to + 128] = low.reshape(4, 64, 128)
                perm[i, :, :, to + 256:to + 384] = high.reshape(4, 64, 128)

    def to_half(tile, odd):
        moved = jnp.where(odd == row % 2, tile, pltpu.roll(tile, 64, 1))
        return jnp.where(lane_half == row % 2, moved, 0.0)

    for l in range(2):
        hst[l] = h0[l].astype(BF16)
        cells = jnp.where(col < 2, c0[l, :, :128], c0[l, :, 128:])
        cstart[l] = to_half(cells, col % 2)
        for m in range(4):
            gate = to_half((b1, b2)[l][:, (m // 2) * 128:(m // 2) * 128 + 128], m % 2)
            for half in range(2):
                for part in range(2):
                    cols = half * 1024 + m * 256 + part * 128
                    mine = (row // 4 == half) & (row % 4 // 2 == part)
                    bst[l, :, cols:cols + 128] = jnp.where(mine, gate, 0.0)
    for i in range(2):
        loads[i].wait()
        gate_major(i)
    pl.semaphore_wait(barrier, n_row * n_col - 1)

    def start_up(l, go):
        xr, kr = (xx + n_x - 2 * l) % n_x, (col + n_col - 2 * l) % n_col
        home = kr < 2
        other_row = n_col - 1 - col
        mine = home & (xr == 0) & (cc == 1)
        by_near = home & (xr == 2) & (cc == 0)
        by_far = jnp.logical_not(home) & (xr == 2)
        by_corner = jnp.logical_not(home) & ((xr == 3) | ((xr == 0) & (cc == 0)))
        relayed = by_near | by_far | by_corner
        rx = jnp.where(by_near, (2 * l + 1) % n_x, jnp.where(by_far, (2 * l + 2) % n_x, 2 * l))
        rdev = at(rx, jnp.where(by_far, 0, 1), jnp.where(by_near, col, other_row))
        slot = jnp.where(by_near, 0, jnp.where(by_far, cc, jnp.where(xr == 0, 0, 2 - cc)))
        owner = owner_at(l, col)
        small = [
            remote(hst.at[l], hin.at[row], hc_send.at[l, 0], hin_recv.at[row], owner),
            remote(cstart.at[l], cin.at[row], hc_send.at[l, 1], cin_recv.at[row], owner),
        ]
        direct = [remote(perm.at[l, j], wbuf.at[j, row], w_send.at[l, j], w_recv.at[row, j], owner) for j in range(n_col)]
        by_relay = [remote(perm.at[l, j], relay.at[slot, j], w_send.at[l, j], rel_recv.at[slot, j], rdev) for j in range(n_col)]

        @pl.when(jnp.logical_not(mine))
        def _():
            for cp in small:
                cp.start() if go else cp.wait_send()

        @pl.when(jnp.logical_not(mine | relayed))
        def _():
            for cp in direct:
                cp.start() if go else cp.wait_send()

        @pl.when(relayed)
        def _():
            for cp in by_relay:
                cp.start() if go else cp.wait_send()

        if go:
            @pl.when(mine)
            def _():
                wbuf[:, row] = perm[l]
                hin[row] = hst[l]
                cin[row] = cstart[l]

    for l in range(2):
        start_up(l, True)

    x_load = pltpu.make_async_copy(x_in, xb.at[cc], x_local.at[0])
    give = [
        remote(s, d, in_send.at[i], in_recv.at[i], me_else) for i, (s, d) in enumerate((
            (x_in, xb.at[cc]), (bst, bb.at[cc]), (perm.at[2], wi1b.at[cc]), (perm.at[3], wi2b.at[:, cc])))
    ]

    @pl.when(is_input)
    def _():
        x_load.start()
        bb[cc] = bst[...]

    @pl.when(not_input)
    def _():
        give[0].start()
        give[1].start()

    for i in (2, 3):
        loads[i].wait()
        gate_major(i)

        @pl.when(is_input)
        def _(i=i):
            if i == 2:
                wi1b[cc] = perm[2]
            else:
                wi2b[:, cc] = perm[3]

        @pl.when(not_input)
        def _(i=i):
            give[i].start()

    def pass_on(l, slots, sources, to_x):
        dev = at(to_x, 1, col)
        for group in slots:
            for j in range(n_col):
                for s in group:
                    remote(relay.at[s, j], relay.at[s, j], rel_send.at[s, j], rel_recv.at[s, j], dev).wait_recv()
                    remote(relay.at[s, j], wbuf.at[j, sources[s]], rel_send.at[s, j], w_recv.at[sources[s], j], dev).start()
        for group in slots:
            for j in range(n_col):
                for s in group:
                    remote(relay.at[s, j], wbuf.at[j, sources[s]], rel_send.at[s, j], w_recv.at[sources[s], j], dev).wait_send()

    for l in range(2):
        x0, x1, x2, x3 = [(2 * l + i) % n_x for i in range(4)]
        here = (col // 2) == l

        @pl.when(here & (cc == 1) & (xx == x0))
        def _(l=l, x0=x0, x1=x1, x3=x3):
            pass_on(l, ((1, 2), (0,)), (2 * x0, 2 * x3 + 1, 2 * x3), x1)

        @pl.when(here & (cc == 1) & (xx == x1))
        def _(l=l, x0=x0, x2=x2):
            pass_on(l, ((0,),), (2 * x2,), x0)

        @pl.when(here & (cc == 0) & (xx == x2))
        def _(l=l, x1=x1, x2=x2):
            pass_on(l, ((0, 1),), (2 * x2, 2 * x2 + 1), x1)
            if l == 0:
                pl.semaphore_signal(passed, inc=1, device_id=me_else, device_id_type=MESH)

    @pl.when(is_rec)
    def _():
        home = xx % 2 == 0
        own = jnp.where(home, col, n_col - 1 - col)
        last = (own + 2) % n_col

        def peer(d):
            k = (own + d) % n_col
            away = (k + n_col - 2 * layer) % n_col // 2
            return at(2 * layer + away, 1, jnp.where(away == 0, k, n_col - 1 - k))

        def h_copy(t, owner, d, par):
            ref = hist.at[t, owner]
            return remote(ref, ref, hx_send.at[par, d - 1], hx_recv.at[par, owner], peer(d))

        def product(t, owner, cols=slice(None)):
            w = wbuf[owner, :, :, cols].reshape(512, -1)
            return jnp.dot(hist[t, owner], w, preferred_element_type=F32)

        def z_arrives(t):
            remote(za.at[t], za.at[t], z_send.at[0, 0], za_recv.at[t], me_else).wait_recv()
            zpre[...] += za[t]

            @pl.when(home)
            def _():
                remote(zb.at[t], zb.at[t], z_send.at[0, 0], zb_recv.at[t], me_else).wait_recv()
                remote(zc.at[t], zc.at[t], z_send.at[0, 0], zc_recv.at[t], me_else).wait_recv()
                zpre[...] += zb[t] + zc[t]

        def forward(t, go):
            near = jnp.where(home, 0, 1), jnp.where(home, 3, 2)
            for i, (x, y) in enumerate(((near[1], col), (near[1], n_col - 1 - col), (near[0], n_col - 1 - col), (near[0], col))):
                src = hist.at[t + 1, :, :, pl.ds(pl.multiple_of(x * 128, 128), 128)]
                cp = remote(src, h1in.at[t], h1_send.at[i], h1_recv.at[t], at(x, int(i < 3), y))
                cp.start() if go else cp.wait_send()

        def hand_h1(t):
            return remote(h1in.at[t], h1in.at[t], h1_send.at[0], h1_recv.at[t], me_else)

        def middle(u, go):
            cp = remote(zmid.at[u % 2], zc.at[u], zm_send.at[u % 2], zc_recv.at[u], at(2 * layer, 1, col))
            if not go:
                cp.wait_send()
                return
            remote(zb.at[u], zb.at[u], z_send.at[0, 0], zb_recv.at[u], me_else).wait_recv()
            remote(zc.at[u], zc.at[u], z_send.at[0, 0], zc_recv.at[u], me_else).wait_recv()
            zmid[u % 2] = zb[u] + zc[u]
            cp.start()

        lead = jnp.where(layer == 0, MIDDLE[0], MIDDLE[1])

        def out_copy(src, dst, ssem, rsem, r, home_row, go):
            away = remote(src, dst, ssem, rsem, {"row": r, "col": own})
            if r != home_row:
                away.start() if go else away.wait_send()
                return
            local = pltpu.make_async_copy(src, dst, ssem)

            @pl.when(home)
            def _():
                local.start() if go else local.wait()

            @pl.when(jnp.logical_not(home))
            def _():
                away.start() if go else away.wait_send()

        def out_copies(n):
            rows = pl.ds(n * OUT_STEPS, OUT_STEPS)
            for r in range(n_row):
                src = hist.at[pl.ds(n * OUT_STEPS + 1, OUT_STEPS), own, :, pl.ds((r // 2) * 128, 128)]
                out_copy(src, h2_out.at[rows], o_send.at[r], o_recv.at[0], r, 5, True)

        def outs_sent():
            for r in range(n_row):
                out_copy(h2_out, h2_out, o_send.at[r], o_recv.at[0], r, 5, False)

        def c_copies(l, go):
            for r in range(n_row):
                x = r // 2
                src = cst.at[x // 2, :, pl.ds((x % 2) * 128, 128)]
                out_copy(src, (c1_out, c2_out)[l], c_send.at[r], c_recv.at[l], r, 4 * l + 1, go)

        for r in range(n_row):
            @pl.when(jnp.logical_not(home & (row == r)))
            def _(r=r):
                remote(hst.at[0], hin.at[r], hc_send.at[0, 0], hin_recv.at[r], me_else).wait_recv()
                remote(cstart.at[0], cin.at[r], hc_send.at[0, 1], cin_recv.at[r], me_else).wait_recv()
        for x in range(n_x):
            cst[x // 2, :, (x % 2) * 128:(x % 2) * 128 + 128] = cin[2 * x] + cin[2 * x + 1]
        hist[0, last] = jnp.zeros(hist.shape[2:], BF16)
        for r in range(n_row):
            @pl.when(jnp.logical_not(home & (row == r)))
            def _(r=r):
                for j in range(n_col):
                    remote(perm.at[0, j], wbuf.at[j, r], w_send.at[0, j], w_recv.at[r, j], me_else).wait_recv()

        start = jnp.dot(hin[0], wbuf[:, 0].reshape(256, 2048), preferred_element_type=F32)
        for r in range(1, n_row):
            start += jnp.dot(hin[r], wbuf[:, r].reshape(256, 2048), preferred_element_type=F32)
        zpre[...] = start

        @pl.when(layer == 1)
        def _():
            for u in range(H1_AHEAD):
                hand_h1(u).wait_recv()
                hand_h1(u).start()
                hand_h1(u).wait_send()

        @pl.when(jnp.logical_not(home))
        def _():
            for u in range(max(MIDDLE)):
                @pl.when(u < lead)
                def _(u=u):
                    if u >= 2:
                        middle(u - 2, False)
                    middle(u, True)

        z_arrives(0)

        def finish(t, send):
            par, par_before = t % 2, (t + 1) % 2

            @pl.when(t > 0)
            def _():
                h_copy(t, last, 2, par_before).wait_recv()

            z = []
            for g in range(8):
                cols = slice(g * 256, g * 256 + 256)
                z.append(product(t, last, cols) + zpre[:, cols])
            for half in range(2):
                i, f, g, o = z[half * 4:half * 4 + 4]
                c_new = sigmoid(f) * cst[half] + sigmoid(i) * jnp.tanh(g)
                cst[half] = c_new
                hist[t + 1, own, :, half * 256:half * 256 + 256] = (sigmoid(o) * jnp.tanh(c_new)).astype(BF16)
            if send:
                for d in (2, 1, 3):
                    h_copy(t + 1, own, d, par).start()

        def sent(t):
            for d in (2, 1, 3):
                h_copy(t + 1, own, d, t % 2).wait_send()

        def outputs(t):
            @pl.when((layer == 1) & (t % OUT_STEPS == OUT_STEPS - 1))
            def _():
                out_copies(t // OUT_STEPS)

        def step(t, carry):
            par = t % 2
            finish(t, True)
            zpre[...] = product(t + 1, own)
            u = t + lead

            @pl.when(jnp.logical_not(home) & (u < steps))
            def _():
                middle(u - 2, False)
                middle(u, True)

            @pl.when((layer == 1) & (t + H1_AHEAD < steps))
            def _():
                @pl.when(t > 0)
                def _():
                    hand_h1(t + H1_AHEAD).wait_send()

                hand_h1(t + H1_AHEAD).wait_recv()
                hand_h1(t + H1_AHEAD).start()

            z_arrives(t + 1)

            @pl.when((t > 1) & (layer == 0))
            def _():
                forward(t - 2, False)

            @pl.when((t > 0) & (layer == 0))
            def _():
                forward(t - 1, True)

            @pl.when(t > 0)
            def _():
                sent(t - 1)

            outputs(t)
            owners = [(own + d) % n_col for d in (1, 3)]
            for d, owner in zip((1, 3), owners):
                h_copy(t + 1, owner, d, par).wait_recv()
            zpre[...] += product(t + 1, owners[0]) + product(t + 1, owners[1])

            return carry

        lax.fori_loop(0, steps - 1, step, 0)
        end = steps - 1

        @pl.when(jnp.logical_not(home))
        def _():
            middle(steps - 2, False)
            middle(steps - 1, False)

        sent(end - 1)

        @pl.when(layer == 0)
        def _():
            forward(end - 2, False)
            finish(end, True)
            c_copies(0, True)
            forward(end - 1, True)
            forward(end - 1, False)
            for d in (1, 3, 2):
                h_copy(steps, (own + d) % n_col, d, end % 2).wait_recv()
            forward(end, True)
            forward(end, False)
            sent(end)
            c_copies(0, False)

        @pl.when(layer == 1)
        def _():
            hand_h1(0).wait_send()
            finish(end, False)
            outputs(end)
            c_copies(1, True)
            outs_sent()
            c_copies(1, False)

    @pl.when(is_input)
    def _():
        x_load.wait()
        for i, ref in enumerate((xb.at[1 - cc], bb.at[1 - cc], wi1b.at[1 - cc], wi2b.at[:, 1 - cc])):
            remote(ref, ref, in_send.at[i], in_recv.at[i], me_else).wait_recv()
        bias2[...] = bb[0] + bb[1]

        places, heads, middles, homes = [], [], [], []
        for l in range(2):
            xr, kr = (xx + n_x - 2 * l) % n_x, (col + n_col - 2 * l) % n_col
            places.append(jnp.where(kr < 2, xr, (1 + n_x - xr) % n_x))
            heads.append((2 * l + jnp.where(kr < 2, 0, 1)) % n_x)
            homes.append(kr < 2)
            middles.append((2 * l + jnp.where(kr < 2, 1, 0)) % n_x)

        def arrival(buf, sem, u):
            return remote(buf.at[u], buf.at[u], z_send.at[0, 0], sem.at[u], me_else)

        def departure(l, u, start):
            p, home = places[l], homes[l]
            src = zout.at[l, u % 2]
            dst_x = jnp.where(p == 2, middles[l], jnp.where(home & (p == 1), xx, heads[l]))
            on = at(dst_x, jnp.where(home, 1, input_core(dst_x, col)), col)
            owner = owner_at(l, col)
            dev = {axis: jnp.where(p == 0, owner[axis], on[axis]) for axis in ("row", "col")}
            ways = [remote(src, buf.at[u], z_send.at[l, u % 2], sem.at[u], dev)
                    for buf, sem in ((za, za_recv), (zb, zb_recv), (zc, zc_recv))]
            if not start:
                ways[0].wait_send()
                return
            to_c = home & (p == 1)
            to_b = (home & (p >= 2)) | (jnp.logical_not(home) & (p == 1))
            for way, here in zip(ways, (jnp.logical_not(to_b | to_c), to_b, to_c)):
                @pl.when(here)
                def _(way=way):
                    way.start()

        def input_sum(l, u):
            p = places[l]

            @pl.when(u >= 2)
            def _():
                departure(l, u - 2, False)

            if l == 0:
                part = jnp.dot(xb[0, u], wi1b[0].reshape(256, 2048), preferred_element_type=F32)
                part += jnp.dot(xb[1, u], wi1b[1].reshape(256, 2048), preferred_element_type=F32)
            else:
                h1 = jnp.concatenate([h1in[u, j] for j in range(n_col)], axis=1)
                part = jnp.dot(h1, wi2b[...].reshape(512, 2048), preferred_element_type=F32)
            out = zout.at[l, u % 2]
            out[...] = part + bias2[l]
            adds = jnp.logical_not(homes[l])

            @pl.when(adds & (p < 2))
            def _():
                arrival(za, za_recv, u).wait_recv()
                out[...] += za[u]

            @pl.when(adds & (p == 0))
            def _():
                arrival(zb, zb_recv, u).wait_recv()
                out[...] += zb[u]

            departure(l, u, True)

        def ahead(u, carry):
            input_sum(0, u)
            return carry

        def by_place(values):
            p = places[0]
            return jnp.where(p == 0, values[0], jnp.where(p == 1, values[1], jnp.where(p == 2, values[2], values[3])))

        first, lead = by_place(FIRST), by_place(AHEAD)

        def made(t):
            return jnp.minimum(steps, jnp.minimum(first + 2 * t, lead + t))

        early = jnp.minimum(made(0), EARLY)
        lax.fori_loop(0, early, ahead, 0)

        @pl.when((places[0] == 2) & (col < 2))
        def _():
            pl.semaphore_wait(passed, 1)

        lax.fori_loop(early, made(0), ahead, 0)

        def step(t, carry):
            lax.fori_loop(made(t), made(t + 1), ahead, 0)
            remote(h1in.at[t], h1in.at[t], h1_send.at[0], h1_recv.at[t], me_else).wait_recv()
            input_sum(1, t)
            return carry

        lax.fori_loop(0, steps, step, 0)
        for l in range(2):
            for u in range(steps - 2, steps):
                departure(l, u, False)

    for l in range(2):
        start_up(l, False)

    @pl.when(not_input)
    def _():
        for cp in give:
            cp.wait_send()

    keeps_own = is_rec & (xx % 2 == 0)
    for l, out in enumerate((c1_out, c2_out)):
        @pl.when(jnp.logical_not(keeps_own & (layer == l)))
        def _(l=l, out=out):
            remote(out, out, c_send.at[0], c_recv.at[l], me_else).wait_recv()

    @pl.when(jnp.logical_not(keeps_own & (layer == 1)))
    def _():
        remote(h2_out, h2_out, o_send.at[0], o_recv.at[0], me_else).wait_recv()


def solution(mesh):
    n_row, n_col = mesh.shape["row"], mesh.shape["col"]

    def local_program(seq_in, w_in1, w_rec1, b_gate1, w_in2, w_rec2, b_gate2, h_init, c_init):
        steps, batch, k_rows = seq_in.shape
        unit = b_gate1.shape[0] // 4
        cols = w_in1.shape[1]
        row = lax.axis_index("row")
        hid = n_row * unit

        hbm = pl.BlockSpec(memory_space=pl.ANY)
        near = pl.BlockSpec(memory_space=pltpu.VMEM)
        dma = pltpu.SemaphoreType.DMA
        vm = pltpu.VMEM
        h2_pair, c1_pair, c2_pair = pl.pallas_call(
            functools.partial(lstm_kernel, n_row, n_col),
            out_shape=(
                jax.ShapeDtypeStruct((steps, batch, 2 * unit), BF16),
                jax.ShapeDtypeStruct((batch, 2 * unit), F32),
                jax.ShapeDtypeStruct((batch, 2 * unit), F32),
            ),
            in_specs=[hbm] * 5 + [near] * 4,
            out_specs=(hbm, hbm, hbm),
            scratch_shapes=[
                vm((4, k_rows, cols), BF16),
                vm((4, n_col, unit, cols), BF16),
                vm((3, n_col, unit, cols), BF16),
                vm((n_col, n_row, unit, cols), BF16),
                vm((2, n_col, unit, cols), BF16),
                vm((n_col, 2, unit, cols), BF16),
                vm((2, steps, batch, k_rows), BF16),
                vm((2, 2, 1, cols), F32),
                vm((2, 1, cols), F32),
                vm((steps + 1, n_col, batch, hid), BF16),
                vm((steps, batch, cols), F32),
                vm((steps, batch, cols), F32),
                vm((steps, batch, cols), F32),
                vm((2, batch, cols), F32),
                vm((steps, n_col, batch, 2 * unit), BF16),
                vm((2, 2, batch, cols), F32),
                vm((batch, cols), F32),
                vm((2, batch, hid // 2), F32),
                vm((n_row, batch, k_rows), BF16),
                vm((n_row, batch, 2 * unit), F32),
                vm((2, batch, k_rows), BF16),
                vm((2, batch, 2 * unit), F32),
                vm((2, 1, cols), F32),
                dma((4,)), dma((2, n_col)), dma((n_row, n_col)), dma((3, n_col)), dma((3, n_col)),
                dma((4,)), dma((4,)), dma((1,)),
                dma((2, 2)), dma((n_row,)), dma((n_row,)),
                dma((2, n_col - 1)), dma((2, n_col)),
                dma((steps,)), dma((steps,)), dma((steps,)), dma((2, 2)), dma((2,)),
                dma((n_row // 2,)), dma((steps,)),
                dma((n_row,)), dma((1,)),
                dma((n_row,)), dma((2,)), pltpu.SemaphoreType.REGULAR,
            ],
            compiler_params=pltpu.CompilerParams(
                collective_id=0, has_side_effects=True, vmem_limit_bytes=60 * 2**20),
        )(
            w_rec1, w_rec2, w_in1, w_in2, seq_in, b_gate1.reshape(1, -1), b_gate2.reshape(1, -1), h_init, c_init,
        )

        def own_half(pair):
            return lax.dynamic_slice_in_dim(pair, (row % 2) * unit, unit, axis=pair.ndim - 1)

        return own_half(h2_pair), own_half(c1_pair), own_half(c2_pair)

    row_spec = P(None, "dp", "row")
    weight_spec = P("row", "col")
    bias_spec = P(("col", "row"))
    seq_out_spec = P(None, "dp", ("row", "col"))
    cell_out_spec = P("dp", ("row", "col"))
    return jax.shard_map(
        local_program,
        mesh=mesh,
        in_specs=(row_spec, weight_spec, weight_spec, bias_spec, weight_spec, weight_spec, bias_spec, row_spec, row_spec),
        out_specs=(seq_out_spec, cell_out_spec, cell_out_spec),
        check_vma=False,
    )
```

```python
import functools

import jax
import jax.numpy as jnp
from jax import lax
from jax.experimental import pallas as pl
from jax.experimental.pallas import tpu as pltpu
from jax.sharding import PartitionSpec as P


MESH = pl.DeviceIdType.MESH
F32, BF16 = jnp.float32, jnp.bfloat16
AHEAD = (6, 9, 13, 12)
FIRST = (4, 4, 13, 4)
EARLY = 4
MIDDLE = (3, 2)
H1_AHEAD = 3
OUT_STEPS = 2


def sigmoid(v):
    return 0.5 * jnp.tanh(0.5 * v) + 0.5


def lstm_kernel(
    n_row, n_col, wr1, wr2, wi1, wi2, x_in, b1, b2, h0, c0, h2_out, c1_out, c2_out,
    raw, perm, relay, wbuf, wi1b, wi2b, xb, bb, bias2, hist, za, zb, zc, zmid, h1in, zout, zpre, cst, hin, cin, hst, cstart, bst,
    raw_sem, w_send, w_recv, rel_recv, rel_send, in_send, in_recv, x_local, hc_send, hin_recv, cin_recv,
    hx_send, hx_recv, za_recv, zb_recv, zc_recv, z_send, zm_send, h1_send, h1_recv, o_send, o_recv, c_send, c_recv, passed,
):
    steps = x_in.shape[0]
    n_x = n_row // 2
    col, row = lax.axis_index("col"), lax.axis_index("row")
    xx, cc = row // 2, row % 2
    in_block = (xx < 2) == (col < 2)
    layer = xx // 2
    is_rec = in_block & (cc == 1)
    is_input = in_block == (cc == 0)
    not_input = jnp.logical_not(is_input)

    def at(x, c, y):
        return {"row": x * 2 + c, "col": y}

    def input_core(x, y):
        return jnp.where((x < 2) == (y < 2), 0, 1)

    def owner_at(l, k):
        away = (k + n_col - 2 * l) % n_col // 2
        return at(2 * l + away, 1, jnp.where(away == 0, k, n_col - 1 - k))

    def remote(src, dst, ssem, rsem, dev):
        return pltpu.make_async_remote_copy(
            src_ref=src, dst_ref=dst, send_sem=ssem, recv_sem=rsem, device_id=dev, device_id_type=MESH)

    me_else = at(xx, 1 - cc, col)

    def dots(pieces):
        sums = [jnp.dot(rows, weights, preferred_element_type=F32) for rows, weights in pieces]
        return functools.reduce(jnp.add, sums)

    def cols_of(tile):
        return slice(tile * 256, tile * 256 + 256)

    loads = [pltpu.make_async_copy(w, raw.at[i], raw_sem.at[i]) for i, w in enumerate((wr1, wr2, wi1, wi2))]
    for load in loads:
        load.start()
    barrier = pltpu.get_barrier_semaphore()
    for dy in range(n_col):
        for dx in range(n_row):
            if dx or dy:
                pl.semaphore_signal(
                    barrier, inc=1, device_id={"row": (row + dx) % n_row, "col": (col + dy) % n_col}, device_id_type=MESH)

    lane_half = lax.broadcasted_iota(jnp.int32, (1, 128), 1) // 64

    def gate_major(i):
        for q in range(n_row // 2):
            for pair in range(2):
                left = raw[i, :, q * 512 + pair * 128:q * 512 + pair * 128 + 128]
                right = raw[i, :, q * 512 + 256 + pair * 128:q * 512 + 256 + pair * 128 + 128]
                to = (q // 2) * 1024 + pair * 512 + (q % 2) * 128
                low = jnp.concatenate([left[:, :64], right[:, :64]], axis=1)
                high = jnp.concatenate([left[:, 64:], right[:, 64:]], axis=1)
                perm[i, :, :, to:to + 128] = low.reshape(4, 64, 128)
                perm[i, :, :, to + 256:to + 384] = high.reshape(4, 64, 128)

    def to_half(tile, odd):
        moved = jnp.where(odd == row % 2, tile, pltpu.roll(tile, 64, 1))
        return jnp.where(lane_half == row % 2, moved, 0.0)

    for l in range(2):
        hst[l] = h0[l].astype(BF16)
        cells = jnp.where(col < 2, c0[l, :, :128], c0[l, :, 128:])
        cstart[l] = to_half(cells, col % 2)
        for m in range(4):
            gate = to_half((b1, b2)[l][:, (m // 2) * 128:(m // 2) * 128 + 128], m % 2)
            for half in range(2):
                for part in range(2):
                    cols = half * 1024 + m * 256 + part * 128
                    mine = (row // 4 == half) & (row % 4 // 2 == part)
                    bst[l, :, cols:cols + 128] = jnp.where(mine, gate, 0.0)
    for i in range(2):
        loads[i].wait()
        gate_major(i)
    pl.semaphore_wait(barrier, n_row * n_col - 1)

    def start_up(l, go):
        xr, kr = (xx + n_x - 2 * l) % n_x, (col + n_col - 2 * l) % n_col
        home = kr < 2
        other_row = n_col - 1 - col
        mine = home & (xr == 0) & (cc == 1)
        by_near = home & (xr == 2) & (cc == 0)
        by_far = jnp.logical_not(home) & (xr == 2)
        by_corner = jnp.logical_not(home) & ((xr == 3) | ((xr == 0) & (cc == 0)))
        relayed = by_near | by_far | by_corner
        rx = jnp.where(by_near, (2 * l + 1) % n_x, jnp.where(by_far, (2 * l + 2) % n_x, 2 * l))
        rdev = at(rx, jnp.where(by_far, 0, 1), jnp.where(by_near, col, other_row))
        slot = jnp.where(by_near, 0, jnp.where(by_far, cc, jnp.where(xr == 0, 0, 2 - cc)))
        owner = owner_at(l, col)
        small = [
            remote(hst.at[l], hin.at[row], hc_send.at[l, 0], hin_recv.at[row], owner),
            remote(cstart.at[l], cin.at[row], hc_send.at[l, 1], cin_recv.at[row], owner),
        ]
        direct = [remote(perm.at[l, j], wbuf.at[j, row], w_send.at[l, j], w_recv.at[row, j], owner) for j in range(n_col)]
        by_relay = [remote(perm.at[l, j], relay.at[slot, j], w_send.at[l, j], rel_recv.at[slot, j], rdev) for j in range(n_col)]

        @pl.when(jnp.logical_not(mine))
        def _():
            for cp in small:
                cp.start() if go else cp.wait_send()

        @pl.when(jnp.logical_not(mine | relayed))
        def _():
            for cp in direct:
                cp.start() if go else cp.wait_send()

        @pl.when(relayed)
        def _():
            for cp in by_relay:
                cp.start() if go else cp.wait_send()

        if go:
            @pl.when(mine)
            def _():
                wbuf[:, row] = perm[l]
                hin[row] = hst[l]
                cin[row] = cstart[l]

    for l in range(2):
        start_up(l, True)

    x_load = pltpu.make_async_copy(x_in, xb.at[cc], x_local.at[0])
    give = [
        remote(s, d, in_send.at[i], in_recv.at[i], me_else) for i, (s, d) in enumerate((
            (x_in, xb.at[cc]), (bst, bb.at[cc]), (perm.at[2], wi1b.at[cc]), (perm.at[3], wi2b.at[:, cc])))
    ]

    @pl.when(is_input)
    def _():
        x_load.start()
        bb[cc] = bst[...]

    @pl.when(not_input)
    def _():
        give[0].start()
        give[1].start()

    for i in (2, 3):
        loads[i].wait()
        gate_major(i)

        @pl.when(is_input)
        def _(i=i):
            if i == 2:
                wi1b[cc] = perm[2]
            else:
                wi2b[:, cc] = perm[3]

        @pl.when(not_input)
        def _(i=i):
            give[i].start()

    def pass_on(l, slots, sources, to_x):
        dev = at(to_x, 1, col)
        for group in slots:
            for j in range(n_col):
                for s in group:
                    remote(relay.at[s, j], relay.at[s, j], rel_send.at[s, j], rel_recv.at[s, j], dev).wait_recv()
                    remote(relay.at[s, j], wbuf.at[j, sources[s]], rel_send.at[s, j], w_recv.at[sources[s], j], dev).start()
        for group in slots:
            for j in range(n_col):
                for s in group:
                    remote(relay.at[s, j], wbuf.at[j, sources[s]], rel_send.at[s, j], w_recv.at[sources[s], j], dev).wait_send()

    for l in range(2):
        x0, x1, x2, x3 = [(2 * l + i) % n_x for i in range(4)]
        here = (col // 2) == l

        @pl.when(here & (cc == 1) & (xx == x0))
        def _(l=l, x0=x0, x1=x1, x3=x3):
            pass_on(l, ((1, 2), (0,)), (2 * x0, 2 * x3 + 1, 2 * x3), x1)

        @pl.when(here & (cc == 1) & (xx == x1))
        def _(l=l, x0=x0, x2=x2):
            pass_on(l, ((0,),), (2 * x2,), x0)

        @pl.when(here & (cc == 0) & (xx == x2))
        def _(l=l, x1=x1, x2=x2):
            pass_on(l, ((0, 1),), (2 * x2, 2 * x2 + 1), x1)
            if l == 0:
                pl.semaphore_signal(passed, inc=1, device_id=me_else, device_id_type=MESH)

    @pl.when(is_rec)
    def _():
        home = xx % 2 == 0
        own = jnp.where(home, col, n_col - 1 - col)
        last = (own + 2) % n_col

        def peer(d):
            k = (own + d) % n_col
            away = (k + n_col - 2 * layer) % n_col // 2
            return at(2 * layer + away, 1, jnp.where(away == 0, k, n_col - 1 - k))

        def h_copy(t, owner, half, d, par):
            ref = hist.at[t, owner, half]
            return remote(ref, ref, hx_send.at[par, d - 1, half], hx_recv.at[par, owner, half], peer(d))

        def products(t, pieces, cols=slice(None)):
            return dots([
                (hist[t, owner, half], wbuf[owner, half * 4:half * 4 + 4, :, cols].reshape(256, -1)) for owner, half in pieces])

        def z_arrives(t):
            remote(za.at[t], za.at[t], z_send.at[0, 0], za_recv.at[t], me_else).wait_recv()
            zpre[...] += za[t]

            @pl.when(home)
            def _():
                remote(zb.at[t], zb.at[t], z_send.at[0, 0], zb_recv.at[t], me_else).wait_recv()
                remote(zc.at[t], zc.at[t], z_send.at[0, 0], zc_recv.at[t], me_else).wait_recv()
                zpre[...] += zb[t] + zc[t]

        def forward(t, go):
            near = jnp.where(home, 0, 1), jnp.where(home, 3, 2)
            for i, (x, y) in enumerate(((near[1], col), (near[1], n_col - 1 - col), (near[0], n_col - 1 - col), (near[0], col))):
                src = hist.at[t + 1, :, x // 2, :, pl.ds(pl.multiple_of(x % 2 * 128, 128), 128)]
                cp = remote(src, h1in.at[t], h1_send.at[i], h1_recv.at[t], at(x, int(i < 3), y))
                cp.start() if go else cp.wait_send()

        def hand_h1(t):
            return remote(h1in.at[t], h1in.at[t], h1_send.at[0], h1_recv.at[t], me_else)

        def middle(u, go):
            cp = remote(zmid.at[u % 2], zc.at[u], zm_send.at[u % 2], zc_recv.at[u], at(2 * layer, 1, col))
            if not go:
                cp.wait_send()
                return
            remote(zb.at[u], zb.at[u], z_send.at[0, 0], zb_recv.at[u], me_else).wait_recv()
            remote(zc.at[u], zc.at[u], z_send.at[0, 0], zc_recv.at[u], me_else).wait_recv()
            zmid[u % 2] = zb[u] + zc[u]
            cp.start()

        lead = jnp.where(layer == 0, MIDDLE[0], MIDDLE[1])

        def out_copy(src, dst, ssem, rsem, r, home_row, go):
            away = remote(src, dst, ssem, rsem, {"row": r, "col": own})
            if r != home_row:
                away.start() if go else away.wait_send()
                return
            local = pltpu.make_async_copy(src, dst, ssem)

            @pl.when(home)
            def _():
                local.start() if go else local.wait()

            @pl.when(jnp.logical_not(home))
            def _():
                away.start() if go else away.wait_send()

        def out_copies(n):
            rows = pl.ds(n * OUT_STEPS, OUT_STEPS)
            for r in range(n_row):
                src = hist.at[pl.ds(n * OUT_STEPS + 1, OUT_STEPS), own, r // 4, :, pl.ds(r // 2 % 2 * 128, 128)]
                out_copy(src, h2_out.at[rows], o_send.at[r], o_recv.at[0], r, 5, True)

        def outs_sent():
            for r in range(n_row):
                out_copy(h2_out, h2_out, o_send.at[r], o_recv.at[0], r, 5, False)

        def c_copies(l, go):
            for r in range(n_row):
                x = r // 2
                src = cst.at[x // 2, :, pl.ds((x % 2) * 128, 128)]
                out_copy(src, (c1_out, c2_out)[l], c_send.at[r], c_recv.at[l], r, 4 * l + 1, go)

        for r in range(n_row):
            @pl.when(jnp.logical_not(home & (row == r)))
            def _(r=r):
                remote(hst.at[0], hin.at[r], hc_send.at[0, 0], hin_recv.at[r], me_else).wait_recv()
                remote(cstart.at[0], cin.at[r], hc_send.at[0, 1], cin_recv.at[r], me_else).wait_recv()
        for x in range(n_x):
            cst[x // 2, :, (x % 2) * 128:(x % 2) * 128 + 128] = cin[2 * x] + cin[2 * x + 1]
        hist[0, last] = jnp.zeros(hist.shape[2:], BF16)
        for r in range(n_row):
            @pl.when(jnp.logical_not(home & (row == r)))
            def _(r=r):
                for j in range(n_col):
                    remote(perm.at[0, j], wbuf.at[j, r], w_send.at[0, j], w_recv.at[r, j], me_else).wait_recv()

        @pl.when(layer == 1)
        def _():
            for u in range(H1_AHEAD):
                hand_h1(u).wait_recv()
                hand_h1(u).start()
                hand_h1(u).wait_send()

        @pl.when(jnp.logical_not(home))
        def _():
            for u in range(max(MIDDLE)):
                @pl.when(u < lead)
                def _(u=u):
                    if u >= 2:
                        middle(u - 2, False)
                    middle(u, True)

        zpre[...] = dots([(hin[r], wbuf[:, r].reshape(256, -1)) for r in range(n_row)])
        z_arrives(0)

        def finish(t, send):
            par, par_before = t % 2, (t + 1) % 2

            @pl.when(t > 0)
            def _():
                h_copy(t, last, 0, 2, par_before).wait_recv()
                h_copy(t, last, 1, 2, par_before).wait_recv()

            z = [products(t, ((last, 0), (last, 1)), cols_of(tile)) + zpre[:, cols_of(tile)] for tile in range(8)]
            for half in range(2):
                i, f, g, o = z[half * 4:half * 4 + 4]
                c_new = sigmoid(f) * cst[half] + sigmoid(i) * jnp.tanh(g)
                cst[half] = c_new
                hist[t + 1, own, half] = (sigmoid(o) * jnp.tanh(c_new)).astype(BF16)
                if send:
                    for d in (1, 3, 2):
                        h_copy(t + 1, own, half, d, par).start()

        def sent(t):
            for half in range(2):
                for d in (1, 3, 2):
                    h_copy(t + 1, own, half, d, t % 2).wait_send()

        def outputs(t):
            @pl.when((layer == 1) & (t % OUT_STEPS == OUT_STEPS - 1))
            def _():
                out_copies(t // OUT_STEPS)

        def step(t, carry):
            par = t % 2
            finish(t, True)
            beside, across = (own + 1) % n_col, (own + 3) % n_col
            zpre[...] = products(t + 1, ((own, 0), (own, 1)))
            u = t + lead

            @pl.when(jnp.logical_not(home) & (u < steps))
            def _():
                middle(u - 2, False)
                middle(u, True)

            @pl.when((layer == 1) & (t + H1_AHEAD < steps))
            def _():
                @pl.when(t > 0)
                def _():
                    hand_h1(t + H1_AHEAD).wait_send()

                hand_h1(t + H1_AHEAD).wait_recv()
                hand_h1(t + H1_AHEAD).start()

            z_arrives(t + 1)

            @pl.when((t > 1) & (layer == 0))
            def _():
                forward(t - 2, False)

            @pl.when((t > 0) & (layer == 0))
            def _():
                forward(t - 1, True)

            @pl.when(t > 0)
            def _():
                sent(t - 1)

            outputs(t)
            for half in range(2):
                h_copy(t + 1, beside, half, 1, par).wait_recv()
                h_copy(t + 1, across, half, 3, par).wait_recv()
                zpre[...] += products(t + 1, ((beside, half), (across, half)))

            return carry

        lax.fori_loop(0, steps - 1, step, 0)
        end = steps - 1

        @pl.when(jnp.logical_not(home))
        def _():
            middle(steps - 2, False)
            middle(steps - 1, False)

        sent(end - 1)

        @pl.when(layer == 0)
        def _():
            forward(end - 2, False)
            finish(end, True)
            c_copies(0, True)
            forward(end - 1, True)
            forward(end - 1, False)
            for d in (1, 3, 2):
                for half in range(2):
                    h_copy(steps, (own + d) % n_col, half, d, end % 2).wait_recv()
            forward(end, True)
            forward(end, False)
            sent(end)
            c_copies(0, False)

        @pl.when(layer == 1)
        def _():
            hand_h1(0).wait_send()
            finish(end, False)
            outputs(end)
            c_copies(1, True)
            outs_sent()
            c_copies(1, False)

    @pl.when(is_input)
    def _():
        x_load.wait()
        for i, ref in enumerate((xb.at[1 - cc], bb.at[1 - cc], wi1b.at[1 - cc], wi2b.at[:, 1 - cc])):
            remote(ref, ref, in_send.at[i], in_recv.at[i], me_else).wait_recv()
        bias2[...] = bb[0] + bb[1]

        places, heads, middles, homes = [], [], [], []
        for l in range(2):
            xr, kr = (xx + n_x - 2 * l) % n_x, (col + n_col - 2 * l) % n_col
            places.append(jnp.where(kr < 2, xr, (1 + n_x - xr) % n_x))
            heads.append((2 * l + jnp.where(kr < 2, 0, 1)) % n_x)
            homes.append(kr < 2)
            middles.append((2 * l + jnp.where(kr < 2, 1, 0)) % n_x)

        def arrival(buf, sem, u):
            return remote(buf.at[u], buf.at[u], z_send.at[0, 0], sem.at[u], me_else)

        def departure(l, u, start):
            p, home = places[l], homes[l]
            src = zout.at[l, u % 2]
            dst_x = jnp.where(p == 2, middles[l], jnp.where(home & (p == 1), xx, heads[l]))
            on = at(dst_x, jnp.where(home, 1, input_core(dst_x, col)), col)
            owner = owner_at(l, col)
            dev = {axis: jnp.where(p == 0, owner[axis], on[axis]) for axis in ("row", "col")}
            ways = [remote(src, buf.at[u], z_send.at[l, u % 2], sem.at[u], dev)
                    for buf, sem in ((za, za_recv), (zb, zb_recv), (zc, zc_recv))]
            if not start:
                ways[0].wait_send()
                return
            to_c = home & (p == 1)
            to_b = (home & (p >= 2)) | (jnp.logical_not(home) & (p == 1))
            for way, here in zip(ways, (jnp.logical_not(to_b | to_c), to_b, to_c)):
                @pl.when(here)
                def _(way=way):
                    way.start()

        def input_sum(l, u):
            p = places[l]

            @pl.when(u >= 2)
            def _():
                departure(l, u - 2, False)

            if l == 0:
                part = dots([(xb[i, u], wi1b[i].reshape(256, -1)) for i in range(2)])
            else:
                h1 = jnp.concatenate([h1in[u, j] for j in range(n_col)], axis=1)
                part = dots([(h1, wi2b[...].reshape(512, -1))])
            out = zout.at[l, u % 2]
            out[...] = part + bias2[l]

            adds = jnp.logical_not(homes[l])

            @pl.when(adds & (p < 2))
            def _():
                arrival(za, za_recv, u).wait_recv()
                out[...] += za[u]

            @pl.when(adds & (p == 0))
            def _():
                arrival(zb, zb_recv, u).wait_recv()
                out[...] += zb[u]

            departure(l, u, True)

        def ahead(u, carry):
            input_sum(0, u)
            return carry

        def by_place(values):
            p = places[0]
            return jnp.where(p == 0, values[0], jnp.where(p == 1, values[1], jnp.where(p == 2, values[2], values[3])))

        first, lead = by_place(FIRST), by_place(AHEAD)

        def made(t):
            return jnp.minimum(steps, jnp.minimum(first + 2 * t, lead + t))

        early = jnp.minimum(made(0), EARLY)
        lax.fori_loop(0, early, ahead, 0)

        @pl.when((places[0] == 2) & (col < 2))
        def _():
            pl.semaphore_wait(passed, 1)

        lax.fori_loop(early, made(0), ahead, 0)

        def step(t, carry):
            lax.fori_loop(made(t), made(t + 1), ahead, 0)
            remote(h1in.at[t], h1in.at[t], h1_send.at[0], h1_recv.at[t], me_else).wait_recv()
            input_sum(1, t)
            return carry

        lax.fori_loop(0, steps, step, 0)
        for l in range(2):
            for u in range(steps - 2, steps):
                departure(l, u, False)

    for l in range(2):
        start_up(l, False)

    @pl.when(not_input)
    def _():
        for cp in give:
            cp.wait_send()

    keeps_own = is_rec & (xx % 2 == 0)
    for l, out in enumerate((c1_out, c2_out)):
        @pl.when(jnp.logical_not(keeps_own & (layer == l)))
        def _(l=l, out=out):
            remote(out, out, c_send.at[0], c_recv.at[l], me_else).wait_recv()

    @pl.when(jnp.logical_not(keeps_own & (layer == 1)))
    def _():
        remote(h2_out, h2_out, o_send.at[0], o_recv.at[0], me_else).wait_recv()


def solution(mesh):
    n_row, n_col = mesh.shape["row"], mesh.shape["col"]

    def local_program(seq_in, w_in1, w_rec1, b_gate1, w_in2, w_rec2, b_gate2, h_init, c_init):
        steps, batch, k_rows = seq_in.shape
        unit = b_gate1.shape[0] // 4
        cols = w_in1.shape[1]
        row = lax.axis_index("row")
        hid = n_row * unit

        hbm = pl.BlockSpec(memory_space=pl.ANY)
        near = pl.BlockSpec(memory_space=pltpu.VMEM)
        dma = pltpu.SemaphoreType.DMA
        vm = pltpu.VMEM
        h2_pair, c1_pair, c2_pair = pl.pallas_call(
            functools.partial(lstm_kernel, n_row, n_col),
            out_shape=(
                jax.ShapeDtypeStruct((steps, batch, 2 * unit), BF16),
                jax.ShapeDtypeStruct((batch, 2 * unit), F32),
                jax.ShapeDtypeStruct((batch, 2 * unit), F32),
            ),
            in_specs=[hbm] * 5 + [near] * 4,
            out_specs=(hbm, hbm, hbm),
            scratch_shapes=[
                vm((4, k_rows, cols), BF16),
                vm((4, n_col, unit, cols), BF16),
                vm((3, n_col, unit, cols), BF16),
                vm((n_col, n_row, unit, cols), BF16),
                vm((2, n_col, unit, cols), BF16),
                vm((n_col, 2, unit, cols), BF16),
                vm((2, steps, batch, k_rows), BF16),
                vm((2, 2, 1, cols), F32),
                vm((2, 1, cols), F32),
                vm((steps + 1, n_col, 2, batch, hid // 2), BF16),
                vm((steps, batch, cols), F32),
                vm((steps, batch, cols), F32),
                vm((steps, batch, cols), F32),
                vm((2, batch, cols), F32),
                vm((steps, n_col, batch, 2 * unit), BF16),
                vm((2, 2, batch, cols), F32),
                vm((batch, cols), F32),
                vm((2, batch, hid // 2), F32),
                vm((n_row, batch, k_rows), BF16),
                vm((n_row, batch, 2 * unit), F32),
                vm((2, batch, k_rows), BF16),
                vm((2, batch, 2 * unit), F32),
                vm((2, 1, cols), F32),
                dma((4,)), dma((2, n_col)), dma((n_row, n_col)), dma((3, n_col)), dma((3, n_col)),
                dma((4,)), dma((4,)), dma((1,)),
                dma((2, 2)), dma((n_row,)), dma((n_row,)),
                dma((2, n_col - 1, 2)), dma((2, n_col, 2)),
                dma((steps,)), dma((steps,)), dma((steps,)), dma((2, 2)), dma((2,)),
                dma((n_row // 2,)), dma((steps,)),
                dma((n_row,)), dma((1,)),
                dma((n_row,)), dma((2,)), pltpu.SemaphoreType.REGULAR,
            ],
            compiler_params=pltpu.CompilerParams(
                collective_id=0, has_side_effects=True, vmem_limit_bytes=60 * 2**20),
        )(
            w_rec1, w_rec2, w_in1, w_in2, seq_in, b_gate1.reshape(1, -1), b_gate2.reshape(1, -1), h_init, c_init,
        )

        def own_half(pair):
            return lax.dynamic_slice_in_dim(pair, (row % 2) * unit, unit, axis=pair.ndim - 1)

        return own_half(h2_pair), own_half(c1_pair), own_half(c2_pair)

    row_spec = P(None, "dp", "row")
    weight_spec = P("row", "col")
    bias_spec = P(("col", "row"))
    seq_out_spec = P(None, "dp", ("row", "col"))
    cell_out_spec = P("dp", ("row", "col"))
    return jax.shard_map(
        local_program,
        mesh=mesh,
        in_specs=(row_spec, weight_spec, weight_spec, bias_spec, weight_spec, weight_spec, bias_spec, row_spec, row_spec),
        out_specs=(seq_out_spec, cell_out_spec, cell_out_spec),
        check_vma=False,
    )
```

```python
import functools

import jax
import jax.numpy as jnp
from jax import lax
from jax.experimental import pallas as pl
from jax.experimental.pallas import tpu as pltpu
from jax.sharding import PartitionSpec as P


MESH = pl.DeviceIdType.MESH
F32, BF16 = jnp.float32, jnp.bfloat16
HALVES = LAYERS = (0, 1)
GATES = 4
LANES, TILE, PAIR, OWN = 128, 256, 512, 1024
HALF_LANES = 64
CHUNK = 32
HELD = 2
AHEAD = (5, 8, 12, 8)
FIRST = (4, 4, 7, 6)
EARLY = 4
MIDDLE = (3, 2)
H1_AHEAD = 3
RING = 32
OUT_STEPS = 2
LATE = 8
PEERS = (1, 3, 2)


def sigmoid(v):
    return 0.5 * jnp.tanh(0.5 * v) + 0.5


def lstm_kernel(
    n_row, n_col, wr1, wr2, wi1, wi2, x_in, b1, b2, h0, c0, h2_out, c1_out, c2_out,
    raw, perm, relay, wbuf, wi1b, wi2b, xb, bb, bias2, init, hist, za, zb, zc, zmid, h1in, zout, zpre, cst, cin, cstart, bst,
    raw_sem, w_send, w_recv, rel_recv, rel_send, in_send, in_recv, x_local, c0_send, cin_recv,
    hx_send, hx_recv, za_recv, zb_recv, zc_recv, z_send, zm_send, h1_send, h1_recv, o_send, o_recv, c_send, c_recv, passed,
):
    steps = x_in.shape[0]
    n_x = n_row // 2
    n_part = raw.shape[1] // CHUNK
    per_col = n_part // n_col
    col, row = lax.axis_index("col"), lax.axis_index("row")
    xx, cc = row // 2, row % 2
    in_block = (xx < 2) == (col < 2)
    layer = xx // 2
    is_rec = in_block & (cc == 1)
    is_input = in_block == (cc == 0)
    not_input = jnp.logical_not(is_input)
    other_row = n_col - 1 - col

    def at(x, c, y):
        return {"row": x * 2 + c, "col": y}

    def input_core(x, y):
        return jnp.where((x < 2) == (y < 2), 0, 1)

    def is_away(l, k):
        return (k + n_col - 2 * l) % n_col // 2

    def owner_at(l, k):
        away = is_away(l, k)
        return at(2 * l + away, 1, jnp.where(away == 0, k, n_col - 1 - k))

    def remote(src, dst, ssem, rsem, dev):
        return pltpu.make_async_remote_copy(
            src_ref=src, dst_ref=dst, send_sem=ssem, recv_sem=rsem, device_id=dev, device_id_type=MESH)

    me_else = at(xx, 1 - cc, col)

    def arrived(ref, sem):
        remote(ref, ref, x_local.at[0], sem, me_else).wait_recv()

    def run(copies, go):
        for cp in copies:
            cp.start() if go else cp.wait_send()

    def dots(pieces):
        sums = [jnp.dot(rows, weights, preferred_element_type=F32) for rows, weights in pieces]
        return functools.reduce(jnp.add, sums)

    def cols_of(tile):
        return slice(tile * TILE, tile * TILE + TILE)

    loads = [pltpu.make_async_copy(w, raw.at[i], raw_sem.at[i]) for i, w in enumerate((wr1, wr2, wi1, wi2))]
    for load in loads:
        load.start()
    barrier = pltpu.get_barrier_semaphore()
    for dy in range(n_col):
        for dx in range(n_row):
            if dx or dy:
                pl.semaphore_signal(
                    barrier, inc=1, device_id={"row": (row + dx) % n_row, "col": (col + dy) % n_col}, device_id_type=MESH)

    lane_half = lax.broadcasted_iota(jnp.int32, (1, LANES), 1) // HALF_LANES

    def gate_major(i):
        for q in range(n_x):
            for pair in HALVES:
                at_left = q * PAIR + pair * LANES
                left, right = raw[i, :, at_left:at_left + LANES], raw[i, :, at_left + TILE:at_left + TILE + LANES]
                to = q // 2 * OWN + pair * PAIR + q % 2 * LANES
                low = jnp.concatenate([left[:, :HALF_LANES], right[:, :HALF_LANES]], axis=1)
                high = jnp.concatenate([left[:, HALF_LANES:], right[:, HALF_LANES:]], axis=1)
                for part, start in ((low, to), (high, to + TILE)):
                    perm[i, :, :, start:start + LANES] = part.reshape(n_col, -1, LANES)

    def to_half(tile, odd):
        moved = jnp.where(odd == row % 2, tile, pltpu.roll(tile, HALF_LANES, 1))
        return jnp.where(lane_half == row % 2, moved, 0.0)

    for l in LAYERS:
        cells = jnp.where(col < 2, c0[l, :, :LANES], c0[l, :, LANES:])
        cstart[l] = to_half(cells, col % 2)
        for m in range(GATES):
            start = m // 2 * LANES
            gate = to_half((b1, b2)[l][:, start:start + LANES], m % 2)
            for half in HALVES:
                for part in HALVES:
                    start = half * OWN + m * TILE + part * LANES
                    mine = (row // 4 == half) & (row % 4 // 2 == part)
                    bst[l, :, start:start + LANES] = jnp.where(mine, gate, 0.0)
    for l in LAYERS:
        loads[l].wait()
        gate_major(l)
    pl.semaphore_wait(barrier, n_row * n_col - 1)

    def part_of(ref, c):
        return ref.at[c // per_col, pl.ds(c % per_col * CHUNK, CHUNK)]

    def start_up(l, go, chunks):
        xr, kr = (xx + n_x - 2 * l) % n_x, (col + n_col - 2 * l) % n_col
        home = kr < 2
        mine = home & (xr == 0) & (cc == 1)
        by_near = home & (xr == 2) & (cc == 0)
        by_far = jnp.logical_not(home) & (xr == 2)
        by_corner = jnp.logical_not(home) & ((xr == 3) | ((xr == 0) & (cc == 0)))
        relayed = by_near | by_far | by_corner
        rx = jnp.where(by_near, (2 * l + 1) % n_x, jnp.where(by_far, (2 * l + 2) % n_x, 2 * l))
        rdev = at(rx, jnp.where(by_far, 0, 1), jnp.where(by_near, col, other_row))
        slot = jnp.where(by_near, 0, jnp.where(by_far, cc, jnp.where(xr == 0, 0, 2 - cc)))
        owner = owner_at(l, col)
        cells = [remote(cstart.at[l], cin.at[row], c0_send.at[l], cin_recv.at[row], owner)]
        direct, by_relay = [], []
        for c in chunks:
            src = part_of(perm.at[l], c)
            direct.append(remote(src, part_of(wbuf.at[:, row], c), w_send.at[l], w_recv.at[row], owner))
            by_relay.append(remote(src, part_of(relay.at[slot], c), w_send.at[l], rel_recv.at[slot, c], rdev))
        if not go:
            direct = by_relay = [remote(perm.at[l], perm.at[l], w_send.at[l], w_recv.at[row], owner)]
        if chunks[0] == 0:
            @pl.when(jnp.logical_not(mine))
            def _():
                run(cells, go)

            if go:
                @pl.when(mine)
                def _():
                    wbuf[:, row] = perm[l]
                    cin[row] = cstart[l]

        @pl.when(jnp.logical_not(mine | relayed))
        def _():
            run(direct, go)

        @pl.when(relayed)
        def _():
            run(by_relay, go)

    all_chunks = range(n_part)
    held = all_chunks[n_part - HELD:]
    for l in LAYERS:
        start_up(l, True, all_chunks[:n_part - HELD])

    @pl.when(not_input)
    def _():
        for l in LAYERS:
            start_up(l, True, held)

    for l in LAYERS:
        init[cc, l] = jnp.dot(h0[l].astype(BF16), perm[l].reshape(-1, perm.shape[-1]), preferred_element_type=F32)
    x_load = pltpu.make_async_copy(x_in, xb.at[cc], x_local.at[0])
    give = [remote(s, d, in_send.at[i], in_recv.at[i], me_else) for i, (s, d) in enumerate((
        (x_in, xb.at[cc]), (bst, bb.at[cc]), (init.at[cc], init.at[cc]), (perm.at[2], wi1b.at[cc]), (perm.at[3], wi2b.at[:, cc])))]
    soon = len(give) - 2

    @pl.when(is_input)
    def _():
        x_load.start()
        bb[cc] = bst[...]

    @pl.when(not_input)
    def _():
        run(give[:soon], True)

    for l in LAYERS:
        loads[2 + l].wait()
        gate_major(2 + l)

        @pl.when(is_input)
        def _(l=l):
            (wi1b.at[cc], wi2b.at[:, cc])[l][...] = perm[2 + l]

        @pl.when(not_input)
        def _(l=l):
            give[soon + l].start()

    def pass_on(slots, sources, to_x):
        dev = at(to_x, 1, col)

        def onward(s, c):
            return remote(part_of(relay.at[s], c), part_of(wbuf.at[:, sources[s]], c), rel_send.at[s],
                          w_recv.at[sources[s]], dev)

        for group in slots:
            for c in all_chunks:
                for s in group:
                    arrived(part_of(relay.at[s], c), rel_recv.at[s, c])
                    onward(s, c).start()

        def done():
            for group in slots:
                for s in group:
                    remote(relay.at[s], relay.at[s], rel_send.at[s], rel_recv.at[s, 0], dev).wait_send()

        return done

    def relays(then):
        for l in LAYERS:
            x0, x1, x2, x3 = [(2 * l + i) % n_x for i in range(n_x)]
            here = (col // 2) == l
            for core, x, args in (
                (1, x0, (((1, 2), (0,)), (2 * x0, 2 * x3 + 1, 2 * x3), x1)),
                (1, x1, (((0,),), (2 * x2,), x0)),
                (0, x2, (((0, 1),), (2 * x2, 2 * x2 + 1), x1)),
            ):
                yield l, core, here & (cc == core) & (xx == x), args

    for l, core, mine, args in relays(None):
        @pl.when(mine)
        def _(l=l, core=core, args=args):
            done = pass_on(*args)
            if core == 0:
                done()
                if l == 0:
                    pl.semaphore_signal(passed.at[0], inc=1, device_id=me_else, device_id_type=MESH)

    @pl.when(is_rec)
    def _():
        home = xx % 2 == 0
        own = jnp.where(home, col, other_row)
        beside, across, last = [(own + d) % n_col for d in PEERS]

        def peer(d):
            k = (own + d) % n_col
            away = is_away(layer, k)
            return at(2 * layer + away, 1, jnp.where(away == 0, k, n_col - 1 - k))

        def h_copy(t, owner, half, d):
            ref = hist.at[t + 1, owner, half]
            return remote(ref, ref, hx_send.at[t % 2, d - 1, half], hx_recv.at[t % 2, owner, half], peer(d))

        def products(t, pieces, cols=slice(None)):
            return dots([(hist[t + 1, owner, half], wbuf[owner, half * GATES:half * GATES + GATES, :, cols].reshape(TILE, -1))
                         for owner, half in pieces])

        def z_arrives(t):
            arrived(za.at[t], za_recv.at[t % RING])
            zpre[...] += za[t]

            @pl.when(home)
            def _():
                arrived(zb.at[t], zb_recv.at[t % RING])
                arrived(zc.at[t], zc_recv.at[t % RING])
                zpre[...] += zb[t] + zc[t]

        def forward(t, go):
            near, far = jnp.where(home, 0, 1), jnp.where(home, 3, 2)
            for i, (x, c, y) in enumerate(((far, 1, col), (far, 1, other_row), (near, 1, other_row), (near, 0, col))):
                src = hist.at[t + 1, :, x // 2, :, pl.ds(pl.multiple_of(x % 2 * LANES, LANES), LANES)]
                run([remote(src, h1in.at[t], h1_send.at[i], h1_recv.at[t % RING], at(x, c, y))], go)

        def hand_h1(t):
            return remote(h1in.at[t], h1in.at[t], h1_send.at[0], h1_recv.at[t % RING], me_else)

        def middle(u, go):
            cp = remote(zmid.at[u % 2], zc.at[u], zm_send.at[u % 2], zc_recv.at[u % RING], at(2 * layer, 1, col))
            if go:
                arrived(zb.at[u], zb_recv.at[u % RING])
                arrived(zc.at[u], zc_recv.at[u % RING])
                zmid[u % 2] = zb[u] + zc[u]
            run([cp], go)

        lead = jnp.where(layer == 0, MIDDLE[0], MIDDLE[1])

        def out_copy(src, dst, ssem, rsem, r, home_row, go):
            away = remote(src, dst, ssem, rsem, {"row": r, "col": own})
            if r != home_row:
                run([away], go)
                return
            local = pltpu.make_async_copy(src, dst, ssem)

            @pl.when(home)
            def _():
                local.start() if go else local.wait()

            @pl.when(jnp.logical_not(home))
            def _():
                run([away], go)

        home_two = n_row // 2 + 1

        def pair_of(ref, r):
            return ref.at[r // 4, :, pl.ds(r // 2 % 2 * LANES, LANES)]

        def out_copies(n):
            rows = pl.ds(n * OUT_STEPS, OUT_STEPS)
            phase = n * OUT_STEPS // (steps - LATE)
            for r in range(n_row):
                src = hist.at[pl.ds(n * OUT_STEPS + 1, OUT_STEPS), own, r // 4, :, pl.ds(r // 2 % 2 * LANES, LANES)]

                def send(r=r, src=src):
                    out_copy(src, h2_out.at[rows], o_send.at[r, phase], o_recv.at[phase], r, home_two, True)

                if r % 2:
                    send()
                else:
                    pl.when((phase == 1) | (home & (r + 1 == home_two)))(send)

        def outs_sent():
            for phase, ref in enumerate((h2_out.at[pl.ds(0, steps - LATE)], h2_out.at[pl.ds(0, LATE)])):
                for r in range(n_row):
                    def sent(r=r, ref=ref, phase=phase):
                        out_copy(ref, ref, o_send.at[r, phase], o_recv.at[phase], r, home_two, False)

                    if r % 2 or phase:
                        sent()
                    elif r + 1 == home_two:
                        pl.when(home)(sent)

        def c_copies(l, go):
            for r in range(n_row):
                out_copy(pair_of(cst, r), (c1_out, c2_out)[l], c_send.at[r], c_recv.at[l], r, n_x * l + 1, go)

        for r in range(n_row):
            @pl.when(jnp.logical_not(home & (row == r)))
            def _(r=r):
                arrived(cin.at[r], cin_recv.at[r])
        for x in range(n_x):
            pair_of(cst, 2 * x)[...] = cin[2 * x] + cin[2 * x + 1]

        for u in range(H1_AHEAD):
            @pl.when(layer == 1)
            def _(u=u):
                hand = hand_h1(u)
                hand.wait_recv()
                hand.start()
                hand.wait_send()

            @pl.when(jnp.logical_not(home) & (u < lead))
            def _(u=u):
                if u >= 2:
                    middle(u - 2, False)
                middle(u, True)

        zpre[...] = jnp.zeros_like(zpre)
        z_arrives(0)

        def gates(t, z, send):
            for half in HALVES:
                i, f, g, o = z[half * GATES:half * GATES + GATES]
                c_new = sigmoid(f) * cst[half] + sigmoid(i) * jnp.tanh(g)
                cst[half] = c_new
                hist[t + 1, own, half] = (sigmoid(o) * jnp.tanh(c_new)).astype(BF16)
                if send:
                    run([h_copy(t, own, half, d) for d in PEERS], True)

        tiles = range(2 * GATES)

        def finish(t, send):
            for half in HALVES:
                h_copy(t - 1, last, half, 2).wait_recv()
            pieces = [(last, half) for half in HALVES]
            gates(t, [products(t - 1, pieces, cols_of(tile)) + zpre[:, cols_of(tile)] for tile in tiles], send)

        def sent(t):
            for half in HALVES:
                run([h_copy(t, own, half, d) for d in PEERS], False)

        def outputs(t):
            @pl.when((layer == 1) & (t % OUT_STEPS == OUT_STEPS - 1))
            def _():
                out_copies(t // OUT_STEPS)

        def prepare(t):
            @pl.when((t > 1) & (layer == 0))
            def _():
                forward(t - 2, False)

            @pl.when((t > 0) & (layer == 0))
            def _():
                forward(t - 1, True)

            zpre[...] = products(t, [(own, half) for half in HALVES])
            u = t + lead

            @pl.when(jnp.logical_not(home) & (u < steps))
            def _():
                middle(u - 2, False)
                middle(u, True)

            @pl.when((layer == 1) & (t + H1_AHEAD < steps))
            def _():
                hand = hand_h1(t + H1_AHEAD)

                @pl.when(t > 0)
                def _():
                    hand.wait_send()

                hand.wait_recv()
                hand.start()

            @pl.when(t > 0)
            def _():
                sent(t - 1)

            outputs(t)
            for half in HALVES:
                for d, owner in zip(PEERS, (beside, across)):
                    h_copy(t, owner, half, d).wait_recv()
                zpre[...] += products(t, ((beside, half), (across, half)))
                if half == 0:
                    z_arrives(t + 1)

        gates(0, [zpre[:, cols_of(tile)] for tile in tiles], True)
        for _, core, mine, args in relays(None):
            if core == 1:
                @pl.when(mine)
                def _(args=args):
                    slots, sources, to_x = args
                    for group in slots:
                        for s in group:
                            remote(relay.at[s], relay.at[s], rel_send.at[s], rel_recv.at[s, 0], me_else).wait_send()
        for r in range(n_row):
            @pl.when(jnp.logical_not(home & (row == r)))
            def _(r=r):
                arrived(wbuf.at[:, r], w_recv.at[r])

        prepare(0)

        def step(t, carry):
            finish(t, True)
            prepare(t)
            return carry

        lax.fori_loop(1, steps - 1, step, 0)
        end = steps - 1

        @pl.when(jnp.logical_not(home))
        def _():
            middle(end - 1, False)
            middle(end, False)

        sent(end - 1)

        @pl.when(layer == 0)
        def _():
            forward(end - 2, False)
            finish(end, True)
            c_copies(0, True)
            forward(end - 1, True)
            forward(end - 1, False)
            for d, owner in zip(PEERS, (beside, across, last)):
                for half in HALVES:
                    h_copy(end, owner, half, d).wait_recv()
            forward(end, True)
            forward(end, False)
            sent(end)
            c_copies(0, False)

        @pl.when(layer == 1)
        def _():
            hand_h1(0).wait_send()
            finish(end, False)
            outputs(end)
            c_copies(1, True)
            outs_sent()
            c_copies(1, False)

    @pl.when(is_input)
    def _():
        x_load.wait()
        mate = 1 - cc
        for i, ref in enumerate((xb.at[mate], bb.at[mate], init.at[mate], wi1b.at[mate], wi2b.at[:, mate])):
            arrived(ref, in_recv.at[i])
        bias2[...] = bb[0] + bb[1]

        places, heads, middles, homes = [], [], [], []
        for l in LAYERS:
            xr, kr = (xx + n_x - 2 * l) % n_x, (col + n_col - 2 * l) % n_col
            homes.append(kr < 2)
            places.append(jnp.where(kr < 2, xr, (1 + n_x - xr) % n_x))
            heads.append((2 * l + jnp.where(kr < 2, 0, 1)) % n_x)
            middles.append((2 * l + jnp.where(kr < 2, 1, 0)) % n_x)

        def departure(l, u, start):
            p, home = places[l], homes[l]
            src = zout.at[l, u % 2]
            dst_x = jnp.where(p == 2, middles[l], jnp.where(home & (p == 1), xx, heads[l]))
            on = at(dst_x, jnp.where(home, 1, input_core(dst_x, col)), col)
            owner = owner_at(l, col)
            dev = {axis: jnp.where(p == 0, owner[axis], on[axis]) for axis in on}
            ways = [remote(src, buf.at[u], z_send.at[l, u % 2], sem.at[u % RING], dev)
                    for buf, sem in ((za, za_recv), (zb, zb_recv), (zc, zc_recv))]
            if not start:
                ways[0].wait_send()
                return
            to_c = home & (p == 1)
            to_b = (home & (p >= 2)) | (jnp.logical_not(home) & (p == 1))
            for way, here in zip(ways, (jnp.logical_not(to_b | to_c), to_b, to_c)):
                pl.when(here)(way.start)

        def input_sum(l, u):
            p = places[l]

            @pl.when(u >= 2)
            def _():
                departure(l, u - 2, False)

            if l == 0:
                part = dots([(xb[i, u], wi1b[i].reshape(TILE, -1)) for i in HALVES])
            else:
                h1 = jnp.concatenate([h1in[u, j] for j in range(n_col)], axis=1)
                part = dots([(h1, wi2b[...].reshape(2 * TILE, -1))])
            out = zout.at[l, u % 2]
            out[...] = part + bias2[l]

            @pl.when(u == 0)
            def _():
                out[...] += init[0, l] + init[1, l]

            adds = jnp.logical_not(homes[l])

            @pl.when(adds & (p < 2))
            def _():
                arrived(za.at[u], za_recv.at[u % RING])
                out[...] += za[u]

            @pl.when(adds & (p == 0))
            def _():
                arrived(zb.at[u], zb_recv.at[u % RING])
                out[...] += zb[u]

            departure(l, u, True)

        def ahead(u, carry):
            input_sum(0, u)
            return carry

        def by_place(values):
            return functools.reduce(lambda rest, i: jnp.where(places[0] == i, values[i], rest), range(1, n_x), values[0])

        first, lead = by_place(FIRST), by_place(AHEAD)

        def made(t):
            return jnp.minimum(steps, jnp.minimum(first + 2 * t, lead + t))

        soon_made = made(1)
        early = jnp.minimum(soon_made, EARLY)
        lax.fori_loop(0, 1, ahead, 0)
        for l in LAYERS:
            start_up(l, True, held)
        lax.fori_loop(1, early, ahead, 0)

        @pl.when((places[0] == 2) & (col < 2))
        def _():
            pl.semaphore_wait(passed.at[0], 1)

        lax.fori_loop(early, soon_made, ahead, 0)

        def step(t, carry):
            arrived(h1in.at[t], h1_recv.at[t % RING])
            input_sum(1, t)
            lax.fori_loop(made(t + 1), made(t + 2), ahead, 0)
            return carry

        lax.fori_loop(0, steps, step, 0)
        for l in LAYERS:
            for u in HALVES:
                departure(l, steps - 2 + u, False)

    for l in LAYERS:
        start_up(l, False, all_chunks)

    @pl.when(not_input)
    def _():
        run(give, False)

    keeps_own = is_rec & (xx % 2 == 0)
    gets_h2 = jnp.logical_not(keeps_own & (layer == 1))
    early, late = h2_out.at[pl.ds(0, steps - LATE)], h2_out.at[pl.ds(0, LATE)]
    hand_on = remote(early, early, o_send.at[0, 0], o_recv.at[0], me_else)

    @pl.when(gets_h2)
    def _():
        hand_on.wait_recv()
        pl.when(cc == 1)(hand_on.start)

    for l, out in enumerate((c1_out, c2_out)):
        @pl.when(jnp.logical_not(keeps_own & (layer == l)))
        def _(l=l, out=out):
            arrived(out, c_recv.at[l])

    @pl.when(gets_h2)
    def _():
        arrived(late, o_recv.at[1])
        pl.when(cc == 1)(hand_on.wait_send)


def solution(mesh):
    n_row, n_col = mesh.shape["row"], mesh.shape["col"]

    def local_program(seq_in, w_in1, w_rec1, b_gate1, w_in2, w_rec2, b_gate2, h_init, c_init):
        steps, batch, k_rows = seq_in.shape
        unit = b_gate1.shape[0] // GATES
        cols = w_in1.shape[1]
        row = lax.axis_index("row")
        half_own = n_row // 2 * unit
        n_part = k_rows // CHUNK
        pair = 2 * unit

        hbm = pl.BlockSpec(memory_space=pl.ANY)
        near = pl.BlockSpec(memory_space=pltpu.VMEM)
        dma = pltpu.SemaphoreType.DMA
        vm = pltpu.VMEM
        block = (n_col, unit, cols)
        z_all = vm((steps, batch, cols), F32)
        by_step = dma((RING,))
        h2_pair, c1_pair, c2_pair = pl.pallas_call(
            functools.partial(lstm_kernel, n_row, n_col),
            out_shape=(
                jax.ShapeDtypeStruct((steps, batch, pair), BF16),
                jax.ShapeDtypeStruct((batch, pair), F32),
                jax.ShapeDtypeStruct((batch, pair), F32),
            ),
            in_specs=[hbm] * 5 + [near] * 4,
            out_specs=(hbm, hbm, hbm),
            scratch_shapes=[
                vm((4, k_rows, cols), BF16),
                vm((4, *block), BF16),
                vm((3, *block), BF16),
                vm((n_col, n_row, unit, cols), BF16),
                vm((2, *block), BF16),
                vm((n_col, 2, unit, cols), BF16),
                vm((2, steps, batch, k_rows), BF16),
                vm((2, 2, 1, cols), F32),
                vm((2, 1, cols), F32),
                vm((2, 2, batch, cols), F32),
                vm((steps + 1, n_col, 2, batch, half_own), BF16),
                z_all, z_all, z_all,
                vm((2, batch, cols), F32),
                vm((steps, n_col, batch, pair), BF16),
                vm((2, 2, batch, cols), F32),
                vm((batch, cols), F32),
                vm((2, batch, half_own), F32),
                vm((n_row, batch, pair), F32),
                vm((2, batch, pair), F32),
                vm((2, 1, cols), F32),
                dma((4,)), dma((2,)), dma((n_row,)), dma((3, n_part)), dma((3,)),
                dma((5,)), dma((5,)), dma((1,)),
                dma((2,)), dma((n_row,)),
                dma((2, n_col - 1, 2)), dma((2, n_col, 2)),
                by_step, by_step, by_step, dma((2, 2)), dma((2,)),
                dma((n_col,)), by_step,
                dma((n_row, 2)), dma((2,)),
                dma((n_row,)), dma((2,)), pltpu.SemaphoreType.REGULAR((1,)),
            ],
            compiler_params=pltpu.CompilerParams(collective_id=0, has_side_effects=True, vmem_limit_bytes=60 * 2**20),
        )(
            w_rec1, w_rec2, w_in1, w_in2, seq_in, b_gate1.reshape(1, -1), b_gate2.reshape(1, -1), h_init, c_init,
        )

        def own_half(both):
            return lax.dynamic_slice_in_dim(both, (row % 2) * unit, unit, axis=both.ndim - 1)

        return own_half(h2_pair), own_half(c1_pair), own_half(c2_pair)

    row_spec = P(None, "dp", "row")
    weight_spec = P("row", "col")
    bias_spec = P(("col", "row"))
    seq_out_spec = P(None, "dp", ("row", "col"))
    cell_out_spec = P("dp", ("row", "col"))
    return jax.shard_map(
        local_program,
        mesh=mesh,
        in_specs=(row_spec, weight_spec, weight_spec, bias_spec, weight_spec, weight_spec, bias_spec, row_spec, row_spec),
        out_specs=(seq_out_spec, cell_out_spec, cell_out_spec),
        check_vma=False,
    )
```

```python
import functools

import jax
import jax.numpy as jnp
from jax import lax
from jax.experimental import pallas as pl
from jax.experimental.pallas import tpu as pltpu
from jax.sharding import PartitionSpec as P


MESH = pl.DeviceIdType.MESH
F32, BF16 = jnp.float32, jnp.bfloat16
HALVES = LAYERS = (0, 1)
GATES = 4
LANES, TILE, PAIR, OWN = 128, 256, 512, 1024
HALF_LANES = 64
CHUNK = 32
HELD = 2
AHEAD = (5, 8, 12, 8)
FIRST = (4, 4, 7, 6)
EARLY = 3
MIDDLE = (3, 2)
H1_AHEAD = 3
RING = 32
OUT_STEPS = 2
LATE = 8
PEERS = (1, 3, 2)
ORDER = (PEERS, (2, 1, 3))


def sigmoid(v):
    return 0.5 * jnp.tanh(0.5 * v) + 0.5


def lstm_kernel(
    n_row, n_col, wr1, wr2, wi1, wi2, x_in, b1, b2, h0, c0, h2_out, c1_out, c2_out,
    raw, perm, relay, wbuf, wi1b, wi2b, xb, bb, bias2, init, hist, za, zb, zc, zmid, h1in, zout, zpre, cst, cin, cstart, bst,
    raw_sem, w_send, w_recv, rel_recv, rel_send, in_send, in_recv, x_local, c0_send, cin_recv,
    hx_send, hx_recv, za_recv, zb_recv, zc_recv, z_send, zm_send, h1_send, h1_recv, o_send, o_recv, c_send, c_recv, passed,
):
    steps = x_in.shape[0]
    n_x = n_row // 2
    n_part = raw.shape[1] // CHUNK
    per_col = n_part // n_col
    col, row = lax.axis_index("col"), lax.axis_index("row")
    xx, cc = row // 2, row % 2
    in_block = (xx < 2) == (col < 2)
    layer = xx // 2
    is_rec = in_block & (cc == 1)
    is_input = in_block == (cc == 0)
    not_input = jnp.logical_not(is_input)
    other_row = n_col - 1 - col

    def at(x, c, y):
        return {"row": x * 2 + c, "col": y}

    def input_core(x, y):
        return jnp.where((x < 2) == (y < 2), 0, 1)

    def is_away(l, k):
        return (k + n_col - 2 * l) % n_col // 2

    def owner_at(l, k):
        away = is_away(l, k)
        return at(2 * l + away, 1, jnp.where(away == 0, k, n_col - 1 - k))

    def remote(src, dst, ssem, rsem, dev):
        return pltpu.make_async_remote_copy(
            src_ref=src, dst_ref=dst, send_sem=ssem, recv_sem=rsem, device_id=dev, device_id_type=MESH)

    me_else = at(xx, 1 - cc, col)

    def arrived(ref, sem):
        remote(ref, ref, x_local.at[0], sem, me_else).wait_recv()

    def run(copies, go):
        for cp in copies:
            cp.start() if go else cp.wait_send()

    def dots(pieces):
        sums = [jnp.dot(rows, weights, preferred_element_type=F32) for rows, weights in pieces]
        return functools.reduce(jnp.add, sums)

    def cols_of(tile):
        return slice(tile * TILE, tile * TILE + TILE)

    loads = [pltpu.make_async_copy(w, raw.at[i], raw_sem.at[i]) for i, w in enumerate((wr1, wr2, wi1, wi2))]
    for load in loads:
        load.start()
    barrier = pltpu.get_barrier_semaphore()
    for dy in range(n_col):
        for dx in range(n_row):
            if dx or dy:
                pl.semaphore_signal(
                    barrier, inc=1, device_id={"row": (row + dx) % n_row, "col": (col + dy) % n_col}, device_id_type=MESH)

    lane_half = lax.broadcasted_iota(jnp.int32, (1, LANES), 1) // HALF_LANES

    def gate_major(i):
        for q in range(n_x):
            for pair in HALVES:
                at_left = q * PAIR + pair * LANES
                left, right = raw[i, :, at_left:at_left + LANES], raw[i, :, at_left + TILE:at_left + TILE + LANES]
                to = q // 2 * OWN + pair * PAIR + q % 2 * LANES
                low = jnp.concatenate([left[:, :HALF_LANES], right[:, :HALF_LANES]], axis=1)
                high = jnp.concatenate([left[:, HALF_LANES:], right[:, HALF_LANES:]], axis=1)
                for part, start in ((low, to), (high, to + TILE)):
                    perm[i, :, :, start:start + LANES] = part.reshape(n_col, -1, LANES)

    def to_half(tile, odd):
        moved = jnp.where(odd == row % 2, tile, pltpu.roll(tile, HALF_LANES, 1))
        return jnp.where(lane_half == row % 2, moved, 0.0)

    for l in LAYERS:
        cells = jnp.where(col < 2, c0[l, :, :LANES], c0[l, :, LANES:])
        cstart[l] = to_half(cells, col % 2)
        for m in range(GATES):
            start = m // 2 * LANES
            gate = to_half((b1, b2)[l][:, start:start + LANES], m % 2)
            for half in HALVES:
                for part in HALVES:
                    start = half * OWN + m * TILE + part * LANES
                    mine = (row // 4 == half) & (row % 4 // 2 == part)
                    bst[l, :, start:start + LANES] = jnp.where(mine, gate, 0.0)
    loads[0].wait()
    gate_major(0)
    pl.semaphore_wait(barrier, n_row * n_col - 1)

    def part_of(ref, c):
        return ref.at[c // per_col, pl.ds(c % per_col * CHUNK, CHUNK)]

    def start_up(l, go, chunks):
        xr, kr = (xx + n_x - 2 * l) % n_x, (col + n_col - 2 * l) % n_col
        home = kr < 2
        mine = home & (xr == 0) & (cc == 1)
        by_near = home & (xr == 2) & (cc == 0)
        by_far = jnp.logical_not(home) & (xr == 2)
        by_corner = jnp.logical_not(home) & ((xr == 3) | ((xr == 0) & (cc == 0)))
        relayed = by_near | by_far | by_corner
        rx = jnp.where(by_near, (2 * l + 1) % n_x, jnp.where(by_far, (2 * l + 2) % n_x, 2 * l))
        rdev = at(rx, jnp.where(by_far, 0, 1), jnp.where(by_near, col, other_row))
        slot = jnp.where(by_near, 0, jnp.where(by_far, cc, jnp.where(xr == 0, 0, 2 - cc)))
        owner = owner_at(l, col)
        cells = [remote(cstart.at[l], cin.at[row], c0_send.at[l], cin_recv.at[row], owner)]
        direct, by_relay = [], []
        for c in chunks:
            src = part_of(perm.at[l], c)
            direct.append(remote(src, part_of(wbuf.at[:, row], c), w_send.at[l], w_recv.at[row], owner))
            by_relay.append(remote(src, part_of(relay.at[slot], c), w_send.at[l], rel_recv.at[slot, c], rdev))
        if not go:
            direct = by_relay = [remote(perm.at[l], perm.at[l], w_send.at[l], w_recv.at[row], owner)]
        if chunks[0] == 0:
            @pl.when(jnp.logical_not(mine))
            def _():
                run(cells, go)

            if go:
                @pl.when(mine)
                def _():
                    wbuf[:, row] = perm[l]
                    cin[row] = cstart[l]

        @pl.when(jnp.logical_not(mine | relayed))
        def _():
            run(direct, go)

        @pl.when(relayed)
        def _():
            run(by_relay, go)

    all_chunks = range(n_part)
    held = all_chunks[n_part - HELD:]
    for l in LAYERS:
        if l:
            loads[l].wait()
            gate_major(l)
        start_up(l, True, all_chunks[:n_part - HELD])

        @pl.when(not_input)
        def _(l=l):
            start_up(l, True, held)

    for l in LAYERS:
        init[cc, l] = jnp.dot(h0[l].astype(BF16), perm[l].reshape(-1, perm.shape[-1]), preferred_element_type=F32)
    x_load = pltpu.make_async_copy(x_in, xb.at[cc], x_local.at[0])
    give = [remote(s, d, in_send.at[i], in_recv.at[i], me_else) for i, (s, d) in enumerate((
        (x_in, xb.at[cc]), (bst, bb.at[cc]), (init.at[cc], init.at[cc]), (perm.at[2], wi1b.at[cc]), (perm.at[3], wi2b.at[:, cc])))]
    soon = len(give) - 2

    @pl.when(is_input)
    def _():
        x_load.start()
        bb[cc] = bst[...]

    @pl.when(not_input)
    def _():
        run(give[:soon], True)

    for l in LAYERS:
        loads[2 + l].wait()
        gate_major(2 + l)

        @pl.when(is_input)
        def _(l=l):
            (wi1b.at[cc], wi2b.at[:, cc])[l][...] = perm[2 + l]

        @pl.when(not_input)
        def _(l=l):
            give[soon + l].start()

    def pass_on(slots, sources, to_x):
        dev = at(to_x, 1, col)

        def onward(s, c):
            return remote(part_of(relay.at[s], c), part_of(wbuf.at[:, sources[s]], c), rel_send.at[s],
                          w_recv.at[sources[s]], dev)

        for group in slots:
            for c in all_chunks:
                for s in group:
                    arrived(part_of(relay.at[s], c), rel_recv.at[s, c])
                    onward(s, c).start()

        def done():
            for group in slots:
                for s in group:
                    remote(relay.at[s], relay.at[s], rel_send.at[s], rel_recv.at[s, 0], dev).wait_send()

        return done

    def relays(then):
        for l in LAYERS:
            x0, x1, x2, x3 = [(2 * l + i) % n_x for i in range(n_x)]
            here = (col // 2) == l
            for core, x, args in (
                (1, x0, (((1, 2), (0,)), (2 * x0, 2 * x3 + 1, 2 * x3), x1)),
                (1, x1, (((0,),), (2 * x2,), x0)),
                (0, x2, (((0, 1),), (2 * x2, 2 * x2 + 1), x1)),
            ):
                yield l, core, here & (cc == core) & (xx == x), args

    for l, core, mine, args in relays(None):
        @pl.when(mine)
        def _(l=l, core=core, args=args):
            done = pass_on(*args)
            if core == 0:
                done()
                if l == 0:
                    pl.semaphore_signal(passed.at[0], inc=1, device_id=me_else, device_id_type=MESH)

    @pl.when(is_rec)
    def _():
        home = xx % 2 == 0
        own = jnp.where(home, col, other_row)
        beside, across, last = [(own + d) % n_col for d in PEERS]

        def peer(d):
            k = (own + d) % n_col
            away = is_away(layer, k)
            return at(2 * layer + away, 1, jnp.where(away == 0, k, n_col - 1 - k))

        def h_copy(t, owner, half, d):
            ref = hist.at[t + 1, owner, half]
            return remote(ref, ref, hx_send.at[t % 2, d - 1, half], hx_recv.at[t % 2, owner, half], peer(d))

        def products(t, pieces, cols=slice(None)):
            return dots([(hist[t + 1, owner, half], wbuf[owner, half * GATES:half * GATES + GATES, :, cols].reshape(TILE, -1))
                         for owner, half in pieces])

        def z_arrives(t):
            arrived(za.at[t], za_recv.at[t % RING])

            @pl.when(home)
            def _():
                arrived(zb.at[t], zb_recv.at[t % RING])
                arrived(zc.at[t], zc_recv.at[t % RING])

        def input_sums(t):
            return za[t] + jnp.where(home, zb[t] + zc[t], 0.0)

        def forward(t, go):
            near, far = jnp.where(home, 0, 1), jnp.where(home, 3, 2)
            for i, (x, c, y) in enumerate(((far, 1, col), (far, 1, other_row), (near, 1, other_row), (near, 0, col))):
                src = hist.at[t + 1, :, x // 2, :, pl.ds(pl.multiple_of(x % 2 * LANES, LANES), LANES)]
                run([remote(src, h1in.at[t], h1_send.at[i], h1_recv.at[t % RING], at(x, c, y))], go)

        def hand_h1(t):
            return remote(h1in.at[t], h1in.at[t], h1_send.at[0], h1_recv.at[t % RING], me_else)

        def middle(u, go):
            cp = remote(zmid.at[u % 2], zc.at[u], zm_send.at[u % 2], zc_recv.at[u % RING], at(2 * layer, 1, col))
            if go:
                arrived(zb.at[u], zb_recv.at[u % RING])
                arrived(zc.at[u], zc_recv.at[u % RING])
                zmid[u % 2] = zb[u] + zc[u]
            run([cp], go)

        lead = jnp.where(layer == 0, MIDDLE[0], MIDDLE[1])

        def out_copy(src, dst, ssem, rsem, r, home_row, go):
            away = remote(src, dst, ssem, rsem, {"row": r, "col": own})
            if r != home_row:
                run([away], go)
                return
            local = pltpu.make_async_copy(src, dst, ssem)

            @pl.when(home)
            def _():
                local.start() if go else local.wait()

            @pl.when(jnp.logical_not(home))
            def _():
                run([away], go)

        home_two = n_row // 2 + 1

        def pair_of(ref, r):
            return ref.at[r // 4, :, pl.ds(r // 2 % 2 * LANES, LANES)]

        def out_copies(n):
            rows = pl.ds(n * OUT_STEPS, OUT_STEPS)
            phase = n * OUT_STEPS // (steps - LATE)
            for r in range(n_row):
                src = hist.at[pl.ds(n * OUT_STEPS + 1, OUT_STEPS), own, r // 4, :, pl.ds(r // 2 % 2 * LANES, LANES)]

                def send(r=r, src=src):
                    out_copy(src, h2_out.at[rows], o_send.at[r, phase], o_recv.at[phase], r, home_two, True)

                if r % 2:
                    send()
                else:
                    pl.when((phase == 1) | (home & (r + 1 == home_two)))(send)

        def outs_sent():
            for phase, ref in enumerate((h2_out.at[pl.ds(0, steps - LATE)], h2_out.at[pl.ds(0, LATE)])):
                for r in range(n_row):
                    def sent(r=r, ref=ref, phase=phase):
                        out_copy(ref, ref, o_send.at[r, phase], o_recv.at[phase], r, home_two, False)

                    if r % 2 or phase:
                        sent()
                    elif r + 1 == home_two:
                        pl.when(home)(sent)

        def c_copies(l, go):
            for r in range(n_row):
                out_copy(pair_of(cst, r), (c1_out, c2_out)[l], c_send.at[r], c_recv.at[l], r, n_x * l + 1, go)

        for r in range(n_row):
            @pl.when(jnp.logical_not(home & (row == r)))
            def _(r=r):
                arrived(cin.at[r], cin_recv.at[r])
        for x in range(n_x):
            pair_of(cst, 2 * x)[...] = cin[2 * x] + cin[2 * x + 1]

        def run_ahead(u):
            @pl.when(layer == 1)
            def _():
                hand = hand_h1(u)
                hand.wait_recv()
                hand.start()
                hand.wait_send()

            @pl.when(jnp.logical_not(home) & (u < lead))
            def _():
                if u >= 2:
                    middle(u - 2, False)
                middle(u, True)

        for u in range(H1_AHEAD):
            run_ahead(u)
        z_arrives(0)
        zpre[...] = input_sums(0)

        def gates(t, z, send):
            for half in HALVES:
                i, f, g, o = z[half * GATES:half * GATES + GATES]
                c_new = sigmoid(f) * cst[half] + sigmoid(i) * jnp.tanh(g)
                cst[half] = c_new
                hist[t + 1, own, half] = (sigmoid(o) * jnp.tanh(c_new)).astype(BF16)
                if send:
                    run([h_copy(t, own, half, d) for d in ORDER[half]], True)

        tiles = range(2 * GATES)

        def finish(t, send, others):
            for half in HALVES:
                h_copy(t - 1, last, half, 2).wait_recv()
            pieces = [(last, half) for half in HALVES]
            gates(t, [part + products(t - 1, pieces, cols_of(tile)) + zpre[:, cols_of(tile)]
                      for tile, part in zip(tiles, others)], send)

        def sent(t):
            for half in HALVES:
                run([h_copy(t, own, half, d) for d in PEERS], False)

        def outputs(t):
            @pl.when((layer == 1) & (t % OUT_STEPS == OUT_STEPS - 1))
            def _():
                out_copies(t // OUT_STEPS)

        def prepare(t):
            @pl.when((t > 1) & (layer == 0))
            def _():
                forward(t - 2, False)

            @pl.when((t > 0) & (layer == 0))
            def _():
                forward(t - 1, True)

            zpre[...] = products(t, [(own, half) for half in HALVES])
            u = t + lead

            @pl.when(jnp.logical_not(home) & (u < steps))
            def _():
                middle(u - 2, False)
                middle(u, True)

            @pl.when((layer == 1) & (t + H1_AHEAD < steps))
            def _():
                hand = hand_h1(t + H1_AHEAD)

                @pl.when(t > 0)
                def _():
                    hand.wait_send()

                hand.wait_recv()
                hand.start()

            @pl.when(t > 0)
            def _():
                sent(t - 1)

            outputs(t)
            parts = []
            for half in HALVES:
                if half:
                    z_arrives(t + 1)
                for d, owner in zip(PEERS, (beside, across)):
                    h_copy(t, owner, half, d).wait_recv()
                if half:
                    zpre[...] += input_sums(t + 1)
                parts.append([products(t, ((beside, half), (across, half)), cols_of(tile)) for tile in tiles])
            return [a + b for a, b in zip(*parts)]

        gates(0, [zpre[:, cols_of(tile)] for tile in tiles], True)
        for _, core, mine, args in relays(None):
            if core == 1:
                @pl.when(mine)
                def _(args=args):
                    slots, sources, to_x = args
                    for group in slots:
                        for s in group:
                            remote(relay.at[s], relay.at[s], rel_send.at[s], rel_recv.at[s, 0], me_else).wait_send()
        for r in range(n_row):
            @pl.when(jnp.logical_not(home & (row == r)))
            def _(r=r):
                arrived(wbuf.at[:, r], w_recv.at[r])

        end = steps - 1

        def step(t, carry):
            finish(t + 1, True, prepare(t))
            return carry

        lax.fori_loop(0, end - 1, step, 0)
        others = prepare(end - 1)

        @pl.when(jnp.logical_not(home))
        def _():
            middle(end - 1, False)
            middle(end, False)

        sent(end - 1)

        @pl.when(layer == 0)
        def _():
            forward(end - 2, False)
            finish(end, True, others)
            c_copies(0, True)
            forward(end - 1, True)
            forward(end - 1, False)
            for d, owner in zip(PEERS, (beside, across, last)):
                for half in HALVES:
                    h_copy(end, owner, half, d).wait_recv()
            forward(end, True)
            forward(end, False)
            sent(end)
            c_copies(0, False)

        @pl.when(layer == 1)
        def _():
            hand_h1(0).wait_send()
            finish(end, False, others)
            outputs(end)
            c_copies(1, True)
            outs_sent()
            c_copies(1, False)

    @pl.when(is_input)
    def _():
        x_load.wait()
        mate = 1 - cc
        for i, ref in enumerate((xb.at[mate], bb.at[mate], init.at[mate], wi1b.at[mate], wi2b.at[:, mate])):
            arrived(ref, in_recv.at[i])
        bias2[...] = bb[0] + bb[1]

        places, heads, middles, homes = [], [], [], []
        for l in LAYERS:
            xr, kr = (xx + n_x - 2 * l) % n_x, (col + n_col - 2 * l) % n_col
            homes.append(kr < 2)
            places.append(jnp.where(kr < 2, xr, (1 + n_x - xr) % n_x))
            heads.append((2 * l + jnp.where(kr < 2, 0, 1)) % n_x)
            middles.append((2 * l + jnp.where(kr < 2, 1, 0)) % n_x)

        def departure(l, u, start):
            p, home = places[l], homes[l]
            src = zout.at[l, u % 2]
            dst_x = jnp.where(p == 2, middles[l], jnp.where(home & (p == 1), xx, heads[l]))
            on = at(dst_x, jnp.where(home, 1, input_core(dst_x, col)), col)
            owner = owner_at(l, col)
            dev = {axis: jnp.where(p == 0, owner[axis], on[axis]) for axis in on}
            ways = [remote(src, buf.at[u], z_send.at[l, u % 2], sem.at[u % RING], dev)
                    for buf, sem in ((za, za_recv), (zb, zb_recv), (zc, zc_recv))]
            if not start:
                ways[0].wait_send()
                return
            to_c = home & (p == 1)
            to_b = (home & (p >= 2)) | (jnp.logical_not(home) & (p == 1))
            for way, here in zip(ways, (jnp.logical_not(to_b | to_c), to_b, to_c)):
                pl.when(here)(way.start)

        def input_sum(l, u):
            p = places[l]

            @pl.when(u >= 2)
            def _():
                departure(l, u - 2, False)

            if l == 0:
                part = dots([(xb[i, u], wi1b[i].reshape(TILE, -1)) for i in HALVES])
            else:
                h1 = jnp.concatenate([h1in[u, j] for j in range(n_col)], axis=1)
                part = dots([(h1, wi2b[...].reshape(2 * TILE, -1))])
            out = zout.at[l, u % 2]
            out[...] = part + bias2[l]

            @pl.when(u == 0)
            def _():
                out[...] += init[0, l] + init[1, l]

            adds = jnp.logical_not(homes[l])

            @pl.when(adds & (p < 2))
            def _():
                arrived(za.at[u], za_recv.at[u % RING])
                out[...] += za[u]

            @pl.when(adds & (p == 0))
            def _():
                arrived(zb.at[u], zb_recv.at[u % RING])
                out[...] += zb[u]

            departure(l, u, True)

        def ahead(u, carry):
            input_sum(0, u)
            return carry

        def by_place(values):
            return functools.reduce(lambda rest, i: jnp.where(places[0] == i, values[i], rest), range(1, n_x), values[0])

        first, lead = by_place(FIRST), by_place(AHEAD)

        def made(t):
            return jnp.minimum(steps, jnp.minimum(first + 2 * t, lead + t))

        soon_made = made(1)
        early = jnp.minimum(soon_made, EARLY)
        lax.fori_loop(0, 1, ahead, 0)
        for l in LAYERS:
            start_up(l, True, held)
        lax.fori_loop(1, early, ahead, 0)

        @pl.when((places[0] == 2) & (col < 2))
        def _():
            pl.semaphore_wait(passed.at[0], 1)

        lax.fori_loop(early, soon_made, ahead, 0)

        def step(t, carry):
            arrived(h1in.at[t], h1_recv.at[t % RING])
            input_sum(1, t)
            lax.fori_loop(made(t + 1), made(t + 2), ahead, 0)
            return carry

        lax.fori_loop(0, steps, step, 0)
        for l in LAYERS:
            for u in HALVES:
                departure(l, steps - 2 + u, False)

    for l in LAYERS:
        start_up(l, False, all_chunks)

    @pl.when(not_input)
    def _():
        run(give, False)

    keeps_own = is_rec & (xx % 2 == 0)
    gets_h2 = jnp.logical_not(keeps_own & (layer == 1))
    early, late = h2_out.at[pl.ds(0, steps - LATE)], h2_out.at[pl.ds(0, LATE)]
    hand_on = remote(early, early, o_send.at[0, 0], o_recv.at[0], me_else)

    @pl.when(gets_h2)
    def _():
        hand_on.wait_recv()
        pl.when(cc == 1)(hand_on.start)

    for l, out in enumerate((c1_out, c2_out)):
        @pl.when(jnp.logical_not(keeps_own & (layer == l)))
        def _(l=l, out=out):
            arrived(out, c_recv.at[l])

    @pl.when(gets_h2)
    def _():
        arrived(late, o_recv.at[1])
        pl.when(cc == 1)(hand_on.wait_send)


def solution(mesh):
    n_row, n_col = mesh.shape["row"], mesh.shape["col"]

    def local_program(seq_in, w_in1, w_rec1, b_gate1, w_in2, w_rec2, b_gate2, h_init, c_init):
        steps, batch, k_rows = seq_in.shape
        unit = b_gate1.shape[0] // GATES
        cols = w_in1.shape[1]
        row = lax.axis_index("row")
        half_own = n_row // 2 * unit
        n_part = k_rows // CHUNK
        pair = 2 * unit

        hbm = pl.BlockSpec(memory_space=pl.ANY)
        near = pl.BlockSpec(memory_space=pltpu.VMEM)
        dma = pltpu.SemaphoreType.DMA
        vm = pltpu.VMEM
        block = (n_col, unit, cols)
        z_all = vm((steps, batch, cols), F32)
        by_step = dma((RING,))
        h2_pair, c1_pair, c2_pair = pl.pallas_call(
            functools.partial(lstm_kernel, n_row, n_col),
            out_shape=(
                jax.ShapeDtypeStruct((steps, batch, pair), BF16),
                jax.ShapeDtypeStruct((batch, pair), F32),
                jax.ShapeDtypeStruct((batch, pair), F32),
            ),
            in_specs=[hbm] * 5 + [near] * 4,
            out_specs=(hbm, hbm, hbm),
            scratch_shapes=[
                vm((4, k_rows, cols), BF16),
                vm((4, *block), BF16),
                vm((3, *block), BF16),
                vm((n_col, n_row, unit, cols), BF16),
                vm((2, *block), BF16),
                vm((n_col, 2, unit, cols), BF16),
                vm((2, steps, batch, k_rows), BF16),
                vm((2, 2, 1, cols), F32),
                vm((2, 1, cols), F32),
                vm((2, 2, batch, cols), F32),
                vm((steps + 1, n_col, 2, batch, half_own), BF16),
                z_all, z_all, z_all,
                vm((2, batch, cols), F32),
                vm((steps, n_col, batch, pair), BF16),
                vm((2, 2, batch, cols), F32),
                vm((batch, cols), F32),
                vm((2, batch, half_own), F32),
                vm((n_row, batch, pair), F32),
                vm((2, batch, pair), F32),
                vm((2, 1, cols), F32),
                dma((4,)), dma((2,)), dma((n_row,)), dma((3, n_part)), dma((3,)),
                dma((5,)), dma((5,)), dma((1,)),
                dma((2,)), dma((n_row,)),
                dma((2, n_col - 1, 2)), dma((2, n_col, 2)),
                by_step, by_step, by_step, dma((2, 2)), dma((2,)),
                dma((n_col,)), by_step,
                dma((n_row, 2)), dma((2,)),
                dma((n_row,)), dma((2,)), pltpu.SemaphoreType.REGULAR((1,)),
            ],
            compiler_params=pltpu.CompilerParams(collective_id=0, has_side_effects=True, vmem_limit_bytes=60 * 2**20),
        )(
            w_rec1, w_rec2, w_in1, w_in2, seq_in, b_gate1.reshape(1, -1), b_gate2.reshape(1, -1), h_init, c_init,
        )

        def own_half(both):
            return lax.dynamic_slice_in_dim(both, (row % 2) * unit, unit, axis=both.ndim - 1)

        return own_half(h2_pair), own_half(c1_pair), own_half(c2_pair)

    row_spec = P(None, "dp", "row")
    weight_spec = P("row", "col")
    bias_spec = P(("col", "row"))
    seq_out_spec = P(None, "dp", ("row", "col"))
    cell_out_spec = P("dp", ("row", "col"))
    return jax.shard_map(
        local_program,
        mesh=mesh,
        in_specs=(row_spec, weight_spec, weight_spec, bias_spec, weight_spec, weight_spec, bias_spec, row_spec, row_spec),
        out_specs=(seq_out_spec, cell_out_spec, cell_out_spec),
        check_vma=False,
    )
```

```python
import functools

import jax
import jax.numpy as jnp
from jax import lax
from jax.experimental import pallas as pl
from jax.experimental.pallas import tpu as pltpu
from jax.sharding import PartitionSpec as P


MESH = pl.DeviceIdType.MESH
F32, BF16 = jnp.float32, jnp.bfloat16
HALVES = LAYERS = (0, 1)
GATES = 4
LANES, TILE, PAIR, OWN = 128, 256, 512, 1024
HALF_LANES = 64
CHUNK = 32
HELD = 1
AHEAD = (5, 8, 12, 8)
FIRST = (4, 4, 7, 6)
EARLY = 3
MIDDLE = (3, 2)
H1_AHEAD = 3
RING = 24
OUT_STEPS = 2
LATE = 8
PEERS = (1, 3, 2)
ORDER = (PEERS, (2, 1, 3))


def sigmoid(v):
    return 0.5 * jnp.tanh(0.5 * v) + 0.5


def lstm_kernel(
    n_row, n_col, wr1, wr2, wi1, wi2, x_in, b1, b2, h0, c0, h2_out, c1_out, c2_out,
    raw, perm, relay, wbuf, wi1b, wi2b, xb, bb, bias2, init, hist, za, zb, zc, zmid, h1in, zout, zpre, cst, cin, cstart, bst,
    raw_sem, w_send, w_recv, rel_recv, rel_send, in_send, in_recv, x_local, c0_send, cin_recv,
    hx_send, hx_recv, za_recv, zb_recv, zc_recv, z_send, zm_send, h1_send, h1_recv, o_send, o_recv, c_send, c_recv, passed,
):
    steps = x_in.shape[0]
    n_x = n_row // 2
    n_part = raw.shape[1] // CHUNK
    per_col = n_part // n_col
    col, row = lax.axis_index("col"), lax.axis_index("row")
    xx, cc = row // 2, row % 2
    in_block = (xx < 2) == (col < 2)
    layer = xx // 2
    is_rec = in_block & (cc == 1)
    is_input = in_block == (cc == 0)
    not_input = jnp.logical_not(is_input)
    other_row = n_col - 1 - col

    def at(x, c, y):
        return {"row": x * 2 + c, "col": y}

    def input_core(x, y):
        return jnp.where((x < 2) == (y < 2), 0, 1)

    def is_away(l, k):
        return (k + n_col - 2 * l) % n_col // 2

    def owner_at(l, k):
        away = is_away(l, k)
        return at(2 * l + away, 1, jnp.where(away == 0, k, n_col - 1 - k))

    def remote(src, dst, ssem, rsem, dev):
        return pltpu.make_async_remote_copy(
            src_ref=src, dst_ref=dst, send_sem=ssem, recv_sem=rsem, device_id=dev, device_id_type=MESH)

    me_else = at(xx, 1 - cc, col)

    def arrived(ref, sem):
        remote(ref, ref, x_local.at[0], sem, me_else).wait_recv()

    def run(copies, go):
        for cp in copies:
            cp.start() if go else cp.wait_send()

    def dots(pieces):
        sums = [jnp.dot(rows, weights, preferred_element_type=F32) for rows, weights in pieces]
        return functools.reduce(jnp.add, sums)

    def cols_of(tile):
        return slice(tile * TILE, tile * TILE + TILE)

    loads = [pltpu.make_async_copy(w, raw.at[i], raw_sem.at[i]) for i, w in enumerate((wr1, wr2, wi1, wi2))]
    for load in loads:
        load.start()
    barrier = pltpu.get_barrier_semaphore()
    for dy in range(n_col):
        for dx in range(n_row):
            if dx or dy:
                pl.semaphore_signal(
                    barrier, inc=1, device_id={"row": (row + dx) % n_row, "col": (col + dy) % n_col}, device_id_type=MESH)

    lane_half = lax.broadcasted_iota(jnp.int32, (1, LANES), 1) // HALF_LANES

    def gate_major(i):
        for q in range(n_x):
            for pair in HALVES:
                at_left = q * PAIR + pair * LANES
                left, right = raw[i, :, at_left:at_left + LANES], raw[i, :, at_left + TILE:at_left + TILE + LANES]
                to = q // 2 * OWN + pair * PAIR + q % 2 * LANES
                low = jnp.concatenate([left[:, :HALF_LANES], right[:, :HALF_LANES]], axis=1)
                high = jnp.concatenate([left[:, HALF_LANES:], right[:, HALF_LANES:]], axis=1)
                for part, start in ((low, to), (high, to + TILE)):
                    perm[i, :, :, start:start + LANES] = part.reshape(n_col, -1, LANES)

    def to_half(tile, odd):
        moved = jnp.where(odd == row % 2, tile, pltpu.roll(tile, HALF_LANES, 1))
        return jnp.where(lane_half == row % 2, moved, 0.0)

    for l in LAYERS:
        cells = jnp.where(col < 2, c0[l, :, :LANES], c0[l, :, LANES:])
        cstart[l] = to_half(cells, col % 2)
        for m in range(GATES):
            start = m // 2 * LANES
            gate = to_half((b1, b2)[l][:, start:start + LANES], m % 2)
            for half in HALVES:
                for part in HALVES:
                    start = half * OWN + m * TILE + part * LANES
                    mine = (row // 4 == half) & (row % 4 // 2 == part)
                    bst[l, :, start:start + LANES] = jnp.where(mine, gate, 0.0)
    loads[0].wait()
    gate_major(0)
    pl.semaphore_wait(barrier, n_row * n_col - 1)

    def part_of(ref, c):
        return ref.at[c // per_col, pl.ds(c % per_col * CHUNK, CHUNK)]

    def start_up(l, go, chunks):
        xr, kr = (xx + n_x - 2 * l) % n_x, (col + n_col - 2 * l) % n_col
        home = kr < 2
        mine = home & (xr == 0) & (cc == 1)
        by_near = home & (xr == 2) & (cc == 0)
        by_far = jnp.logical_not(home) & (xr == 2)
        by_corner = jnp.logical_not(home) & ((xr == 3) | ((xr == 0) & (cc == 0)))
        relayed = by_near | by_far | by_corner
        rx = jnp.where(by_near, (2 * l + 1) % n_x, jnp.where(by_far, (2 * l + 2) % n_x, 2 * l))
        rdev = at(rx, jnp.where(by_far, 0, 1), jnp.where(by_near, col, other_row))
        slot = jnp.where(by_near, 0, jnp.where(by_far, cc, jnp.where(xr == 0, 0, 2 - cc)))
        owner = owner_at(l, col)
        cells = [remote(cstart.at[l], cin.at[row], c0_send.at[l], cin_recv.at[row], owner)]
        direct, by_relay = [], []
        for c in chunks:
            src = part_of(perm.at[l], c)
            direct.append(remote(src, part_of(wbuf.at[:, row], c), w_send.at[l], w_recv.at[row], owner))
            by_relay.append(remote(src, part_of(relay.at[slot], c), w_send.at[l], rel_recv.at[slot, c], rdev))
        if not go:
            direct = by_relay = [remote(perm.at[l], perm.at[l], w_send.at[l], w_recv.at[row], owner)]
        if chunks[0] == 0:
            @pl.when(jnp.logical_not(mine))
            def _():
                run(cells, go)

            if go:
                @pl.when(mine)
                def _():
                    wbuf[:, row] = perm[l]
                    cin[row] = cstart[l]

        @pl.when(jnp.logical_not(mine | relayed))
        def _():
            run(direct, go)

        @pl.when(relayed)
        def _():
            run(by_relay, go)

    all_chunks = range(n_part)
    held = all_chunks[n_part - HELD:]
    for l in LAYERS:
        if l:
            loads[l].wait()
            gate_major(l)
        start_up(l, True, all_chunks[:n_part - HELD])

        @pl.when(not_input)
        def _(l=l):
            start_up(l, True, held)

    for l in LAYERS:
        init[cc, l] = jnp.dot(h0[l].astype(BF16), perm[l].reshape(-1, perm.shape[-1]), preferred_element_type=F32)
    x_load = pltpu.make_async_copy(x_in, xb.at[cc], x_local.at[0])
    give = [remote(s, d, in_send.at[i], in_recv.at[i], me_else) for i, (s, d) in enumerate((
        (x_in, xb.at[cc]), (bst, bb.at[cc]), (init.at[cc], init.at[cc]), (perm.at[2], wi1b.at[cc]), (perm.at[3], wi2b.at[:, cc])))]
    soon = len(give) - 2

    @pl.when(is_input)
    def _():
        x_load.start()
        bb[cc] = bst[...]

    @pl.when(not_input)
    def _():
        run(give[:soon], True)

    for l in LAYERS:
        loads[2 + l].wait()
        gate_major(2 + l)

        @pl.when(is_input)
        def _(l=l):
            (wi1b.at[cc], wi2b.at[:, cc])[l][...] = perm[2 + l]

        @pl.when(not_input)
        def _(l=l):
            give[soon + l].start()

    def pass_on(slots, sources, to_x):
        dev = at(to_x, 1, col)

        def onward(s, c):
            return remote(part_of(relay.at[s], c), part_of(wbuf.at[:, sources[s]], c), rel_send.at[s],
                          w_recv.at[sources[s]], dev)

        for group in slots:
            for c in all_chunks:
                for s in group:
                    arrived(part_of(relay.at[s], c), rel_recv.at[s, c])
                    onward(s, c).start()

        def done():
            for group in slots:
                for s in group:
                    remote(relay.at[s], relay.at[s], rel_send.at[s], rel_recv.at[s, 0], dev).wait_send()

        return done

    def relays(then):
        for l in LAYERS:
            x0, x1, x2, x3 = [(2 * l + i) % n_x for i in range(n_x)]
            here = (col // 2) == l
            for core, x, args in (
                (1, x0, (((1, 2), (0,)), (2 * x0, 2 * x3 + 1, 2 * x3), x1)),
                (1, x1, (((0,),), (2 * x2,), x0)),
                (0, x2, (((0, 1),), (2 * x2, 2 * x2 + 1), x1)),
            ):
                yield l, core, here & (cc == core) & (xx == x), args

    for l, core, mine, args in relays(None):
        @pl.when(mine)
        def _(l=l, core=core, args=args):
            done = pass_on(*args)
            if core == 0:
                done()
                if l == 0:
                    pl.semaphore_signal(passed.at[0], inc=1, device_id=me_else, device_id_type=MESH)

    @pl.when(is_rec)
    def _():
        home = xx % 2 == 0
        own = jnp.where(home, col, other_row)
        beside, across, last = [(own + d) % n_col for d in PEERS]

        def peer(d):
            k = (own + d) % n_col
            away = is_away(layer, k)
            return at(2 * layer + away, 1, jnp.where(away == 0, k, n_col - 1 - k))

        def h_copy(t, owner, half, d):
            ref = hist.at[t + 1, owner, half]
            return remote(ref, ref, hx_send.at[t % 2, d - 1, half], hx_recv.at[t % 2, owner, half], peer(d))

        def products(t, pieces, cols=slice(None)):
            return dots([(hist[t + 1, owner, half], wbuf[owner, half * GATES:half * GATES + GATES, :, cols].reshape(TILE, -1))
                         for owner, half in pieces])

        def z_arrives(t):
            arrived(za.at[t], za_recv.at[t % RING])

            @pl.when(home)
            def _():
                arrived(zb.at[t], zb_recv.at[t % RING])
                arrived(zc.at[t], zc_recv.at[t % RING])

        def input_sums(t):
            return za[t] + jnp.where(home, zb[t] + zc[t], 0.0)

        def forward(t, go):
            near, far = jnp.where(home, 0, 1), jnp.where(home, 3, 2)
            for i, (x, c, y) in enumerate(((far, 1, col), (far, 1, other_row), (near, 1, other_row), (near, 0, col))):
                src = hist.at[t + 1, :, x // 2, :, pl.ds(pl.multiple_of(x % 2 * LANES, LANES), LANES)]
                run([remote(src, h1in.at[t], h1_send.at[i], h1_recv.at[t % RING], at(x, c, y))], go)

        def hand_h1(t):
            return remote(h1in.at[t], h1in.at[t], h1_send.at[0], h1_recv.at[t % RING], me_else)

        def middle(u, go):
            cp = remote(zmid.at[u % 2], zc.at[u], zm_send.at[u % 2], zc_recv.at[u % RING], at(2 * layer, 1, col))
            if go:
                arrived(zb.at[u], zb_recv.at[u % RING])
                arrived(zc.at[u], zc_recv.at[u % RING])
                zmid[u % 2] = zb[u] + zc[u]
            run([cp], go)

        lead = jnp.where(layer == 0, MIDDLE[0], MIDDLE[1])

        def out_copy(src, dst, ssem, rsem, r, home_row, go):
            away = remote(src, dst, ssem, rsem, {"row": r, "col": own})
            if r != home_row:
                run([away], go)
                return
            local = pltpu.make_async_copy(src, dst, ssem)

            @pl.when(home)
            def _():
                local.start() if go else local.wait()

            @pl.when(jnp.logical_not(home))
            def _():
                run([away], go)

        home_two = n_row // 2 + 1

        def pair_of(ref, r):
            return ref.at[r // 4, :, pl.ds(r // 2 % 2 * LANES, LANES)]

        def out_copies(n):
            rows = pl.ds(n * OUT_STEPS, OUT_STEPS)
            phase = n * OUT_STEPS // (steps - LATE)
            for r in range(n_row):
                src = hist.at[pl.ds(n * OUT_STEPS + 1, OUT_STEPS), own, r // 4, :, pl.ds(r // 2 % 2 * LANES, LANES)]

                def send(r=r, src=src):
                    out_copy(src, h2_out.at[rows], o_send.at[r, phase], o_recv.at[phase], r, home_two, True)

                if r % 2:
                    send()
                else:
                    pl.when((phase == 1) | (home & (r + 1 == home_two)))(send)

        def outs_sent():
            for phase, ref in enumerate((h2_out.at[pl.ds(0, steps - LATE)], h2_out.at[pl.ds(0, LATE)])):
                for r in range(n_row):
                    def sent(r=r, ref=ref, phase=phase):
                        out_copy(ref, ref, o_send.at[r, phase], o_recv.at[phase], r, home_two, False)

                    if r % 2 or phase:
                        sent()
                    elif r + 1 == home_two:
                        pl.when(home)(sent)

        def c_copies(l, go):
            for r in range(n_row):
                out_copy(pair_of(cst, r), (c1_out, c2_out)[l], c_send.at[r], c_recv.at[l], r, n_x * l + 1, go)

        for r in range(n_row):
            @pl.when(jnp.logical_not(home & (row == r)))
            def _(r=r):
                arrived(cin.at[r], cin_recv.at[r])
        for x in range(n_x):
            pair_of(cst, 2 * x)[...] = cin[2 * x] + cin[2 * x + 1]

        def run_ahead(u):
            @pl.when(layer == 1)
            def _():
                hand = hand_h1(u)
                hand.wait_recv()
                hand.start()
                hand.wait_send()

            @pl.when(jnp.logical_not(home) & (u < lead))
            def _():
                if u >= 2:
                    middle(u - 2, False)
                middle(u, True)

        for u in range(H1_AHEAD):
            run_ahead(u)
        z_arrives(0)
        zpre[...] = input_sums(0)

        def gates(t, z, send):
            for half in HALVES:
                i, f, g, o = z[half * GATES:half * GATES + GATES]
                c_new = sigmoid(f) * cst[half] + sigmoid(i) * jnp.tanh(g)
                cst[half] = c_new
                hist[t + 1, own, half] = (sigmoid(o) * jnp.tanh(c_new)).astype(BF16)
                if send:
                    run([h_copy(t, own, half, d) for d in ORDER[half]], True)

        tiles = range(2 * GATES)

        def finish(t, send, others):
            for half in HALVES:
                h_copy(t - 1, last, half, 2).wait_recv()
            pieces = [(last, half) for half in HALVES]
            gates(t, [part + products(t - 1, pieces, cols_of(tile)) + zpre[:, cols_of(tile)]
                      for tile, part in zip(tiles, others)], send)

        def sent(t):
            for half in HALVES:
                run([h_copy(t, own, half, d) for d in PEERS], False)

        def outputs(t):
            @pl.when((layer == 1) & (t % OUT_STEPS == OUT_STEPS - 1))
            def _():
                out_copies(t // OUT_STEPS)

        def prepare(t):
            @pl.when((t > 1) & (layer == 0))
            def _():
                forward(t - 2, False)

            @pl.when((t > 0) & (layer == 0))
            def _():
                forward(t - 1, True)

            zpre[...] = products(t, [(own, half) for half in HALVES])
            u = t + lead

            @pl.when(jnp.logical_not(home) & (u < steps))
            def _():
                middle(u - 2, False)
                middle(u, True)

            @pl.when((layer == 1) & (t + H1_AHEAD < steps))
            def _():
                hand = hand_h1(t + H1_AHEAD)

                @pl.when(t > 0)
                def _():
                    hand.wait_send()

                hand.wait_recv()
                hand.start()

            @pl.when(t > 0)
            def _():
                sent(t - 1)

            outputs(t)
            parts = []
            for half in HALVES:
                if half:
                    z_arrives(t + 1)
                for d, owner in zip(PEERS, (beside, across)):
                    h_copy(t, owner, half, d).wait_recv()
                if half:
                    zpre[...] += input_sums(t + 1)
                parts.append([products(t, ((beside, half), (across, half)), cols_of(tile)) for tile in tiles])
            return [a + b for a, b in zip(*parts)]

        gates(0, [zpre[:, cols_of(tile)] for tile in tiles], True)
        for _, core, mine, args in relays(None):
            if core == 1:
                @pl.when(mine)
                def _(args=args):
                    slots, sources, to_x = args
                    for group in slots:
                        for s in group:
                            remote(relay.at[s], relay.at[s], rel_send.at[s], rel_recv.at[s, 0], me_else).wait_send()
        for r in range(n_row):
            @pl.when(jnp.logical_not(home & (row == r)))
            def _(r=r):
                arrived(wbuf.at[:, r], w_recv.at[r])

        end = steps - 1

        def step(t, carry):
            finish(t + 1, True, prepare(t))
            return carry

        lax.fori_loop(0, end - 1, step, 0)
        others = prepare(end - 1)

        @pl.when(jnp.logical_not(home))
        def _():
            middle(end - 1, False)
            middle(end, False)

        sent(end - 1)

        @pl.when(layer == 0)
        def _():
            forward(end - 2, False)
            finish(end, True, others)
            c_copies(0, True)
            forward(end - 1, True)
            forward(end - 1, False)
            for d, owner in zip(PEERS, (beside, across, last)):
                for half in HALVES:
                    h_copy(end, owner, half, d).wait_recv()
            forward(end, True)
            forward(end, False)
            sent(end)
            c_copies(0, False)

        @pl.when(layer == 1)
        def _():
            hand_h1(0).wait_send()
            finish(end, False, others)
            outputs(end)
            c_copies(1, True)
            outs_sent()
            c_copies(1, False)

    @pl.when(is_input)
    def _():
        x_load.wait()
        mate = 1 - cc
        for i, ref in enumerate((xb.at[mate], bb.at[mate], init.at[mate], wi1b.at[mate], wi2b.at[:, mate])):
            arrived(ref, in_recv.at[i])
        bias2[...] = bb[0] + bb[1]

        places, heads, middles, homes = [], [], [], []
        for l in LAYERS:
            xr, kr = (xx + n_x - 2 * l) % n_x, (col + n_col - 2 * l) % n_col
            homes.append(kr < 2)
            places.append(jnp.where(kr < 2, xr, (1 + n_x - xr) % n_x))
            heads.append((2 * l + jnp.where(kr < 2, 0, 1)) % n_x)
            middles.append((2 * l + jnp.where(kr < 2, 1, 0)) % n_x)

        def departure(l, u, start):
            p, home = places[l], homes[l]
            src = zout.at[l, u % 2]
            dst_x = jnp.where(p == 2, middles[l], jnp.where(home & (p == 1), xx, heads[l]))
            on = at(dst_x, jnp.where(home, 1, input_core(dst_x, col)), col)
            owner = owner_at(l, col)
            dev = {axis: jnp.where(p == 0, owner[axis], on[axis]) for axis in on}
            ways = [remote(src, buf.at[u], z_send.at[l, u % 2], sem.at[u % RING], dev)
                    for buf, sem in ((za, za_recv), (zb, zb_recv), (zc, zc_recv))]
            if not start:
                ways[0].wait_send()
                return
            to_c = home & (p == 1)
            to_b = (home & (p >= 2)) | (jnp.logical_not(home) & (p == 1))
            for way, here in zip(ways, (jnp.logical_not(to_b | to_c), to_b, to_c)):
                pl.when(here)(way.start)

        def input_sum(l, u):
            p = places[l]

            @pl.when(u >= 2)
            def _():
                departure(l, u - 2, False)

            if l == 0:
                part = dots([(xb[i, u], wi1b[i].reshape(TILE, -1)) for i in HALVES])
            else:
                h1 = jnp.concatenate([h1in[u, j] for j in range(n_col)], axis=1)
                part = dots([(h1, wi2b[...].reshape(2 * TILE, -1))])
            out = zout.at[l, u % 2]
            out[...] = part + bias2[l]

            @pl.when(u == 0)
            def _():
                out[...] += init[0, l] + init[1, l]

            adds = jnp.logical_not(homes[l])

            @pl.when(adds & (p < 2))
            def _():
                arrived(za.at[u], za_recv.at[u % RING])
                out[...] += za[u]

            @pl.when(adds & (p == 0))
            def _():
                arrived(zb.at[u], zb_recv.at[u % RING])
                out[...] += zb[u]

            departure(l, u, True)

        def ahead(u, carry):
            input_sum(0, u)
            return carry

        def by_place(values):
            return functools.reduce(lambda rest, i: jnp.where(places[0] == i, values[i], rest), range(1, n_x), values[0])

        first, lead = by_place(FIRST), by_place(AHEAD)

        def made(t):
            return jnp.minimum(steps, jnp.minimum(first + 2 * t, lead + t))

        soon_made = made(1)
        early = jnp.minimum(soon_made, EARLY)
        lax.fori_loop(0, 1, ahead, 0)
        for l in LAYERS:
            start_up(l, True, held)
        lax.fori_loop(1, early, ahead, 0)

        @pl.when((places[0] == 2) & (col < 2))
        def _():
            pl.semaphore_wait(passed.at[0], 1)

        lax.fori_loop(early, soon_made, ahead, 0)

        def step(t, carry):
            arrived(h1in.at[t], h1_recv.at[t % RING])
            input_sum(1, t)
            lax.fori_loop(made(t + 1), made(t + 2), ahead, 0)
            return carry

        lax.fori_loop(0, steps, step, 0)
        for l in LAYERS:
            for u in HALVES:
                departure(l, steps - 2 + u, False)

    for l in LAYERS:
        start_up(l, False, all_chunks)

    @pl.when(not_input)
    def _():
        run(give, False)

    keeps_own = is_rec & (xx % 2 == 0)
    gets_h2 = jnp.logical_not(keeps_own & (layer == 1))
    early, late = h2_out.at[pl.ds(0, steps - LATE)], h2_out.at[pl.ds(0, LATE)]
    hand_on = remote(early, early, o_send.at[0, 0], o_recv.at[0], me_else)

    @pl.when(gets_h2)
    def _():
        hand_on.wait_recv()
        pl.when(cc == 1)(hand_on.start)

    for l, out in enumerate((c1_out, c2_out)):
        @pl.when(jnp.logical_not(keeps_own & (layer == l)))
        def _(l=l, out=out):
            arrived(out, c_recv.at[l])

    @pl.when(gets_h2)
    def _():
        arrived(late, o_recv.at[1])
        pl.when(cc == 1)(hand_on.wait_send)


def solution(mesh):
    n_row, n_col = mesh.shape["row"], mesh.shape["col"]

    def local_program(seq_in, w_in1, w_rec1, b_gate1, w_in2, w_rec2, b_gate2, h_init, c_init):
        steps, batch, k_rows = seq_in.shape
        unit = b_gate1.shape[0] // GATES
        cols = w_in1.shape[1]
        row = lax.axis_index("row")
        half_own = n_row // 2 * unit
        n_part = k_rows // CHUNK
        pair = 2 * unit

        hbm = pl.BlockSpec(memory_space=pl.ANY)
        near = pl.BlockSpec(memory_space=pltpu.VMEM)
        dma = pltpu.SemaphoreType.DMA
        vm = pltpu.VMEM
        block = (n_col, unit, cols)
        z_all = vm((steps, batch, cols), F32)
        by_step = dma((RING,))
        h2_pair, c1_pair, c2_pair = pl.pallas_call(
            functools.partial(lstm_kernel, n_row, n_col),
            out_shape=(
                jax.ShapeDtypeStruct((steps, batch, pair), BF16),
                jax.ShapeDtypeStruct((batch, pair), F32),
                jax.ShapeDtypeStruct((batch, pair), F32),
            ),
            in_specs=[hbm] * 5 + [near] * 4,
            out_specs=(hbm, hbm, hbm),
            scratch_shapes=[
                vm((4, k_rows, cols), BF16),
                vm((4, *block), BF16),
                vm((3, *block), BF16),
                vm((n_col, n_row, unit, cols), BF16),
                vm((2, *block), BF16),
                vm((n_col, 2, unit, cols), BF16),
                vm((2, steps, batch, k_rows), BF16),
                vm((2, 2, 1, cols), F32),
                vm((2, 1, cols), F32),
                vm((2, 2, batch, cols), F32),
                vm((steps + 1, n_col, 2, batch, half_own), BF16),
                z_all, z_all, z_all,
                vm((2, batch, cols), F32),
                vm((steps, n_col, batch, pair), BF16),
                vm((2, 2, batch, cols), F32),
                vm((batch, cols), F32),
                vm((2, batch, half_own), F32),
                vm((n_row, batch, pair), F32),
                vm((2, batch, pair), F32),
                vm((2, 1, cols), F32),
                dma((4,)), dma((2,)), dma((n_row,)), dma((3, n_part)), dma((3,)),
                dma((5,)), dma((5,)), dma((1,)),
                dma((2,)), dma((n_row,)),
                dma((2, n_col - 1, 2)), dma((2, n_col, 2)),
                by_step, by_step, by_step, dma((2, 2)), dma((2,)),
                dma((n_col,)), by_step,
                dma((n_row, 2)), dma((2,)),
                dma((n_row,)), dma((2,)), pltpu.SemaphoreType.REGULAR((1,)),
            ],
            compiler_params=pltpu.CompilerParams(collective_id=0, has_side_effects=True, vmem_limit_bytes=60 * 2**20),
        )(
            w_rec1, w_rec2, w_in1, w_in2, seq_in, b_gate1.reshape(1, -1), b_gate2.reshape(1, -1), h_init, c_init,
        )

        def own_half(both):
            return lax.dynamic_slice_in_dim(both, (row % 2) * unit, unit, axis=both.ndim - 1)

        return own_half(h2_pair), own_half(c1_pair), own_half(c2_pair)

    row_spec = P(None, "dp", "row")
    weight_spec = P("row", "col")
    bias_spec = P(("col", "row"))
    seq_out_spec = P(None, "dp", ("row", "col"))
    cell_out_spec = P("dp", ("row", "col"))
    return jax.shard_map(
        local_program,
        mesh=mesh,
        in_specs=(row_spec, weight_spec, weight_spec, bias_spec, weight_spec, weight_spec, bias_spec, row_spec, row_spec),
        out_specs=(seq_out_spec, cell_out_spec, cell_out_spec),
        check_vma=False,
    )
```

```python
import functools

import jax
import jax.numpy as jnp
from jax import lax
from jax.experimental import pallas as pl
from jax.experimental.pallas import tpu as pltpu
from jax.sharding import PartitionSpec as P


MESH = pl.DeviceIdType.MESH
F32, BF16 = jnp.float32, jnp.bfloat16
HALVES = LAYERS = (0, 1)
GATES = 4
LANES, TILE, PAIR, OWN = 128, 256, 512, 1024
HALF_LANES = 64
CHUNK = 32
HELD = 1
AHEAD = (5, 8, 12, 8)
FIRST = (4, 4, 7, 6)
EARLY = 3
MIDDLE = (3, 2)
H1_AHEAD = 3
RING = 24
OUT_STEPS = 2
LATE = 8
PEERS = (1, 3, 2)
ORDER = (PEERS, (2, 1, 3))


def sigmoid(v):
    return 0.5 * jnp.tanh(0.5 * v) + 0.5


def lstm_kernel(
    n_row, n_col, wr1, wr2, wi1, wi2, x_in, b1, b2, h0, c0, h2_out, c1_out, c2_out,
    raw, perm, relay, wbuf, wi1b, wi2b, xb, bb, bias2, init, hist, za, zb, zc, zmid, h1in, zout, zpre, cst, cin, cstart, bst,
    raw_sem, w_send, w_recv, rel_recv, rel_send, in_send, in_recv, x_local, c0_send, cin_recv,
    hx_send, hx_recv, za_recv, zb_recv, zc_recv, z_send, zm_send, h1_send, h1_recv, o_send, o_recv, c_send, c_recv, passed,
):
    steps = x_in.shape[0]
    n_x = n_row // 2
    n_part = raw.shape[1] // CHUNK
    per_col = n_part // n_col
    col, row = lax.axis_index("col"), lax.axis_index("row")
    xx, cc = row // 2, row % 2
    in_block = (xx < 2) == (col < 2)
    layer = xx // 2
    is_rec = in_block & (cc == 1)
    is_input = in_block == (cc == 0)
    not_input = jnp.logical_not(is_input)
    other_row = n_col - 1 - col

    def at(x, c, y):
        return {"row": x * 2 + c, "col": y}

    def input_core(x, y):
        return jnp.where((x < 2) == (y < 2), 0, 1)

    def is_away(l, k):
        return (k + n_col - 2 * l) % n_col // 2

    def owner_at(l, k):
        away = is_away(l, k)
        return at(2 * l + away, 1, jnp.where(away == 0, k, n_col - 1 - k))

    def remote(src, dst, ssem, rsem, dev):
        return pltpu.make_async_remote_copy(
            src_ref=src, dst_ref=dst, send_sem=ssem, recv_sem=rsem, device_id=dev, device_id_type=MESH)

    me_else = at(xx, 1 - cc, col)

    def arrived(ref, sem):
        remote(ref, ref, x_local.at[0], sem, me_else).wait_recv()

    def run(copies, go):
        for cp in copies:
            cp.start() if go else cp.wait_send()

    def dots(pieces):
        sums = [jnp.dot(rows, weights, preferred_element_type=F32) for rows, weights in pieces]
        return functools.reduce(jnp.add, sums)

    def cols_of(tile):
        return slice(tile * TILE, tile * TILE + TILE)

    loads = [pltpu.make_async_copy(w, raw.at[i], raw_sem.at[i]) for i, w in enumerate((wr1, wr2, wi1, wi2))]
    for load in loads:
        load.start()
    barrier = pltpu.get_barrier_semaphore()
    for dy in range(n_col):
        for dx in range(n_row):
            if dx or dy:
                pl.semaphore_signal(
                    barrier, inc=1, device_id={"row": (row + dx) % n_row, "col": (col + dy) % n_col}, device_id_type=MESH)

    lane_half = lax.broadcasted_iota(jnp.int32, (1, LANES), 1) // HALF_LANES

    def gate_major(i):
        for q in range(n_x):
            for pair in HALVES:
                at_left = q * PAIR + pair * LANES
                left, right = raw[i, :, at_left:at_left + LANES], raw[i, :, at_left + TILE:at_left + TILE + LANES]
                to = q // 2 * OWN + pair * PAIR + q % 2 * LANES
                low = jnp.concatenate([left[:, :HALF_LANES], right[:, :HALF_LANES]], axis=1)
                high = jnp.concatenate([left[:, HALF_LANES:], right[:, HALF_LANES:]], axis=1)
                for part, start in ((low, to), (high, to + TILE)):
                    perm[i, :, :, start:start + LANES] = part.reshape(n_col, -1, LANES)

    def to_half(tile, odd):
        moved = jnp.where(odd == row % 2, tile, pltpu.roll(tile, HALF_LANES, 1))
        return jnp.where(lane_half == row % 2, moved, 0.0)

    for l in LAYERS:
        cells = jnp.where(col < 2, c0[l, :, :LANES], c0[l, :, LANES:])
        cstart[l] = to_half(cells, col % 2)
        for m in range(GATES):
            start = m // 2 * LANES
            gate = to_half((b1, b2)[l][:, start:start + LANES], m % 2)
            for half in HALVES:
                for part in HALVES:
                    start = half * OWN + m * TILE + part * LANES
                    mine = (row // 4 == half) & (row % 4 // 2 == part)
                    bst[l, :, start:start + LANES] = jnp.where(mine, gate, 0.0)
    loads[0].wait()
    gate_major(0)
    pl.semaphore_wait(barrier, n_row * n_col - 1)

    def part_of(ref, c):
        return ref.at[c // per_col, pl.ds(c % per_col * CHUNK, CHUNK)]

    def start_up(l, go, chunks):
        xr, kr = (xx + n_x - 2 * l) % n_x, (col + n_col - 2 * l) % n_col
        home = kr < 2
        mine = home & (xr == 0) & (cc == 1)
        by_near = home & (xr == 2) & (cc == 0)
        by_far = jnp.logical_not(home) & (xr == 2)
        by_corner = jnp.logical_not(home) & ((xr == 3) | ((xr == 0) & (cc == 0)))
        relayed = by_near | by_far | by_corner
        rx = jnp.where(by_near, (2 * l + 1) % n_x, jnp.where(by_far, (2 * l + 2) % n_x, 2 * l))
        rdev = at(rx, jnp.where(by_far, 0, 1), jnp.where(by_near, col, other_row))
        slot = jnp.where(by_near, 0, jnp.where(by_far, cc, jnp.where(xr == 0, 0, 2 - cc)))
        owner = owner_at(l, col)
        cells = [remote(cstart.at[l], cin.at[row], c0_send.at[l], cin_recv.at[row], owner)]
        direct, by_relay = [], []
        for c in chunks:
            src = part_of(perm.at[l], c)
            direct.append(remote(src, part_of(wbuf.at[:, row], c), w_send.at[l], w_recv.at[row], owner))
            by_relay.append(remote(src, part_of(relay.at[slot], c), w_send.at[l], rel_recv.at[slot, c], rdev))
        if not go:
            direct = by_relay = [remote(perm.at[l], perm.at[l], w_send.at[l], w_recv.at[row], owner)]
        if chunks[0] == 0:
            @pl.when(jnp.logical_not(mine))
            def _():
                run(cells, go)

            if go:
                @pl.when(mine)
                def _():
                    wbuf[:, row] = perm[l]
                    cin[row] = cstart[l]

        @pl.when(jnp.logical_not(mine | relayed))
        def _():
            run(direct, go)

        @pl.when(relayed)
        def _():
            run(by_relay, go)

    all_chunks = range(n_part)
    held = all_chunks[n_part - HELD:]
    for l in LAYERS:
        if l:
            loads[l].wait()
            gate_major(l)
        start_up(l, True, all_chunks[:n_part - HELD])

        @pl.when(not_input)
        def _(l=l):
            start_up(l, True, held)

    for l in LAYERS:
        init[cc, l] = jnp.dot(h0[l].astype(BF16), perm[l].reshape(-1, perm.shape[-1]), preferred_element_type=F32)
    x_load = pltpu.make_async_copy(x_in, xb.at[cc], x_local.at[0])
    give = [remote(s, d, in_send.at[i], in_recv.at[i], me_else) for i, (s, d) in enumerate((
        (x_in, xb.at[cc]), (bst, bb.at[cc]), (init.at[cc], init.at[cc]), (perm.at[2], wi1b.at[cc]), (perm.at[3], wi2b.at[:, cc])))]
    soon = len(give) - 2

    @pl.when(is_input)
    def _():
        x_load.start()
        bb[cc] = bst[...]

    @pl.when(not_input)
    def _():
        run(give[:soon], True)

    for l in LAYERS:
        loads[2 + l].wait()
        gate_major(2 + l)

        @pl.when(is_input)
        def _(l=l):
            (wi1b.at[cc], wi2b.at[:, cc])[l][...] = perm[2 + l]

        @pl.when(not_input)
        def _(l=l):
            give[soon + l].start()

    def pass_on(slots, sources, to_x):
        dev = at(to_x, 1, col)

        def onward(s, c):
            return remote(part_of(relay.at[s], c), part_of(wbuf.at[:, sources[s]], c), rel_send.at[s],
                          w_recv.at[sources[s]], dev)

        for group in slots:
            for c in all_chunks:
                for s in group:
                    arrived(part_of(relay.at[s], c), rel_recv.at[s, c])
                    onward(s, c).start()

        def done():
            for group in slots:
                for s in group:
                    remote(relay.at[s], relay.at[s], rel_send.at[s], rel_recv.at[s, 0], dev).wait_send()

        return done

    def relays(then):
        for l in LAYERS:
            x0, x1, x2, x3 = [(2 * l + i) % n_x for i in range(n_x)]
            here = (col // 2) == l
            for core, x, args in (
                (1, x0, (((1, 2), (0,)), (2 * x0, 2 * x3 + 1, 2 * x3), x1)),
                (1, x1, (((0,),), (2 * x2,), x0)),
                (0, x2, (((0, 1),), (2 * x2, 2 * x2 + 1), x1)),
            ):
                yield l, core, here & (cc == core) & (xx == x), args

    for l, core, mine, args in relays(None):
        @pl.when(mine)
        def _(l=l, core=core, args=args):
            done = pass_on(*args)
            if core == 0:
                done()
                if l == 0:
                    pl.semaphore_signal(passed.at[0], inc=1, device_id=me_else, device_id_type=MESH)

    @pl.when(is_rec)
    def _():
        home = xx % 2 == 0
        own = jnp.where(home, col, other_row)
        beside, across, last = [(own + d) % n_col for d in PEERS]

        def peer(d):
            k = (own + d) % n_col
            away = is_away(layer, k)
            return at(2 * layer + away, 1, jnp.where(away == 0, k, n_col - 1 - k))

        def h_copy(t, owner, half, d):
            ref = hist.at[t + 1, owner, half]
            return remote(ref, ref, hx_send.at[t % 2, d - 1, half], hx_recv.at[t % 2, owner, half], peer(d))

        def products(t, pieces, cols=slice(None)):
            return dots([(hist[t + 1, owner, half], wbuf[owner, half * GATES:half * GATES + GATES, :, cols].reshape(TILE, -1))
                         for owner, half in pieces])

        def z_arrives(t):
            arrived(za.at[t], za_recv.at[t % RING])

            @pl.when(home)
            def _():
                arrived(zb.at[t], zb_recv.at[t % RING])
                arrived(zc.at[t], zc_recv.at[t % RING])

        def input_sums(t):
            return za[t] + jnp.where(home, zb[t] + zc[t], 0.0)

        def forward(t, go):
            near, far = jnp.where(home, 0, 1), jnp.where(home, 3, 2)
            for i, (x, c, y) in enumerate(((far, 1, col), (far, 1, other_row), (near, 1, other_row), (near, 0, col))):
                src = hist.at[t + 1, :, x // 2, :, pl.ds(pl.multiple_of(x % 2 * LANES, LANES), LANES)]
                run([remote(src, h1in.at[t], h1_send.at[i], h1_recv.at[t % RING], at(x, c, y))], go)

        def hand_h1(t):
            return remote(h1in.at[t], h1in.at[t], h1_send.at[0], h1_recv.at[t % RING], me_else)

        def middle(u, go):
            cp = remote(zmid.at[u % 2], zc.at[u], zm_send.at[u % 2], zc_recv.at[u % RING], at(2 * layer, 1, col))
            if go:
                arrived(zb.at[u], zb_recv.at[u % RING])
                arrived(zc.at[u], zc_recv.at[u % RING])
                zmid[u % 2] = zb[u] + zc[u]
            run([cp], go)

        lead = jnp.where(layer == 0, MIDDLE[0], MIDDLE[1])

        def out_copy(src, dst, ssem, rsem, r, home_row, go):
            away = remote(src, dst, ssem, rsem, {"row": r, "col": own})
            if r != home_row:
                run([away], go)
                return
            local = pltpu.make_async_copy(src, dst, ssem)

            @pl.when(home)
            def _():
                local.start() if go else local.wait()

            @pl.when(jnp.logical_not(home))
            def _():
                run([away], go)

        home_two = n_row // 2 + 1

        def pair_of(ref, r):
            return ref.at[r // 4, :, pl.ds(r // 2 % 2 * LANES, LANES)]

        def out_copies(n):
            rows = pl.ds(n * OUT_STEPS, OUT_STEPS)
            phase = n * OUT_STEPS // (steps - LATE)
            for r in range(n_row):
                src = hist.at[pl.ds(n * OUT_STEPS + 1, OUT_STEPS), own, r // 4, :, pl.ds(r // 2 % 2 * LANES, LANES)]

                def send(r=r, src=src):
                    out_copy(src, h2_out.at[rows], o_send.at[r, phase], o_recv.at[phase], r, home_two, True)

                if r % 2:
                    send()
                else:
                    pl.when((phase == 1) | (home & (r + 1 == home_two)))(send)

        def outs_sent():
            for phase, ref in enumerate((h2_out.at[pl.ds(0, steps - LATE)], h2_out.at[pl.ds(0, LATE)])):
                for r in range(n_row):
                    def sent(r=r, ref=ref, phase=phase):
                        out_copy(ref, ref, o_send.at[r, phase], o_recv.at[phase], r, home_two, False)

                    if r % 2 or phase:
                        sent()
                    elif r + 1 == home_two:
                        pl.when(home)(sent)

        def c_copies(l, go):
            for r in range(n_row):
                out_copy(pair_of(cst, r), (c1_out, c2_out)[l], c_send.at[r], c_recv.at[l], r, n_x * l + 1, go)

        for r in range(n_row):
            @pl.when(jnp.logical_not(home & (row == r)))
            def _(r=r):
                arrived(cin.at[r], cin_recv.at[r])
        for x in range(n_x):
            pair_of(cst, 2 * x)[...] = cin[2 * x] + cin[2 * x + 1]

        def run_ahead(u):
            @pl.when(layer == 1)
            def _():
                hand = hand_h1(u)
                hand.wait_recv()
                hand.start()
                hand.wait_send()

            @pl.when(jnp.logical_not(home) & (u < lead))
            def _():
                if u >= 2:
                    middle(u - 2, False)
                middle(u, True)

        for u in range(H1_AHEAD):
            run_ahead(u)
        z_arrives(0)
        zpre[...] = input_sums(0)

        def gates(t, z, send):
            for half in HALVES:
                i, f, g, o = z[half * GATES:half * GATES + GATES]
                c_new = sigmoid(f) * cst[half] + sigmoid(i) * jnp.tanh(g)
                cst[half] = c_new
                hist[t + 1, own, half] = (sigmoid(o) * jnp.tanh(c_new)).astype(BF16)
                if send:
                    run([h_copy(t, own, half, d) for d in ORDER[half]], True)

        tiles = range(2 * GATES)

        def finish(t, send, others):
            parts = others
            for half in HALVES:
                h_copy(t - 1, last, half, 2).wait_recv()
                parts = [part + products(t - 1, ((last, half),), cols_of(tile)) for tile, part in zip(tiles, parts)]
            gates(t, [part + zpre[:, cols_of(tile)] for tile, part in zip(tiles, parts)], send)

        def sent(t):
            for half in HALVES:
                run([h_copy(t, own, half, d) for d in PEERS], False)

        def outputs(t):
            @pl.when((layer == 1) & (t % OUT_STEPS == OUT_STEPS - 1))
            def _():
                out_copies(t // OUT_STEPS)

        def prepare(t):
            @pl.when((t > 1) & (layer == 0))
            def _():
                forward(t - 2, False)

            @pl.when((t > 0) & (layer == 0))
            def _():
                forward(t - 1, True)

            zpre[...] = products(t, [(own, half) for half in HALVES])
            u = t + lead

            @pl.when(jnp.logical_not(home) & (u < steps))
            def _():
                middle(u - 2, False)
                middle(u, True)

            @pl.when((layer == 1) & (t + H1_AHEAD < steps))
            def _():
                hand = hand_h1(t + H1_AHEAD)

                @pl.when(t > 0)
                def _():
                    hand.wait_send()

                hand.wait_recv()
                hand.start()

            @pl.when(t > 0)
            def _():
                sent(t - 1)

            outputs(t)
            parts = []
            for half in HALVES:
                if half:
                    z_arrives(t + 1)
                for d, owner in zip(PEERS, (beside, across)):
                    h_copy(t, owner, half, d).wait_recv()
                if half:
                    zpre[...] += input_sums(t + 1)
                parts.append([products(t, ((beside, half), (across, half)), cols_of(tile)) for tile in tiles])
            return [a + b for a, b in zip(*parts)]

        gates(0, [zpre[:, cols_of(tile)] for tile in tiles], True)
        for _, core, mine, args in relays(None):
            if core == 1:
                @pl.when(mine)
                def _(args=args):
                    slots, sources, to_x = args
                    for group in slots:
                        for s in group:
                            remote(relay.at[s], relay.at[s], rel_send.at[s], rel_recv.at[s, 0], me_else).wait_send()
        for r in range(n_row):
            @pl.when(jnp.logical_not(home & (row == r)))
            def _(r=r):
                arrived(wbuf.at[:, r], w_recv.at[r])

        end = steps - 1

        def step(t, carry):
            finish(t + 1, True, prepare(t))
            return carry

        lax.fori_loop(0, end - 1, step, 0)
        others = prepare(end - 1)

        @pl.when(jnp.logical_not(home))
        def _():
            middle(end - 1, False)
            middle(end, False)

        sent(end - 1)

        @pl.when(layer == 0)
        def _():
            forward(end - 2, False)
            finish(end, True, others)
            c_copies(0, True)
            forward(end - 1, True)
            forward(end - 1, False)
            for d, owner in zip(PEERS, (beside, across, last)):
                for half in HALVES:
                    h_copy(end, owner, half, d).wait_recv()
            forward(end, True)
            forward(end, False)
            sent(end)
            c_copies(0, False)

        @pl.when(layer == 1)
        def _():
            hand_h1(0).wait_send()
            finish(end, False, others)
            outputs(end)
            c_copies(1, True)
            outs_sent()
            c_copies(1, False)

    @pl.when(is_input)
    def _():
        x_load.wait()
        mate = 1 - cc
        for i, ref in enumerate((xb.at[mate], bb.at[mate], init.at[mate], wi1b.at[mate], wi2b.at[:, mate])):
            arrived(ref, in_recv.at[i])
        bias2[...] = bb[0] + bb[1]

        places, heads, middles, homes = [], [], [], []
        for l in LAYERS:
            xr, kr = (xx + n_x - 2 * l) % n_x, (col + n_col - 2 * l) % n_col
            homes.append(kr < 2)
            places.append(jnp.where(kr < 2, xr, (1 + n_x - xr) % n_x))
            heads.append((2 * l + jnp.where(kr < 2, 0, 1)) % n_x)
            middles.append((2 * l + jnp.where(kr < 2, 1, 0)) % n_x)

        def departure(l, u, start):
            p, home = places[l], homes[l]
            src = zout.at[l, u % 2]
            dst_x = jnp.where(p == 2, middles[l], jnp.where(home & (p == 1), xx, heads[l]))
            on = at(dst_x, jnp.where(home, 1, input_core(dst_x, col)), col)
            owner = owner_at(l, col)
            dev = {axis: jnp.where(p == 0, owner[axis], on[axis]) for axis in on}
            ways = [remote(src, buf.at[u], z_send.at[l, u % 2], sem.at[u % RING], dev)
                    for buf, sem in ((za, za_recv), (zb, zb_recv), (zc, zc_recv))]
            if not start:
                ways[0].wait_send()
                return
            to_c = home & (p == 1)
            to_b = (home & (p >= 2)) | (jnp.logical_not(home) & (p == 1))
            for way, here in zip(ways, (jnp.logical_not(to_b | to_c), to_b, to_c)):
                pl.when(here)(way.start)

        def input_sum(l, u):
            p = places[l]

            @pl.when(u >= 2)
            def _():
                departure(l, u - 2, False)

            if l == 0:
                part = dots([(xb[i, u], wi1b[i].reshape(TILE, -1)) for i in HALVES])
            else:
                h1 = jnp.concatenate([h1in[u, j] for j in range(n_col)], axis=1)
                part = dots([(h1, wi2b[...].reshape(2 * TILE, -1))])
            out = zout.at[l, u % 2]
            out[...] = part + bias2[l]

            @pl.when(u == 0)
            def _():
                out[...] += init[0, l] + init[1, l]

            adds = jnp.logical_not(homes[l])

            @pl.when(adds & (p < 2))
            def _():
                arrived(za.at[u], za_recv.at[u % RING])
                out[...] += za[u]

            @pl.when(adds & (p == 0))
            def _():
                arrived(zb.at[u], zb_recv.at[u % RING])
                out[...] += zb[u]

            departure(l, u, True)

        def ahead(u, carry):
            input_sum(0, u)
            return carry

        def by_place(values):
            return functools.reduce(lambda rest, i: jnp.where(places[0] == i, values[i], rest), range(1, n_x), values[0])

        first, lead = by_place(FIRST), by_place(AHEAD)

        def made(t):
            return jnp.minimum(steps, jnp.minimum(first + 2 * t, lead + t))

        soon_made = made(1)
        early = jnp.minimum(soon_made, EARLY)
        lax.fori_loop(0, 1, ahead, 0)
        for l in LAYERS:
            start_up(l, True, held)
        lax.fori_loop(1, early, ahead, 0)

        @pl.when((places[0] == 2) & (col < 2))
        def _():
            pl.semaphore_wait(passed.at[0], 1)

        lax.fori_loop(early, soon_made, ahead, 0)

        def step(t, carry):
            arrived(h1in.at[t], h1_recv.at[t % RING])
            input_sum(1, t)
            lax.fori_loop(made(t + 1), made(t + 2), ahead, 0)
            return carry

        lax.fori_loop(0, steps, step, 0)
        for l in LAYERS:
            for u in HALVES:
                departure(l, steps - 2 + u, False)

    for l in LAYERS:
        start_up(l, False, all_chunks)

    @pl.when(not_input)
    def _():
        run(give, False)

    keeps_own = is_rec & (xx % 2 == 0)
    gets_h2 = jnp.logical_not(keeps_own & (layer == 1))
    early, late = h2_out.at[pl.ds(0, steps - LATE)], h2_out.at[pl.ds(0, LATE)]
    hand_on = remote(early, early, o_send.at[0, 0], o_recv.at[0], me_else)

    @pl.when(gets_h2)
    def _():
        hand_on.wait_recv()
        pl.when(cc == 1)(hand_on.start)

    for l, out in enumerate((c1_out, c2_out)):
        @pl.when(jnp.logical_not(keeps_own & (layer == l)))
        def _(l=l, out=out):
            arrived(out, c_recv.at[l])

    @pl.when(gets_h2)
    def _():
        arrived(late, o_recv.at[1])
        pl.when(cc == 1)(hand_on.wait_send)


def solution(mesh):
    n_row, n_col = mesh.shape["row"], mesh.shape["col"]

    def local_program(seq_in, w_in1, w_rec1, b_gate1, w_in2, w_rec2, b_gate2, h_init, c_init):
        steps, batch, k_rows = seq_in.shape
        unit = b_gate1.shape[0] // GATES
        cols = w_in1.shape[1]
        row = lax.axis_index("row")
        half_own = n_row // 2 * unit
        n_part = k_rows // CHUNK
        pair = 2 * unit

        hbm = pl.BlockSpec(memory_space=pl.ANY)
        near = pl.BlockSpec(memory_space=pltpu.VMEM)
        dma = pltpu.SemaphoreType.DMA
        vm = pltpu.VMEM
        block = (n_col, unit, cols)
        z_all = vm((steps, batch, cols), F32)
        by_step = dma((RING,))
        h2_pair, c1_pair, c2_pair = pl.pallas_call(
            functools.partial(lstm_kernel, n_row, n_col),
            out_shape=(
                jax.ShapeDtypeStruct((steps, batch, pair), BF16),
                jax.ShapeDtypeStruct((batch, pair), F32),
                jax.ShapeDtypeStruct((batch, pair), F32),
            ),
            in_specs=[hbm] * 5 + [near] * 4,
            out_specs=(hbm, hbm, hbm),
            scratch_shapes=[
                vm((4, k_rows, cols), BF16),
                vm((4, *block), BF16),
                vm((3, *block), BF16),
                vm((n_col, n_row, unit, cols), BF16),
                vm((2, *block), BF16),
                vm((n_col, 2, unit, cols), BF16),
                vm((2, steps, batch, k_rows), BF16),
                vm((2, 2, 1, cols), F32),
                vm((2, 1, cols), F32),
                vm((2, 2, batch, cols), F32),
                vm((steps + 1, n_col, 2, batch, half_own), BF16),
                z_all, z_all, z_all,
                vm((2, batch, cols), F32),
                vm((steps, n_col, batch, pair), BF16),
                vm((2, 2, batch, cols), F32),
                vm((batch, cols), F32),
                vm((2, batch, half_own), F32),
                vm((n_row, batch, pair), F32),
                vm((2, batch, pair), F32),
                vm((2, 1, cols), F32),
                dma((4,)), dma((2,)), dma((n_row,)), dma((3, n_part)), dma((3,)),
                dma((5,)), dma((5,)), dma((1,)),
                dma((2,)), dma((n_row,)),
                dma((2, n_col - 1, 2)), dma((2, n_col, 2)),
                by_step, by_step, by_step, dma((2, 2)), dma((2,)),
                dma((n_col,)), by_step,
                dma((n_row, 2)), dma((2,)),
                dma((n_row,)), dma((2,)), pltpu.SemaphoreType.REGULAR((1,)),
            ],
            compiler_params=pltpu.CompilerParams(collective_id=0, has_side_effects=True, vmem_limit_bytes=60 * 2**20),
        )(
            w_rec1, w_rec2, w_in1, w_in2, seq_in, b_gate1.reshape(1, -1), b_gate2.reshape(1, -1), h_init, c_init,
        )

        def own_half(both):
            return lax.dynamic_slice_in_dim(both, (row % 2) * unit, unit, axis=both.ndim - 1)

        return own_half(h2_pair), own_half(c1_pair), own_half(c2_pair)

    row_spec = P(None, "dp", "row")
    weight_spec = P("row", "col")
    bias_spec = P(("col", "row"))
    seq_out_spec = P(None, "dp", ("row", "col"))
    cell_out_spec = P("dp", ("row", "col"))
    return jax.shard_map(
        local_program,
        mesh=mesh,
        in_specs=(row_spec, weight_spec, weight_spec, bias_spec, weight_spec, weight_spec, bias_spec, row_spec, row_spec),
        out_specs=(seq_out_spec, cell_out_spec, cell_out_spec),
        check_vma=False,
    )
```
